32 devices in a mesh: pod: 2 (over x), data: 4 (over z), expert: 4 (over y, core).
Axes of the slice: x: 2, y: 2, z: 4, core: 2. Of those that a mesh axis runs over, the one named last changes fastest.
Arguments:
- tokens: bfloat16 [16384, 1024], P(('pod', 'data', 'expert')), parts along dimension 0
- routes: int32 [16384, 8], P(('pod', 'data', 'expert')), parts along dimension 0
- gates: float32 [16384, 8], P(('pod', 'data', 'expert')), parts along dimension 0
- grad_y: bfloat16 [16384, 1024], P(('pod', 'data', 'expert')), parts along dimension 0
- w_in1: bfloat16 [32, 1024, 512], P('expert')
- w_in3: bfloat16 [32, 1024, 512], P('expert')
- w_out: bfloat16 [32, 512, 1024], P('expert')
Outputs:
- output 1: bfloat16 [16384, 1024], P(('pod', 'data', 'expert')), parts along dimension 0
- output 2: bfloat16 [16384, 1024], P(('pod', 'data', 'expert')), parts along dimension 0
- output 3: float32 [64, 1024, 512], P(('pod', 'expert')), parts along dimension 0
- output 4: float32 [64, 1024, 512], P(('pod', 'expert')), parts along dimension 0
- output 5: float32 [64, 512, 1024], P(('pod', 'expert')), parts along dimension 0
There are 2 independent parts. The reference program is written for one: setup_inputs(seed, part) draws one part's arguments, and reference() takes and returns one part's arrays. A program takes and returns all parts, laid end to end along the dimension named above; an argument that names none is the same for every part.
All inputs are finite; a program needn't handle non-finite values.
Results may differ from the reference program's by a relative error of at most 0.0106931.
Values are sent between devices in bfloat16 or wider.
A program may use at most 1 GiB of HBM per device.

```python
import functools
import jax
import jax.numpy as jnp
from jax import lax

D_MODEL = 1024
D_FF = 512
N_EXPERTS = 32
TOP_K = 8
TOK_DEV = 512
N_DATA = 4
N_EXPERT_DEV = 4
CAP_COLD = 128
CAP_HOT = 192
N_HOT = 2

GROUPS = N_DATA * N_EXPERT_DEV
TOK_PART = GROUPS * TOK_DEV


def hot_index_table(expert_ids):
    return jnp.where(expert_ids == 0, 0, jnp.where(expert_ids == N_EXPERTS // 2, 1, -1))


def draw_routes(key):
    key_hot, key_pos, key_base_a, key_base_b, key_step = jax.random.split(key, 5)
    n_cold = N_EXPERTS - N_HOT
    pattern = jnp.concatenate([
        jnp.zeros((CAP_HOT,), jnp.int32),
        jnp.ones((CAP_HOT,), jnp.int32),
        jnp.full((TOK_DEV - N_HOT * CAP_HOT,), -1, jnp.int32)])
    hot_of_tok = jax.random.permutation(key_hot, pattern)
    hot_slot = jax.random.randint(key_pos, (TOK_DEV, 1), 0, TOP_K)
    base_rank = jnp.minimum(jax.random.randint(key_base_a, (TOK_DEV, 1), 0, n_cold),
                            jax.random.randint(key_base_b, (TOK_DEV, 1), 0, n_cold))
    step_max = max(1, (n_cold - 1) // max(TOP_K - 1, 1))
    step_size = jax.random.randint(key_step, (TOK_DEV, 1), 1, step_max + 1)
    slot_ids = jnp.arange(TOP_K)[None, :]
    cold_rank = (base_rank + slot_ids * step_size) % n_cold
    cold_expert = cold_rank + 1 + (cold_rank + 1 >= N_EXPERTS // 2).astype(jnp.int32)
    use_hot = (hot_of_tok[:, None] >= 0) & (slot_ids == hot_slot)
    return jnp.where(use_hot, hot_of_tok[:, None] * (N_EXPERTS // 2), cold_expert).astype(jnp.int32)


def setup_inputs(seed: int = 0, part: int = 0) -> dict:
    key = jax.random.key(seed)
    key_part = jax.random.fold_in(key, part)
    key_tok, key_route, key_gate, key_grad = jax.random.split(key_part, 4)
    key_one, key_three, key_two = jax.random.split(jax.random.fold_in(key, 99991), 3)
    routes = jax.vmap(draw_routes)(jax.random.split(key_route, GROUPS)).reshape(TOK_PART, TOP_K)
    tokens = jax.random.normal(key_tok, (TOK_PART, D_MODEL), jnp.float32).astype(jnp.bfloat16)
    gates = jax.random.uniform(key_gate, (TOK_PART, TOP_K), jnp.float32, 0.5, 1.5)
    grad_y = jax.random.normal(key_grad, (TOK_PART, D_MODEL), jnp.float32).astype(jnp.bfloat16)
    w_in1 = (jax.random.normal(key_one, (N_EXPERTS, D_MODEL, D_FF), jnp.float32) * D_MODEL ** -0.5).astype(jnp.bfloat16)
    w_in3 = (jax.random.normal(key_three, (N_EXPERTS, D_MODEL, D_FF), jnp.float32) * D_MODEL ** -0.5).astype(jnp.bfloat16)
    w_out = (jax.random.normal(key_two, (N_EXPERTS, D_FF, D_MODEL), jnp.float32) * D_FF ** -0.5).astype(jnp.bfloat16)
    return dict(tokens=tokens, routes=routes, gates=gates, grad_y=grad_y, w_in1=w_in1, w_in3=w_in3, w_out=w_out)


def route_rows(routes_dev):
    flat_exp = routes_dev.reshape(-1)
    n_slots = flat_exp.shape[0]
    order = jnp.argsort(flat_exp, stable=True)
    counts = jax.ops.segment_sum(jnp.ones((n_slots,), jnp.int32), flat_exp, num_segments=N_EXPERTS)
    starts = jnp.cumsum(counts) - counts
    rank_sorted = jnp.arange(n_slots, dtype=jnp.int32) - starts[flat_exp[order]]
    slot_rank = jnp.zeros((n_slots,), jnp.int32).at[order].set(rank_sorted)
    hot_index = hot_index_table(flat_exp)
    cold_row = jnp.where((hot_index < 0) & (slot_rank < CAP_COLD), flat_exp * CAP_COLD + slot_rank, N_EXPERTS * CAP_COLD)
    hot_row = jnp.where(hot_index >= 0, hot_index * CAP_HOT + slot_rank, N_HOT * CAP_HOT)
    return cold_row, hot_row


def gather_rows(slot_rows, x_local, dy_local, gate_flat, n_rows):
    n_slots = slot_rows.shape[0]
    tok_n = x_local.shape[0]
    top_k = n_slots // tok_n
    src_tok = jnp.full((n_rows,), tok_n, jnp.int32).at[slot_rows].set(
        jnp.arange(n_slots, dtype=jnp.int32) // top_k, mode='drop')
    src_gate = jnp.zeros((n_rows,), jnp.float32).at[slot_rows].set(gate_flat, mode='drop')
    x_rows = jnp.take(x_local, src_tok, axis=0, mode='fill', fill_value=0)
    dy_rows = jnp.take(dy_local, src_tok, axis=0, mode='fill', fill_value=0)
    do_rows = (dy_rows.astype(jnp.float32) * src_gate[:, None]).astype(jnp.bfloat16)
    return x_rows, do_rows


def expert_pass(x_rows, do_rows, w_a, w_b, w_c):
    pre_a = jnp.dot(x_rows, w_a, preferred_element_type=jnp.float32).astype(jnp.bfloat16)
    pre_b = jnp.dot(x_rows, w_b, preferred_element_type=jnp.float32).astype(jnp.bfloat16)
    act_a = pre_a.astype(jnp.float32)
    act_b = pre_b.astype(jnp.float32)
    sigma_a = jax.nn.sigmoid(act_a)
    hidden = (act_a * sigma_a * act_b).astype(jnp.bfloat16)
    outs = jnp.dot(hidden, w_c, preferred_element_type=jnp.float32).astype(jnp.bfloat16)
    d_hidden = jnp.dot(do_rows, w_c.T, preferred_element_type=jnp.float32)
    d_pre_b = (d_hidden * act_a * sigma_a).astype(jnp.bfloat16)
    d_pre_a = (d_hidden * act_b * sigma_a * (1.0 + act_a * (1.0 - sigma_a))).astype(jnp.bfloat16)
    d_rows = (jnp.dot(d_pre_a, w_a.T, preferred_element_type=jnp.float32)
              + jnp.dot(d_pre_b, w_b.T, preferred_element_type=jnp.float32)).astype(jnp.bfloat16)
    grad_a = jnp.dot(x_rows.T, d_pre_a, preferred_element_type=jnp.float32)
    grad_b = jnp.dot(x_rows.T, d_pre_b, preferred_element_type=jnp.float32)
    grad_c = jnp.dot(hidden.T, do_rows, preferred_element_type=jnp.float32)
    return outs, d_rows, grad_a, grad_b, grad_c


def run_expert(operands):
    return expert_pass(*operands)


def combine(cold_rows, hot_rows, cold_vals, hot_vals, weights):
    slot_vals = (jnp.take(cold_vals, cold_rows, axis=0, mode='fill', fill_value=0)
                 + jnp.take(hot_vals, hot_rows, axis=0, mode='fill', fill_value=0))
    weighted = weights.reshape(TOK_DEV, TOP_K, 1) * slot_vals.reshape(TOK_DEV, TOP_K, D_MODEL).astype(jnp.float32)
    return jnp.sum(weighted, axis=1).astype(jnp.bfloat16)


def by_expert(buffers, n_buf, cap):
    return buffers.reshape(GROUPS, n_buf, cap, D_MODEL).transpose(1, 0, 2, 3).reshape(n_buf, GROUPS * cap, D_MODEL)


def by_device(buffers, n_buf, cap):
    return buffers.reshape(n_buf, GROUPS, cap, D_MODEL).transpose(1, 0, 2, 3).reshape(GROUPS, n_buf * cap, D_MODEL)


def reference(tokens, routes, gates, grad_y, w_in1, w_in3, w_out):
    x_dev = tokens.reshape(GROUPS, TOK_DEV, D_MODEL)
    dy_dev = grad_y.reshape(GROUPS, TOK_DEV, D_MODEL)
    gate_dev = gates.reshape(GROUPS, TOK_DEV * TOP_K)
    cold_row, hot_row = jax.vmap(route_rows)(routes.reshape(GROUPS, TOK_DEV, TOP_K))
    cold_x, cold_do = jax.vmap(functools.partial(gather_rows, n_rows=N_EXPERTS * CAP_COLD))(cold_row, x_dev, dy_dev, gate_dev)
    hot_x, hot_do = jax.vmap(functools.partial(gather_rows, n_rows=N_HOT * CAP_HOT))(hot_row, x_dev, dy_dev, gate_dev)
    hot_ids = jnp.array([0, N_EXPERTS // 2])
    cold_out, cold_dx, grad_one, grad_three, grad_two = lax.map(run_expert, (
        by_expert(cold_x, N_EXPERTS, CAP_COLD), by_expert(cold_do, N_EXPERTS, CAP_COLD), w_in1, w_in3, w_out))
    hot_out, hot_dx, hot_one, hot_three, hot_two = lax.map(run_expert, (
        by_expert(hot_x, N_HOT, CAP_HOT), by_expert(hot_do, N_HOT, CAP_HOT),
        w_in1[hot_ids], w_in3[hot_ids], w_out[hot_ids]))
    y_out = jax.vmap(combine)(cold_row, hot_row, by_device(cold_out, N_EXPERTS, CAP_COLD),
                              by_device(hot_out, N_HOT, CAP_HOT), gate_dev)
    grad_x = jax.vmap(combine)(cold_row, hot_row, by_device(cold_dx, N_EXPERTS, CAP_COLD),
                               by_device(hot_dx, N_HOT, CAP_HOT), jnp.ones_like(gate_dev))
    return (y_out.reshape(TOK_PART, D_MODEL), grad_x.reshape(TOK_PART, D_MODEL),
            grad_one.at[hot_ids].add(hot_one), grad_three.at[hot_ids].add(hot_three),
            grad_two.at[hot_ids].add(hot_two))
```

```python
import functools

import jax
import jax.numpy as jnp
from jax import lax
from jax.experimental import pallas as pl
from jax.experimental.pallas import tpu as pltpu
from jax.sharding import PartitionSpec as P

N_HOT = 2
RG_ROWS = 16
F32, BF16 = jnp.float32, jnp.bfloat16


def caps(tok_dev, top_k, n_exp):
    cap_hot = 3 * tok_dev // 8
    cap_cold = max(8, ((tok_dev * top_k - N_HOT * cap_hot) // (n_exp - N_HOT) + 7) // 8 * 8)
    return cap_cold, cap_hot


def dot_nn(a, b):
    return lax.dot_general(a, b, (((1,), (0,)), ((), ())), preferred_element_type=F32)


def dot_nt(a, b):
    return lax.dot_general(a, b, (((1,), (1,)), ((), ())), preferred_element_type=F32)


def dot_tn(a, b):
    return lax.dot_general(a, b, (((0,), (0,)), ((), ())), preferred_element_type=F32)


def prefix(m):
    lane = lax.broadcasted_iota(jnp.int32, m.shape, 1)
    step = 1
    while step < m.shape[1]:
        m = m + jnp.where(lane >= step, pltpu.roll(m, step, 1), 0.0)
        step *= 2
    return m


def stage_kernel(cfg, *refs):
    n_src, n_own, first = cfg["n_src"], cfg["n_own"], cfg["first"]
    tok, d_model, n_loc, n_exp = cfg["tok"], cfg["d_model"], cfg["n_loc"], cfg["n_exp"]
    cap, extra = cfg["cap"], cfg["extra"]
    refs = list(refs)
    rank_ref = refs.pop(0)
    srcs = [refs.pop(0) for _ in range(n_src)]
    w1, w3, w2 = (refs.pop(0) for _ in range(3))
    acc = None if first else [refs.pop(0) for _ in range(3)]
    outs = [refs.pop(0) for _ in range(3)]
    part_y, part_x = (refs.pop(0), refs.pop(0)) if n_own else (None, None)
    rows_x, rows_d, meta, buf, sem = refs
    step = pl.program_id(0)
    lead = rank_ref[0, 0]

    def fetch(s, src):
        return pltpu.make_async_copy(src, buf.at[s % 2], sem.at[s % 2])

    @pl.when(step == 0)
    def _():
        fetch(0, srcs[0]).start()

    for s in range(n_src):
        @pl.when(step == s)
        def _(s=s):
            fetch(s, srcs[s]).wait()
            if s + 1 < n_src:
                fetch(s + 1, srcs[s + 1]).start()

    slot = step % 2

    @pl.when(step < n_src)
    def gather():
        rg = buf[slot, 2 * tok:2 * tok + RG_ROWS, :].astype(F32)
        routes = rg[0:8, :tok]
        gates = (rg[8:16, :tok] + rg[0:8, tok:]) + rg[8:16, tok:]
        member, weight = [], []
        for i in range(n_loc):
            match = routes == (lead * n_loc + i).astype(F32)
            member.append(jnp.sum(jnp.where(match, 1.0, 0.0), axis=0, keepdims=True))
            weight.append(jnp.sum(jnp.where(match, gates, 0.0), axis=0, keepdims=True))
        member = jnp.concatenate(member, axis=0)
        weight = jnp.concatenate(weight, axis=0)
        rank = jnp.where(member > 0.0, prefix(member) - 1.0, -1.0)
        meta[step, 0:8, :] = rank
        meta[step, 8:16, :] = weight
        x = buf[slot, 0:tok, :]
        dy = buf[slot, tok:2 * tok, :]

        def rows_of(i, base, size):
            iota = lax.broadcasted_iota(jnp.int32, (size, tok), 0).astype(F32) + base
            match = iota == meta[step, pl.ds(i, 1), :]
            gate = jnp.sum(jnp.where(match, meta[step, pl.ds(8 + i, 1), :], 0.0), axis=1, keepdims=True)
            return jnp.where(match, 1.0, 0.0).astype(BF16), gate

        def put(pick, gate, at, size):
            rows_x[step, pl.ds(at, size), :] = dot_nn(pick, x).astype(BF16)
            rows_d[step, pl.ds(at, size), :] = (dot_nn(pick, dy) * gate).astype(BF16)

        def pair(k, carry):
            p0, g0 = rows_of(2 * k, 0.0, cap)
            p1, g1 = rows_of(2 * k + 1, 0.0, cap)
            put(jnp.concatenate([p0, p1], axis=0), jnp.concatenate([g0, g1], axis=0),
                pl.multiple_of(2 * cap * k, 2 * cap), 2 * cap)
            return carry

        lax.fori_loop(0, n_loc // 2, pair, 0)
        lead_exp = lead * n_loc
        hot = jnp.logical_or(lead_exp == 0, lead_exp == n_exp // 2)
        far = jnp.where(hot, float(cap), float(2 * tok))
        p, g = rows_of(0, far, extra)
        put(p, g, n_loc * cap, extra)

    def block(at, size, fresh):
        xe = rows_x[:, pl.ds(at, size), :].reshape(n_src * size, d_model)
        de = rows_d[:, pl.ds(at, size), :].reshape(n_src * size, d_model)
        a = dot_nn(xe, w1[0]).astype(BF16).astype(F32)
        b = dot_nn(xe, w3[0]).astype(BF16).astype(F32)
        dh = dot_nt(de, w2[0])
        sig = 0.5 * jnp.tanh(0.5 * a) + 0.5
        act = a * sig
        h = (act * b).astype(BF16)
        db = (dh * act).astype(BF16)
        da = (dh * b * sig * (1.0 + a * (1.0 - sig))).astype(BF16)
        for out, base, lhs, rhs in zip(outs, acc or outs, (xe, xe, h), (da, db, de)):
            if fresh and first:
                out[0] = dot_tn(lhs, rhs)
            else:
                src = base if fresh else out
                out[0] = src[0] + dot_tn(lhs, rhs)
        if n_own:
            m = n_own * size
            o = dot_nn(h[:m], w2[0]).astype(BF16)
            dx = (dot_nt(da[:m], w1[0]) + dot_nt(db[:m], w3[0])).astype(BF16)
            rows_x[0:n_own, pl.ds(at, size), :] = o.reshape(n_own, size, d_model)
            rows_d[0:n_own, pl.ds(at, size), :] = dx.reshape(n_own, size, d_model)

    exp = step - n_src

    @pl.when(jnp.logical_and(exp >= 0, exp < n_loc))
    def main():
        block(pl.multiple_of(exp * cap, cap), cap, True)

    @pl.when(exp == 0)
    def more():
        block(n_loc * cap, extra, False)

    if n_own:
        src = exp - n_loc

        @pl.when(src >= 0)
        def combine():
            def weights_of(i, base, size):
                iota = lax.broadcasted_iota(jnp.int32, (size, tok), 0).astype(F32) + base
                match = iota == meta[src, pl.ds(i, 1), :]
                gate = meta[src, pl.ds(8 + i, 1), :]
                hi = gate.astype(BF16).astype(F32)
                mid = (gate - hi).astype(BF16).astype(F32)
                low = gate - hi - mid
                return [jnp.where(match, v, 0.0).astype(BF16) for v in (1.0, hi, mid, low)]

            def sums(pieces, at, size):
                o = rows_x[src, pl.ds(at, size), :]
                dx = rows_d[src, pl.ds(at, size), :]
                one, hi, mid, low = pieces
                return dot_tn(hi, o) + dot_tn(mid, o) + dot_tn(low, o), dot_tn(one, dx)

            lead_exp = lead * n_loc
            hot = jnp.logical_or(lead_exp == 0, lead_exp == n_exp // 2)
            far = jnp.where(hot, float(cap), float(2 * tok))
            py, px = sums(weights_of(0, far, extra), n_loc * cap, extra)
            part_y[0] = py
            part_x[0] = px

            def pair(k, carry):
                both = [jnp.concatenate(z, axis=0) for z in zip(weights_of(2 * k, 0.0, cap), weights_of(2 * k + 1, 0.0, cap))]
                py, px = sums(both, pl.multiple_of(2 * cap * k, 2 * cap), 2 * cap)
                part_y[0] += py
                part_x[0] += px
                return carry

            lax.fori_loop(0, n_loc // 2, pair, 0)


def run_stage(name, lead, srcs, weights, acc, n_own, n_exp):
    w1, w3, w2 = weights
    n_loc, d_model, d_ff = w1.shape
    tok = (srcs[0].shape[0] - RG_ROWS) // 2
    n_src = len(srcs)
    cap, cap_hot = caps(tok, 8, n_exp)
    extra = cap_hot - cap
    first = acc is None
    cfg = dict(n_src=n_src, n_own=n_own, first=first, tok=tok, d_model=d_model, n_loc=n_loc, n_exp=n_exp, cap=cap, extra=extra)
    per_exp = lambda i: (jnp.clip(i - n_src, 0, n_loc - 1), 0, 0)
    per_src = lambda i: (jnp.clip(i - n_src - n_loc, 0, max(n_own, 1) - 1), 0, 0)
    spec_in = pl.BlockSpec((1, d_model, d_ff), per_exp)
    spec_out = pl.BlockSpec((1, d_ff, d_model), per_exp)
    spec_tok = pl.BlockSpec((1, tok, d_model), per_src)
    in_specs = [pl.BlockSpec(memory_space=pltpu.SMEM)] + [pl.BlockSpec(memory_space=pl.ANY)] * n_src + [spec_in, spec_in, spec_out]
    args = [lead, *srcs, w1, w3, w2]
    aliases = {}
    if not first:
        for k in range(3):
            aliases[len(args) + k] = k
        in_specs += [spec_in, spec_in, spec_out]
        args += list(acc)
    shapes = [jax.ShapeDtypeStruct((n_loc, d_model, d_ff), F32)] * 2 + [jax.ShapeDtypeStruct((n_loc, d_ff, d_model), F32)]
    out_specs = [spec_in, spec_in, spec_out]
    if n_own:
        shapes += [jax.ShapeDtypeStruct((n_own, tok, d_model), F32)] * 2
        out_specs += [spec_tok, spec_tok]
    per_src_rows = n_loc * cap + extra
    unit = 2 * d_model * d_ff * per_src_rows
    return pl.pallas_call(
        functools.partial(stage_kernel, cfg),
        grid=(n_src + n_loc + n_own,),
        in_specs=in_specs,
        out_specs=out_specs,
        out_shape=shapes,
        input_output_aliases=aliases,
        scratch_shapes=[
            pltpu.VMEM((n_src, per_src_rows, d_model), BF16),
            pltpu.VMEM((n_src, per_src_rows, d_model), BF16),
            pltpu.VMEM((n_src, 16, tok), F32),
            pltpu.VMEM((2, 2 * tok + RG_ROWS, d_model), BF16),
            pltpu.SemaphoreType.DMA((2,)),
        ],
        compiler_params=pltpu.CompilerParams(vmem_limit_bytes=67_000_000, dimension_semantics=("arbitrary",)),
        cost_estimate=pl.CostEstimate(flops=unit * (8 * n_src + 7 * n_own) // 8, bytes_accessed=100 << 20, transcendentals=0),
        name=name,
    )(*args)


def solution(mesh):
    n_data, n_er = mesh.shape["data"], mesh.shape["expert"]
    row_spec = P(("pod", "data", "expert"), None)
    w_spec = P("expert", None, None)
    grad_spec = P(("pod", "expert"), None, None)
    partner = [(r, r ^ 1) for r in range(n_er)]
    across = [(r, r ^ 2) for r in range(n_er)]
    around = [(q, (q + 1) % n_data) for q in range(n_data)]

    def body(tokens, routes, gates, grad_y, w_in1, w_in3, w_out):
        n_exp = w_in1.shape[0] * n_er
        lead = lax.axis_index("expert").astype(jnp.int32).reshape(1, 1)
        gate = gates.T
        hi = lax.reduce_precision(gate, 8, 7)
        mid = lax.reduce_precision(gate - hi, 8, 7)
        low = gate - hi - mid
        rg = jnp.concatenate([jnp.concatenate([routes.T.astype(F32), hi], 0), jnp.concatenate([mid, low], 0)], 1)
        pack = jnp.concatenate([tokens, grad_y, rg.astype(BF16)], 0)

        to_partner = lambda v: lax.ppermute(v, "expert", partner)
        to_across = lambda v: lax.ppermute(v, "expert", across)
        to_next = lambda v: lax.ppermute(v, "data", around)

        here, other, far, zed = pack, to_partner(pack), to_across(pack), to_next(pack)
        weights = (w_in1, w_in3, w_out)
        acc1, acc3, acc2, py0, px0 = run_stage("own_chip", lead, [here, other], weights, None, 2, n_exp)
        acc1, acc3, acc2, far, zed = lax.optimization_barrier((acc1, acc3, acc2, far, zed))
        far_other = to_partner(far)
        acc1, acc3, acc2, py1, px1 = run_stage("near_chip", lead, [far, far_other], weights, (acc1, acc3, acc2), 2, n_exp)
        got, got_far = to_partner(jnp.stack([py0[1], px0[1]])), to_partner(jnp.stack([py1[1], px1[1]]))
        for k in range(n_data - 1):
            yed, zed_other = to_across(zed), to_partner(zed)
            after = to_next(zed) if k + 2 < n_data else zed
            acc1, acc3, acc2, zed, zed_other, yed, after = lax.optimization_barrier((acc1, acc3, acc2, zed, zed_other, yed, after))
            if k == 1:
                got_far, acc1 = lax.optimization_barrier((got_far, acc1))
                back = to_across(jnp.stack([py1[0] + got_far[0], px1[0] + got_far[1]]))
            block = [zed, zed_other, yed, to_partner(yed)]
            acc1, acc3, acc2 = run_stage(f"hop{k}", lead, block, weights, (acc1, acc3, acc2), 0, n_exp)
            zed = after

        y_out = (py0[0] + got[0] + back[0]).astype(BF16)
        grad_x = (px0[0] + got[1] + back[1]).astype(BF16)
        return y_out, grad_x, acc1, acc3, acc2

    return jax.shard_map(body, mesh=mesh,
                         in_specs=(row_spec, row_spec, row_spec, row_spec, w_spec, w_spec, w_spec),
                         out_specs=(row_spec, row_spec, grad_spec, grad_spec, grad_spec),
                         check_vma=False)
```

```python
import functools

import jax
import jax.numpy as jnp
from jax import lax
from jax.experimental import pallas as pl
from jax.experimental.pallas import tpu as pltpu
from jax.sharding import PartitionSpec as P

N_HOT = 2
RG_ROWS = 16
F32, BF16 = jnp.float32, jnp.bfloat16


def caps(tok_dev, top_k, n_exp):
    cap_hot = 3 * tok_dev // 8
    cap_cold = max(8, ((tok_dev * top_k - N_HOT * cap_hot) // (n_exp - N_HOT) + 7) // 8 * 8)
    return cap_cold, cap_hot


def dot_nn(a, b):
    return lax.dot_general(a, b, (((1,), (0,)), ((), ())), preferred_element_type=F32)


def dot_nt(a, b):
    return lax.dot_general(a, b, (((1,), (1,)), ((), ())), preferred_element_type=F32)


def dot_tn(a, b):
    return lax.dot_general(a, b, (((0,), (0,)), ((), ())), preferred_element_type=F32)


def prefix(m):
    lane = lax.broadcasted_iota(jnp.int32, m.shape, 1)
    step = 1
    while step < m.shape[1]:
        m = m + jnp.where(lane >= step, pltpu.roll(m, step, 1), 0.0)
        step *= 2
    return m


def stage_kernel(cfg, *refs):
    n_src, n_own, first = cfg["n_src"], cfg["n_own"], cfg["first"]
    tok, d_model, n_loc, n_exp = cfg["tok"], cfg["d_model"], cfg["n_loc"], cfg["n_exp"]
    cap, extra, d_ff = cfg["cap"], cfg["extra"], cfg["d_ff"]
    cold = n_loc * cap
    refs = list(refs)
    take = lambda n: [refs.pop(0) for _ in range(n)]
    (rank_ref,) = take(1)
    srcs, weights = take(n_src), take(3)
    bases = [] if first else take(3)
    outs, parts = take(3), take(n_own)
    rows_x, rows_d, meta, pick, buf = take(5)
    hid, dab = take(2)
    w_bufs, g_bufs = take(2), take(2)
    src_sem, w_sem, in_sem, out_sem = take(4)
    gpick, sums, part_sem = take(3) if n_own else (None, None, None)
    step = pl.program_id(0)
    lead = rank_ref[0, 0]
    exp = step - n_src
    hot = jnp.logical_or(lead * n_loc == 0, lead * n_loc == n_exp // 2)
    far = jnp.where(hot, float(cap), float(2 * tok))

    def fetch(s):
        return pltpu.make_async_copy(srcs[s], buf.at[s % 2], src_sem.at[s % 2])

    def halves(bufs, slot):
        both, single = bufs[0].at[slot], bufs[1].at[slot]
        return both.at[:, 0:d_ff], both.at[:, d_ff:2 * d_ff], single

    def load_w(e):
        slot = lax.rem(e, 2)
        return [pltpu.make_async_copy(w.at[e], b, w_sem.at[slot, k]) for k, (w, b) in enumerate(zip(weights, halves(w_bufs, slot)))]

    def load_g(e):
        slot = lax.rem(e, 3)
        return [pltpu.make_async_copy(w.at[e], b, in_sem.at[slot, k]) for k, (w, b) in enumerate(zip(bases, halves(g_bufs, slot)))]

    def save_g(e):
        slot = lax.rem(e, 3)
        return [pltpu.make_async_copy(b, w.at[e], out_sem.at[slot, k]) for k, (w, b) in enumerate(zip(outs, halves(g_bufs, slot)))]

    def start(copies):
        for c in copies:
            c.start()

    def wait(copies):
        for c in copies:
            c.wait()

    @pl.when(step == 0)
    def _():
        fetch(0).start()
        start(load_w(0))
        start(load_g(0))

    for s in range(n_src):
        @pl.when(step == s)
        def _(s=s):
            fetch(s).wait()
            if s + 1 < n_src:
                fetch(s + 1).start()

    def match_rows(src, i, base, size):
        iota = lax.broadcasted_iota(jnp.int32, (size, tok), 0).astype(F32) + base
        return iota == meta[src, i:i + 1, :]

    pieces = [(i, 0.0, i * cap, cap) for i in range(n_loc)] + [(0, far, cold, extra)]

    @pl.when(step < n_src)
    def gather():
        slot = step % 2
        rg = buf[slot, 2 * tok:2 * tok + RG_ROWS, :].astype(F32)
        routes = rg[0:8, :tok]
        gates = (rg[8:16, :tok] + rg[0:8, tok:]) + rg[8:16, tok:]
        member, weight = [], []
        for i in range(n_loc):
            match = routes == (lead * n_loc + i).astype(F32)
            member.append(jnp.sum(jnp.where(match, 1.0, 0.0), axis=0, keepdims=True))
            weight.append(jnp.sum(jnp.where(match, gates, 0.0), axis=0, keepdims=True))
        member = jnp.concatenate(member, axis=0)
        meta[step, 0:8, :] = jnp.where(member > 0.0, prefix(member) - 1.0, -1.0)
        meta[step, 8:16, :] = jnp.concatenate(weight, axis=0)
        gate = []
        for i, base, at, size in pieces:
            match = match_rows(step, i, base, size)
            pick[at:at + size, :] = jnp.where(match, 1.0, 0.0).astype(BF16)
            gate.append(jnp.sum(jnp.where(match, meta[step, 8 + i:9 + i, :], 0.0), axis=1, keepdims=True))
        gate = jnp.concatenate(gate, axis=0)
        rows_x[step] = dot_nn(pick[...], buf[slot, 0:tok, :]).astype(BF16)
        rows_d[step] = (dot_nn(pick[...], buf[slot, tok:2 * tok, :]) * gate).astype(BF16)

    def block(at, size, w, g, g_in):
        w13, w2 = w_bufs[0].at[w], w_bufs[1].at[w]
        rows = n_src * size
        chunk = n_src if rows <= 4 * cap else 2
        for lo in range(0, n_src, chunk):
            m, at_c = chunk * size, lo * size
            x_c = rows_x[lo:lo + chunk, pl.ds(at, size), :].reshape(m, d_model)
            d_c = rows_d[lo:lo + chunk, pl.ds(at, size), :].reshape(m, d_model)
            ab = dot_nn(x_c, w13[...]).astype(BF16).astype(F32)
            dh = dot_nt(d_c, w2[...])
            a, b = ab[:, :d_ff], ab[:, d_ff:]
            sig = 0.5 * jnp.tanh(0.5 * a) + 0.5
            act = a * sig
            hid[at_c:at_c + m, :] = (act * b).astype(BF16)
            dab[at_c:at_c + m, 0:d_ff] = (dh * b * sig * (1.0 + a * (1.0 - sig))).astype(BF16)
            dab[at_c:at_c + m, d_ff:] = (dh * act).astype(BF16)
        xe = rows_x[:, pl.ds(at, size), :].reshape(rows, d_model)
        de = rows_d[:, pl.ds(at, size), :].reshape(rows, d_model)
        for out, lhs, rhs in ((g_bufs[0], xe, dab[0:rows, :]), (g_bufs[1], hid[0:rows, :], de)):
            if g_in:
                out[g] = out[g] + dot_tn(lhs, rhs)
            else:
                out[g] = dot_tn(lhs, rhs)
        if n_own:
            m = n_own * size
            o = dot_nn(hid[0:m, :], w2[...]).astype(BF16)
            dx = dot_nt(dab[0:m, :], w13[...]).astype(BF16)
            rows_x[0:n_own, pl.ds(at, size), :] = o.reshape(n_own, size, d_model)
            rows_d[0:n_own, pl.ds(at, size), :] = dx.reshape(n_own, size, d_model)

    @pl.when(jnp.logical_and(exp >= 0, exp < n_loc))
    def main():
        @pl.when(exp >= 2)
        def _():
            wait(save_g(exp - 2))

        @pl.when(exp + 1 < n_loc)
        def _():
            start(load_w(exp + 1))
            start(load_g(exp + 1))

        wait(load_w(exp))
        wait(load_g(exp))
        block(pl.multiple_of(exp * cap, cap), cap, lax.rem(exp, 2), lax.rem(exp, 3), not first)

        @pl.when(exp == 0)
        def more():
            block(cold, extra, 0, 0, True)

        start(save_g(exp))

    if n_own:
        src = exp - n_loc

        @pl.when(src >= 0)
        def combine():
            for i, base, at, size in pieces:
                match = match_rows(src, i, base, size)
                gate = meta[src, 8 + i:9 + i, :]
                hi = gate.astype(BF16).astype(F32)
                mid = (gate - hi).astype(BF16).astype(F32)
                low = gate - hi - mid
                pick[at:at + size, :] = jnp.where(match, 1.0, 0.0).astype(BF16)
                for k, v in enumerate((hi, mid, low)):
                    at_k = k * cold + at if at < cold else 3 * cold + k * extra
                    gpick[at_k:at_k + size, :] = jnp.where(match, v, 0.0).astype(BF16)
            o, last = rows_x[src, 0:cold, :], rows_x[src, cold:cold + extra, :]
            y = dot_tn(gpick[0:cold, :], o) + dot_tn(gpick[cold:2 * cold, :], o) + dot_tn(gpick[2 * cold:3 * cold, :], o)
            sums[src, 0] = y + dot_tn(gpick[3 * cold:3 * cold + 3 * extra, :], jnp.concatenate([last] * 3, axis=0))
            sums[src, 1] = dot_tn(pick[...], rows_d[src])

        for s in range(n_own):
            @pl.when(src == s)
            def _(s=s):
                pltpu.make_async_copy(sums.at[s], parts[s], part_sem.at[s]).start()

    @pl.when(step == n_src + n_loc + n_own - 1)
    def finish():
        wait(save_g(n_loc - 2))
        wait(save_g(n_loc - 1))
        for s in range(n_own):
            pltpu.make_async_copy(sums.at[s], parts[s], part_sem.at[s]).wait()


def run_stage(name, lead, srcs, weights, acc, n_own, n_exp):
    w1, w3, w2 = weights
    n_loc, d_model, d_ff = w1.shape
    tok = (srcs[0].shape[0] - RG_ROWS) // 2
    n_src = len(srcs)
    cap, cap_hot = caps(tok, 8, n_exp)
    extra = cap_hot - cap
    first = acc is None
    cfg = dict(n_src=n_src, n_own=n_own, first=first, tok=tok, d_model=d_model, d_ff=d_ff, n_loc=n_loc, n_exp=n_exp, cap=cap, extra=extra)
    args = [lead, *srcs, w1, w3, w2]
    aliases = {}
    if not first:
        aliases = {len(args) + k: k for k in range(3)}
        args += list(acc)
    shapes = [jax.ShapeDtypeStruct((n_loc, d_model, d_ff), F32)] * 2 + [jax.ShapeDtypeStruct((n_loc, d_ff, d_model), F32)]
    shapes += [jax.ShapeDtypeStruct((2, tok, d_model), F32)] * n_own
    rows = n_loc * cap + extra
    scratch = [
        pltpu.VMEM((n_src, rows, d_model), BF16),
        pltpu.VMEM((n_src, rows, d_model), BF16),
        pltpu.VMEM((n_src, 16, tok), F32),
        pltpu.VMEM((rows, tok), BF16),
        pltpu.VMEM((2, 2 * tok + RG_ROWS, d_model), BF16),
    ]
    scratch += [pltpu.VMEM((n_src * cap, d_ff), BF16), pltpu.VMEM((n_src * cap, 2 * d_ff), BF16)]
    for slots, kind in ((2, BF16), (3, F32)):
        scratch += [pltpu.VMEM((slots, d_model, 2 * d_ff), kind), pltpu.VMEM((slots, d_ff, d_model), kind)]
    scratch += [pltpu.SemaphoreType.DMA(n) for n in ((2,), (2, 3), (3, 3), (3, 3))]
    if n_own:
        scratch += [pltpu.VMEM((3 * rows, tok), BF16), pltpu.VMEM((n_own, 2, tok, d_model), F32), pltpu.SemaphoreType.DMA((n_own,))]
    unit = 2 * d_model * d_ff * rows
    return pl.pallas_call(
        functools.partial(stage_kernel, cfg),
        grid=(n_src + n_loc + n_own,),
        in_specs=[pl.BlockSpec(memory_space=pltpu.SMEM)] + [pl.BlockSpec(memory_space=pl.ANY)] * (len(args) - 1),
        out_specs=[pl.BlockSpec(memory_space=pl.ANY)] * len(shapes),
        out_shape=shapes,
        input_output_aliases=aliases,
        scratch_shapes=scratch,
        compiler_params=pltpu.CompilerParams(vmem_limit_bytes=67_000_000, dimension_semantics=("arbitrary",)),
        cost_estimate=pl.CostEstimate(flops=unit * (8 * n_src + 7 * n_own) // 8, bytes_accessed=100 << 20, transcendentals=0),
        name=name,
    )(*args)


def solution(mesh):
    n_data, n_er = mesh.shape["data"], mesh.shape["expert"]
    row_spec = P(("pod", "data", "expert"), None)
    w_spec = P("expert", None, None)
    grad_spec = P(("pod", "expert"), None, None)
    partner = [(r, r ^ 1) for r in range(n_er)]
    across = [(r, r ^ 2) for r in range(n_er)]
    around = [(q, (q + 1) % n_data) for q in range(n_data)]

    def body(tokens, routes, gates, grad_y, w_in1, w_in3, w_out):
        n_exp = w_in1.shape[0] * n_er
        lead = lax.axis_index("expert").astype(jnp.int32).reshape(1, 1)
        gate = gates.T
        hi = lax.reduce_precision(gate, 8, 7)
        mid = lax.reduce_precision(gate - hi, 8, 7)
        low = gate - hi - mid
        rg = jnp.concatenate([jnp.concatenate([routes.T.astype(F32), hi], 0), jnp.concatenate([mid, low], 0)], 1)
        pack = jnp.concatenate([tokens, grad_y, rg.astype(BF16)], 0)

        to_partner = lambda v: lax.ppermute(v, "expert", partner)
        to_across = lambda v: lax.ppermute(v, "expert", across)
        to_next = lambda v: lax.ppermute(v, "data", around)
        to_prev = lambda v: lax.ppermute(v, "data", [(b, a) for a, b in around])

        gate_open = lax.optimization_barrier
        weights = (w_in1, w_in3, w_out)
        here, other, far, z1 = pack, to_partner(pack), to_across(pack), to_next(pack)
        *acc, own_a, send_a = run_stage("own_chip", lead, [here, other], weights, None, 2, n_exp)
        far, z1, *acc = gate_open((far, z1, *acc))
        z1y, z2 = to_across(z1), to_next(z1)
        block = [far, to_partner(far), z1, to_partner(z1)]
        *acc, own_b, send_b = run_stage("near_chip", lead, block, weights, acc, 2, n_exp)
        z1y, z2, send_a, send_b, *acc = gate_open((z1y, z2, send_a, send_b, *acc))
        z2y, z3, z3y = to_across(z2), to_prev(here), to_prev(far)
        got_a, got_b = to_partner(send_a), to_partner(send_b)
        block = [z1y, to_partner(z1y), z2, to_partner(z2)]
        acc = run_stage("hop_a", lead, block, weights, acc, 0, n_exp)
        z2y, z3, z3y, got_a, got_b, *acc = gate_open((z2y, z3, z3y, got_a, got_b, *acc))
        back = to_across(own_b + got_b)
        block = [z2y, to_partner(z2y), z3, to_partner(z3), z3y, to_partner(z3y)]
        acc1, acc3, acc2 = run_stage("hop_b", lead, block, weights, acc, 0, n_exp)
        y_out = (own_a[0] + got_a[0] + back[0]).astype(BF16)
        grad_x = (own_a[1] + got_a[1] + back[1]).astype(BF16)
        return y_out, grad_x, acc1, acc3, acc2

    return jax.shard_map(body, mesh=mesh,
                         in_specs=(row_spec, row_spec, row_spec, row_spec, w_spec, w_spec, w_spec),
                         out_specs=(row_spec, row_spec, grad_spec, grad_spec, grad_spec),
                         check_vma=False)
```

```python
import functools

import jax
import jax.numpy as jnp
from jax import lax
from jax.experimental import pallas as pl
from jax.experimental.pallas import tpu as pltpu
from jax.sharding import PartitionSpec as P


N_HOT = 2
RG_ROWS = 16
F32, BF16 = jnp.float32, jnp.bfloat16


def caps(tok_dev, top_k, n_exp):
    cap_hot = 3 * tok_dev // 8
    cap_cold = max(8, ((tok_dev * top_k - N_HOT * cap_hot) // (n_exp - N_HOT) + 7) // 8 * 8)
    return cap_cold, cap_hot


def dot_nn(a, b):
    return lax.dot_general(a, b, (((1,), (0,)), ((), ())), preferred_element_type=F32)


def dot_nt(a, b):
    return lax.dot_general(a, b, (((1,), (1,)), ((), ())), preferred_element_type=F32)


def dot_tn(a, b):
    return lax.dot_general(a, b, (((0,), (0,)), ((), ())), preferred_element_type=F32)


def prefix(m):
    lane = lax.broadcasted_iota(jnp.int32, m.shape, 1)
    step = 1
    while step < m.shape[1]:
        m = m + jnp.where(lane >= step, pltpu.roll(m, step, 1), 0.0)
        step *= 2
    return m


def stage_kernel(cfg, *refs):
    n_src, n_own, first, group = cfg["n_src"], cfg["n_own"], cfg["first"], cfg["group"]
    tok, d_model, n_loc, n_exp = cfg["tok"], cfg["d_model"], cfg["n_loc"], cfg["n_exp"]
    cap, extra, d_ff = cfg["cap"], cfg["extra"], cfg["d_ff"]
    cold, part = n_loc * cap, group * cap
    refs = list(refs)
    take = lambda n: [refs.pop(0) for _ in range(n)]
    (rank_ref,) = take(1)
    srcs, weights = take(n_src), take(3)
    bases = [] if first else take(3)
    outs, parts = take(3), take(n_own)
    rows_x, rows_d, meta, buf, hid, dab = take(6)
    w_bufs, g_bufs = take(2), take(2)
    src_sem, w_sem, in_sem, out_sem = take(4)
    kept_o, kept_x, pick, gpick, sums, part_sem = take(6) if n_own else [None] * 6
    lead = rank_ref[0, 0]
    hot = jnp.logical_or(lead * n_loc == 0, lead * n_loc == n_exp // 2)
    far = jnp.where(hot, float(cap), float(2 * tok))

    def fetch(s):
        return pltpu.make_async_copy(srcs[s], buf.at[s], src_sem.at[s])

    def halves(bufs, slot):
        both, single = bufs[0].at[slot], bufs[1].at[slot]
        return both.at[:, 0:d_ff], both.at[:, d_ff:2 * d_ff], single

    def load_w(e):
        slot = lax.rem(e, 2)
        return [pltpu.make_async_copy(w.at[e], b, w_sem.at[slot, k]) for k, (w, b) in enumerate(zip(weights, halves(w_bufs, slot)))]

    def load_g(e):
        slot = lax.rem(e, 3)
        return [pltpu.make_async_copy(w.at[e], b, in_sem.at[slot, k]) for k, (w, b) in enumerate(zip(bases, halves(g_bufs, slot)))]

    def save_g(e):
        slot = lax.rem(e, 3)
        return [pltpu.make_async_copy(b, w.at[e], out_sem.at[slot, k]) for k, (w, b) in enumerate(zip(outs, halves(g_bufs, slot)))]

    def start(copies):
        for c in copies:
            c.start()

    def wait(copies):
        for c in copies:
            c.wait()

    def ready_slot(e):
        @pl.when(e >= 3)
        def _():
            wait(save_g(e - 3))

        @pl.when(e < n_loc)
        def _():
            start(load_g(e))

    def match_rows(src, i, base, size):
        iota = lax.broadcasted_iota(jnp.int32, (size, tok), 0).astype(F32) + base
        return iota == meta[src, pl.ds(i, 1), :]

    def ranks(s):
        rg = buf[s, 2 * tok:2 * tok + RG_ROWS, :].astype(F32)
        routes = rg[0:8, :tok]
        gates = (rg[8:16, :tok] + rg[0:8, tok:]) + rg[8:16, tok:]
        member, weight = [], []
        for i in range(n_loc):
            match = routes == (lead * n_loc + i).astype(F32)
            member.append(jnp.sum(jnp.where(match, 1.0, 0.0), axis=0, keepdims=True))
            weight.append(jnp.sum(jnp.where(match, gates, 0.0), axis=0, keepdims=True))
        member = jnp.concatenate(member, axis=0)
        meta[s, 0:8, :] = jnp.where(member > 0.0, prefix(member) - 1.0, -1.0)
        meta[s, 8:16, :] = jnp.concatenate(weight, axis=0)

    def gather(s, which):
        pick_s, gate = [], []
        for i, base, at, size in which:
            match = match_rows(s, i, base, size)
            pick_s.append(jnp.where(match, 1.0, 0.0).astype(BF16))
            gate.append(jnp.sum(jnp.where(match, meta[s, pl.ds(8 + i, 1), :], 0.0), axis=1, keepdims=True))
        pick_s, gate = jnp.concatenate(pick_s, axis=0), jnp.concatenate(gate, axis=0)
        at, size = which[0][2], pick_s.shape[0]
        rows_x[s, at:at + size, :] = dot_nn(pick_s, buf[s, 0:tok, :]).astype(BF16)
        rows_d[s, at:at + size, :] = (dot_nn(pick_s, buf[s, tok:2 * tok, :]) * gate).astype(BF16)

    def block(at, size, keep, w, g, g_in):
        w13, w2 = w_bufs[0].at[w], w_bufs[1].at[w]
        rows = n_src * size
        chunk = n_src if rows <= 4 * cap else 2
        for lo in range(0, n_src, chunk):
            m, at_c = chunk * size, lo * size
            x_c = rows_x[lo:lo + chunk, pl.ds(at, size), :].reshape(m, d_model)
            d_c = rows_d[lo:lo + chunk, pl.ds(at, size), :].reshape(m, d_model)
            ab = dot_nn(x_c, w13[...]).astype(BF16).astype(F32)
            dh = dot_nt(d_c, w2[...])
            a, b = ab[:, :d_ff], ab[:, d_ff:]
            sig = 0.5 * jnp.tanh(0.5 * a) + 0.5
            act = a * sig
            hid[at_c:at_c + m, :] = (act * b).astype(BF16)
            dab[at_c:at_c + m, 0:d_ff] = (dh * b * sig * (1.0 + a * (1.0 - sig))).astype(BF16)
            dab[at_c:at_c + m, d_ff:] = (dh * act).astype(BF16)
        xe = rows_x[:, pl.ds(at, size), :].reshape(rows, d_model)
        de = rows_d[:, pl.ds(at, size), :].reshape(rows, d_model)
        for out, lhs, rhs in ((g_bufs[0], xe, dab[0:rows, :]), (g_bufs[1], hid[0:rows, :], de)):
            if g_in:
                out[g] = out[g] + dot_tn(lhs, rhs)
            else:
                out[g] = dot_tn(lhs, rhs)
        if n_own:
            m = n_own * size
            o = dot_nn(hid[0:m, :], w2[...]).astype(BF16)
            dx = dot_nt(dab[0:m, :], w13[...]).astype(BF16)
            kept_o[:, pl.ds(keep, size), :] = o.reshape(n_own, size, d_model)
            kept_x[:, pl.ds(keep, size), :] = dx.reshape(n_own, size, d_model)

    for s in range(n_src):
        fetch(s).start()
    start(load_w(0))
    start(load_g(0))
    start(load_g(1))

    def wave(p, carry):
        for s in range(n_src):
            @pl.when(p == 0)
            def _(s=s):
                fetch(s).wait()
                ranks(s)
                gather(s, [(0, far, part, extra)])

        if n_src % 2:
            raise ValueError("pairs")

        def two(t, carry):
            for s in (2 * t, 2 * t + 1):
                gather(s, [(group * p + i, 0.0, i * cap, cap) for i in range(group)])
            return carry

        lax.fori_loop(0, n_src // 2, two, 0)

        def one(i, carry):
            e = group * p + i
            wait(load_w(e))

            @pl.when(e + 1 < n_loc)
            def _():
                start(load_w(e + 1))

            wait(load_g(e))
            block(pl.multiple_of(i * cap, cap), cap, pl.multiple_of(e * cap, cap), lax.rem(e, 2), lax.rem(e, 3), not first)

            @pl.when(e == 0)
            def more():
                block(part, extra, cold, 0, 0, True)

            start(save_g(e))
            ready_slot(e + 2)
            return carry

        lax.fori_loop(0, group, one, 0)
        return carry

    lax.fori_loop(0, n_loc // group, wave, 0)

    if n_own:
        pieces = [(i, 0.0, i * cap, cap) for i in range(n_loc)] + [(0, far, cold, extra)]

        def combine(src, carry):
            for i, base, at, size in pieces:
                match = match_rows(src, i, base, size)
                gate = meta[src, 8 + i:9 + i, :]
                hi = gate.astype(BF16).astype(F32)
                mid = (gate - hi).astype(BF16).astype(F32)
                low = gate - hi - mid
                pick[at:at + size, :] = jnp.where(match, 1.0, 0.0).astype(BF16)
                for k, v in enumerate((hi, mid, low)):
                    at_k = k * cold + at if at < cold else 3 * cold + k * extra
                    gpick[at_k:at_k + size, :] = jnp.where(match, v, 0.0).astype(BF16)
            o, last = kept_o[src, 0:cold, :], kept_o[src, cold:cold + extra, :]
            y = dot_tn(gpick[0:cold, :], o) + dot_tn(gpick[cold:2 * cold, :], o) + dot_tn(gpick[2 * cold:3 * cold, :], o)
            y = y + dot_tn(gpick[3 * cold:3 * cold + 3 * extra, :], jnp.concatenate([last] * 3, axis=0))
            dx = dot_tn(pick[...], kept_x[src])
            for s in range(1, n_own):
                @pl.when(src == s)
                def _(s=s):
                    pltpu.make_async_copy(sums, parts[s - 1], part_sem).wait()

            sums[0] = y
            sums[1] = dx
            for s in range(n_own):
                @pl.when(src == s)
                def _(s=s):
                    pltpu.make_async_copy(sums, parts[s], part_sem).start()
            return carry

        lax.fori_loop(0, n_own, combine, 0)
        pltpu.make_async_copy(sums, parts[n_own - 1], part_sem).wait()
    wait(save_g(n_loc - 1))


def run_stage(lead, srcs, weights, acc, n_own, n_exp):
    w1, w3, w2 = weights
    n_loc, d_model, d_ff = w1.shape
    tok = (srcs[0].shape[0] - RG_ROWS) // 2
    n_src = len(srcs)
    cap, cap_hot = caps(tok, 8, n_exp)
    extra = cap_hot - cap
    first = acc is None
    group = 2 if n_own else 4
    cfg = dict(n_src=n_src, n_own=n_own, first=first, group=group, tok=tok, d_model=d_model, d_ff=d_ff, n_loc=n_loc, n_exp=n_exp,
               cap=cap, extra=extra)
    args = [lead, *srcs, w1, w3, w2]
    aliases = {}
    if not first:
        aliases = {len(args) + k: k for k in range(3)}
        args += list(acc)
    shapes = [jax.ShapeDtypeStruct((n_loc, d_model, d_ff), F32)] * 2 + [jax.ShapeDtypeStruct((n_loc, d_ff, d_model), F32)]
    shapes += [jax.ShapeDtypeStruct((2, tok, d_model), F32)] * n_own
    rows = n_loc * cap + extra
    scratch = [pltpu.VMEM((n_src, group * cap + extra, d_model), BF16)] * 2 + [
        pltpu.VMEM((n_src, 16, tok), F32),
        pltpu.VMEM((n_src, 2 * tok + RG_ROWS, d_model), BF16),
        pltpu.VMEM((n_src * cap, d_ff), BF16),
        pltpu.VMEM((n_src * cap, 2 * d_ff), BF16),
    ]
    for slots, kind in ((2, BF16), (3, F32)):
        scratch += [pltpu.VMEM((slots, d_model, 2 * d_ff), kind), pltpu.VMEM((slots, d_ff, d_model), kind)]
    scratch += [pltpu.SemaphoreType.DMA(n) for n in ((n_src,), (2, 3), (3, 3), (3, 3))]
    if n_own:
        scratch += [pltpu.VMEM((n_own, rows, d_model), BF16)] * 2
        scratch += [pltpu.VMEM((rows, tok), BF16), pltpu.VMEM((3 * rows, tok), BF16), pltpu.VMEM((2, tok, d_model), F32), pltpu.SemaphoreType.DMA]
    unit = 2 * d_model * d_ff * rows
    return pl.pallas_call(
        functools.partial(stage_kernel, cfg),
        in_specs=[pl.BlockSpec(memory_space=pltpu.SMEM)] + [pl.BlockSpec(memory_space=pl.ANY)] * (len(args) - 1),
        out_specs=[pl.BlockSpec(memory_space=pl.ANY)] * len(shapes),
        out_shape=shapes,
        input_output_aliases=aliases,
        scratch_shapes=scratch,
        compiler_params=pltpu.CompilerParams(vmem_limit_bytes=67_000_000),
        cost_estimate=pl.CostEstimate(flops=unit * (8 * n_src + 7 * n_own) // 8, bytes_accessed=100 << 20, transcendentals=0),
    )(*args)


def solution(mesh):
    n_data, n_er = mesh.shape["data"], mesh.shape["expert"]
    row_spec = P(("pod", "data", "expert"), None)
    w_spec = P("expert", None, None)
    grad_spec = P(("pod", "expert"), None, None)
    partner = [(r, r ^ 1) for r in range(n_er)]
    across = [(r, r ^ 2) for r in range(n_er)]
    around = [(q, (q + 1) % n_data) for q in range(n_data)]

    def move(axis, pairs, value):
        return lax.ppermute(value, axis, pairs)

    def body(tokens, routes, gates, grad_y, w_in1, w_in3, w_out):
        n_exp = w_in1.shape[0] * n_er
        lead = lax.axis_index("expert").astype(jnp.int32).reshape(1, 1)
        gate = gates.T
        hi = lax.reduce_precision(gate, 8, 7)
        mid = lax.reduce_precision(gate - hi, 8, 7)
        low = gate - hi - mid
        rg = jnp.concatenate([jnp.concatenate([routes.T.astype(F32), hi], 0), jnp.concatenate([mid, low], 0)], 1)
        pack = jnp.concatenate([tokens, grad_y, rg.astype(BF16)], 0)

        def to_partner(v):
            return move("expert", partner, v)

        def to_across(v):
            return move("expert", across, v)

        def to_next(v):
            return move("data", around, v)

        def to_prev(v):
            return move("data", [(b, a) for a, b in around], v)

        gate_open = lax.optimization_barrier
        weights = (w_in1, w_in3, w_out)
        here, other, far, z1 = pack, to_partner(pack), to_across(pack), to_next(pack)
        z3 = to_prev(here)
        *acc, own_a, send_a = run_stage(lead, [here, other], weights, None, 2, n_exp)
        far, z1, *acc = gate_open((far, z1, *acc))
        z1y, z2 = to_across(z1), to_next(z1)
        block = [far, to_partner(far), z1, to_partner(z1)]
        *acc, own_b, send_b = run_stage(lead, block, weights, acc, 2, n_exp)
        z1y, z2, send_a, send_b, *acc = gate_open((z1y, z2, send_a, send_b, *acc))
        z2y, z3y = to_across(z2), to_prev(far)
        got_a, got_b = to_partner(send_a), to_partner(send_b)
        block = [z1y, to_partner(z1y), z2, to_partner(z2)]
        acc = run_stage(lead, block, weights, acc, 0, n_exp)
        z2y, z3, z3y, got_a, got_b, *acc = gate_open((z2y, z3, z3y, got_a, got_b, *acc))
        back = to_across(own_b + got_b)
        block = [z2y, to_partner(z2y), z3, to_partner(z3), z3y, to_partner(z3y)]
        acc1, acc3, acc2 = run_stage(lead, block, weights, acc, 0, n_exp)
        y_out = (own_a[0] + got_a[0] + back[0]).astype(BF16)
        grad_x = (own_a[1] + got_a[1] + back[1]).astype(BF16)
        return y_out, grad_x, acc1, acc3, acc2

    return jax.shard_map(body, mesh=mesh,
                         in_specs=(row_spec, row_spec, row_spec, row_spec, w_spec, w_spec, w_spec),
                         out_specs=(row_spec, row_spec, grad_spec, grad_spec, grad_spec),
                         check_vma=False)
```

```python
import functools

import jax
import jax.numpy as jnp
from jax import lax
from jax.experimental import pallas as pl
from jax.experimental.pallas import tpu as pltpu
from jax.sharding import PartitionSpec as P


N_HOT = 2
RG_ROWS = 16
F32, BF16 = jnp.float32, jnp.bfloat16


def caps(tok_dev, top_k, n_exp):
    cap_hot = 3 * tok_dev // 8
    cap_cold = max(8, ((tok_dev * top_k - N_HOT * cap_hot) // (n_exp - N_HOT) + 7) // 8 * 8)
    return cap_cold, cap_hot


def dot_nn(a, b):
    return lax.dot_general(a, b, (((1,), (0,)), ((), ())), preferred_element_type=F32)


def dot_nt(a, b):
    return lax.dot_general(a, b, (((1,), (1,)), ((), ())), preferred_element_type=F32)


def dot_tn(a, b):
    return lax.dot_general(a, b, (((0,), (0,)), ((), ())), preferred_element_type=F32)


def prefix(m):
    lane = lax.broadcasted_iota(jnp.int32, m.shape, 1)
    step = 1
    while step < m.shape[1]:
        m = m + jnp.where(lane >= step, pltpu.roll(m, step, 1), 0.0)
        step *= 2
    return m


def stage_kernel(cfg, *refs):
    n_src, n_own, first, group = cfg["n_src"], cfg["n_own"], cfg["first"], cfg["group"]
    tok, d_model, n_loc, n_exp = cfg["tok"], cfg["d_model"], cfg["n_loc"], cfg["n_exp"]
    cap, extra, d_ff = cfg["cap"], cfg["extra"], cfg["d_ff"]
    cold, part = n_loc * cap, group * cap
    refs = list(refs)
    take = lambda n: [refs.pop(0) for _ in range(n)]
    (rank_ref,) = take(1)
    srcs, weights = take(n_src), take(3)
    bases = [] if first else take(3)
    outs, parts = take(3), take(n_own)
    rows_x, rows_d, meta, buf, hid, dab = take(6)
    w_bufs, g_bufs = take(2), take(2)
    src_sem, w_sem, in_sem, out_sem = take(4)
    kept_o, kept_x, pick, gpick, part_sem = take(5) if n_own else [None] * 5
    lead = rank_ref[0, 0]
    hot = jnp.logical_or(lead * n_loc == 0, lead * n_loc == n_exp // 2)
    far = jnp.where(hot, float(cap), float(2 * tok))

    def fetch(s):
        return pltpu.make_async_copy(srcs[s], buf.at[s], src_sem.at[s])

    def halves(bufs, slot):
        both, single = bufs[0].at[slot], bufs[1].at[slot]
        return both.at[:, 0:d_ff], both.at[:, d_ff:2 * d_ff], single

    def load_w(e):
        slot = lax.rem(e, 2)
        return [pltpu.make_async_copy(w.at[e], b, w_sem.at[slot, k]) for k, (w, b) in enumerate(zip(weights, halves(w_bufs, slot)))]

    def load_g(e):
        slot = lax.rem(e, 4)
        return [pltpu.make_async_copy(w.at[e], b, in_sem.at[slot, k]) for k, (w, b) in enumerate(zip(bases, halves(g_bufs, slot)))]

    def save_g(e):
        slot = lax.rem(e, 4)
        return [pltpu.make_async_copy(b, w.at[e], out_sem.at[slot, k]) for k, (w, b) in enumerate(zip(outs, halves(g_bufs, slot)))]

    def start(copies):
        for c in copies:
            c.start()

    def wait(copies):
        for c in copies:
            c.wait()

    def turn_slot(e):
        @pl.when(e >= 4)
        def _():
            wait(save_g(e - 4))

        @pl.when(e < n_loc)
        def _():
            start(load_g(e))

    def match_rows(src, i, base, size):
        iota = lax.broadcasted_iota(jnp.int32, (size, tok), 0).astype(F32) + base
        return iota == meta[src, pl.ds(i, 1), :]

    def ranks(s):
        rg = buf[s, 2 * tok:2 * tok + RG_ROWS, :].astype(F32)
        routes = rg[0:8, :tok]
        gates = (rg[8:16, :tok] + rg[0:8, tok:]) + rg[8:16, tok:]
        member, weight = [], []
        for i in range(n_loc):
            match = routes == (lead * n_loc + i).astype(F32)
            member.append(jnp.sum(jnp.where(match, 1.0, 0.0), axis=0, keepdims=True))
            weight.append(jnp.sum(jnp.where(match, gates, 0.0), axis=0, keepdims=True))
        member = jnp.concatenate(member, axis=0)
        meta[s, 0:8, :] = jnp.where(member > 0.0, prefix(member) - 1.0, -1.0)
        meta[s, 8:16, :] = jnp.concatenate(weight, axis=0)

    def gather(s, which):
        pick_s, gate = [], []
        for i, base, at, size in which:
            match = match_rows(s, i, base, size)
            pick_s.append(jnp.where(match, 1.0, 0.0).astype(BF16))
            gate.append(jnp.sum(jnp.where(match, meta[s, pl.ds(8 + i, 1), :], 0.0), axis=1, keepdims=True))
        pick_s, gate = jnp.concatenate(pick_s, axis=0), jnp.concatenate(gate, axis=0)
        at, size = which[0][2], pick_s.shape[0]
        rows_x[s, at:at + size, :] = dot_nn(pick_s, buf[s, 0:tok, :]).astype(BF16)
        rows_d[s, at:at + size, :] = (dot_nn(pick_s, buf[s, tok:2 * tok, :]) * gate).astype(BF16)

    def block(at, size, keep, w, g, g_in):
        w13, w2 = w_bufs[0].at[w], w_bufs[1].at[w]
        rows = n_src * size
        chunk = n_src if rows <= 4 * cap else 2
        for lo in range(0, n_src, chunk):
            m, at_c = chunk * size, lo * size
            x_c = rows_x[lo:lo + chunk, pl.ds(at, size), :].reshape(m, d_model)
            d_c = rows_d[lo:lo + chunk, pl.ds(at, size), :].reshape(m, d_model)
            ab = dot_nn(x_c, w13[...]).astype(BF16).astype(F32)
            dh = dot_nt(d_c, w2[...])
            a, b = ab[:, :d_ff], ab[:, d_ff:]
            sig = 0.5 * jnp.tanh(0.5 * a) + 0.5
            act = a * sig
            hid[at_c:at_c + m, :] = (act * b).astype(BF16)
            dab[at_c:at_c + m, 0:d_ff] = (dh * b * sig * (1.0 + a * (1.0 - sig))).astype(BF16)
            dab[at_c:at_c + m, d_ff:] = (dh * act).astype(BF16)
        xe = rows_x[:, pl.ds(at, size), :].reshape(rows, d_model)
        de = rows_d[:, pl.ds(at, size), :].reshape(rows, d_model)
        for out, lhs, rhs in ((g_bufs[0], xe, dab[0:rows, :]), (g_bufs[1], hid[0:rows, :], de)):
            if g_in:
                out[g] = out[g] + dot_tn(lhs, rhs)
            else:
                out[g] = dot_tn(lhs, rhs)
        if n_own:
            m = n_own * size
            o = dot_nn(hid[0:m, :], w2[...]).astype(BF16)
            dx = dot_nt(dab[0:m, :], w13[...]).astype(BF16)
            kept_o[:, pl.ds(keep, size), :] = o.reshape(n_own, size, d_model)
            kept_x[:, pl.ds(keep, size), :] = dx.reshape(n_own, size, d_model)

    for s in range(n_src):
        fetch(s).start()
    start(load_w(0))
    start(load_g(0))
    start(load_g(1))

    def wave(p, carry):
        for s in range(n_src):
            @pl.when(p == 0)
            def _(s=s):
                fetch(s).wait()
                ranks(s)
                gather(s, [(0, far, part, extra)])

        if n_src % 2:
            raise ValueError("pairs")

        def two(t, carry):
            for s in (2 * t, 2 * t + 1):
                gather(s, [(group * p + i, 0.0, i * cap, cap) for i in range(group)])
            return carry

        lax.fori_loop(0, n_src // 2, two, 0)

        def one(i, carry):
            e = group * p + i
            wait(load_w(e))

            @pl.when(e + 1 < n_loc)
            def _():
                start(load_w(e + 1))

            turn_slot(e + 2)
            wait(load_g(e))
            block(pl.multiple_of(i * cap, cap), cap, pl.multiple_of(e * cap, cap), lax.rem(e, 2), lax.rem(e, 4), not first)

            @pl.when(e == 0)
            def more():
                block(part, extra, cold, 0, 0, True)

            start(save_g(e))
            return carry

        lax.fori_loop(0, group, one, 0)
        return carry

    lax.fori_loop(0, n_loc // group, wave, 0)

    if n_own:
        pieces = [(i, 0.0, i * cap, cap) for i in range(n_loc)] + [(0, far, cold, extra)]

        def send_part(s):
            return pltpu.make_async_copy(g_bufs[0].at[s], parts[s], part_sem.at[s])

        def combine(src, carry):
            for i, base, at, size in pieces:
                match = match_rows(src, i, base, size)
                gate = meta[src, 8 + i:9 + i, :]
                hi = gate.astype(BF16).astype(F32)
                mid = (gate - hi).astype(BF16).astype(F32)
                low = gate - hi - mid
                pick[at:at + size, :] = jnp.where(match, 1.0, 0.0).astype(BF16)
                for k, v in enumerate((hi, mid, low)):
                    at_k = k * cold + at if at < cold else 3 * cold + k * extra
                    gpick[at_k:at_k + size, :] = jnp.where(match, v, 0.0).astype(BF16)
            o, last = kept_o[src, 0:cold, :], kept_o[src, cold:cold + extra, :]
            y = dot_tn(gpick[0:cold, :], o) + dot_tn(gpick[cold:2 * cold, :], o) + dot_tn(gpick[2 * cold:3 * cold, :], o)
            y = y + dot_tn(gpick[3 * cold:3 * cold + 3 * extra, :], jnp.concatenate([last] * 3, axis=0))
            dx = dot_tn(pick[...], kept_x[src])
            g_bufs[0][src, 0:tok, :] = y
            g_bufs[0][src, tok:2 * tok, :] = dx
            for s in range(n_own):
                @pl.when(src == s)
                def _(s=s):
                    send_part(s).start()
            return carry

        lax.fori_loop(0, n_own, combine, 0)
        wait([send_part(s) for s in range(n_own)])
    wait(save_g(n_loc - 2))
    wait(save_g(n_loc - 1))


def run_stage(lead, srcs, weights, acc, n_own, n_exp):
    w1, w3, w2 = weights
    n_loc, d_model, d_ff = w1.shape
    tok = (srcs[0].shape[0] - RG_ROWS) // 2
    n_src = len(srcs)
    cap, cap_hot = caps(tok, 8, n_exp)
    extra = cap_hot - cap
    first = acc is None
    group = 2 if n_own or n_src > 4 else 4
    cfg = dict(n_src=n_src, n_own=n_own, first=first, group=group, tok=tok, d_model=d_model, d_ff=d_ff, n_loc=n_loc, n_exp=n_exp,
               cap=cap, extra=extra)
    args = [lead, *srcs, w1, w3, w2]
    aliases = {}
    if not first:
        aliases = {len(args) + k: k for k in range(3)}
        args += list(acc)
    shapes = [jax.ShapeDtypeStruct((n_loc, d_model, d_ff), F32)] * 2 + [jax.ShapeDtypeStruct((n_loc, d_ff, d_model), F32)]
    shapes += [jax.ShapeDtypeStruct((2 * tok, d_model), F32)] * n_own
    rows = n_loc * cap + extra
    scratch = [pltpu.VMEM((n_src, group * cap + extra, d_model), BF16)] * 2 + [
        pltpu.VMEM((n_src, 16, tok), F32),
        pltpu.VMEM((n_src, 2 * tok + RG_ROWS, d_model), BF16),
        pltpu.VMEM((n_src * cap, d_ff), BF16),
        pltpu.VMEM((n_src * cap, 2 * d_ff), BF16),
    ]
    for slots, kind in ((2, BF16), (4, F32)):
        scratch += [pltpu.VMEM((slots, d_model, 2 * d_ff), kind), pltpu.VMEM((slots, d_ff, d_model), kind)]
    scratch += [pltpu.SemaphoreType.DMA(n) for n in ((n_src,), (2, 3), (4, 3), (4, 3))]
    if n_own:
        scratch += [pltpu.VMEM((n_own, rows, d_model), BF16)] * 2
        scratch += [pltpu.VMEM((rows, tok), BF16), pltpu.VMEM((3 * rows, tok), BF16), pltpu.SemaphoreType.DMA((n_own,))]
    unit = 2 * d_model * d_ff * rows
    return pl.pallas_call(
        functools.partial(stage_kernel, cfg),
        in_specs=[pl.BlockSpec(memory_space=pltpu.SMEM)] + [pl.BlockSpec(memory_space=pl.ANY)] * (len(args) - 1),
        out_specs=[pl.BlockSpec(memory_space=pl.ANY)] * len(shapes),
        out_shape=shapes,
        input_output_aliases=aliases,
        scratch_shapes=scratch,
        compiler_params=pltpu.CompilerParams(vmem_limit_bytes=67_000_000),
        cost_estimate=pl.CostEstimate(flops=unit * (8 * n_src + 7 * n_own) // 8, bytes_accessed=100 << 20, transcendentals=0),
    )(*args)


def solution(mesh):
    n_data, n_er = mesh.shape["data"], mesh.shape["expert"]
    row_spec = P(("pod", "data", "expert"), None)
    w_spec = P("expert", None, None)
    grad_spec = P(("pod", "expert"), None, None)
    partner = [(r, r ^ 1) for r in range(n_er)]
    across = [(r, r ^ 2) for r in range(n_er)]
    around = [(q, (q + 1) % n_data) for q in range(n_data)]

    def move(axis, pairs, value):
        return lax.ppermute(value, axis, pairs)

    def body(tokens, routes, gates, grad_y, w_in1, w_in3, w_out):
        n_exp = w_in1.shape[0] * n_er
        lead = lax.axis_index("expert").astype(jnp.int32).reshape(1, 1)
        gate = gates.T
        hi = lax.reduce_precision(gate, 8, 7)
        mid = lax.reduce_precision(gate - hi, 8, 7)
        low = gate - hi - mid
        rg = jnp.concatenate([jnp.concatenate([routes.T.astype(F32), hi], 0), jnp.concatenate([mid, low], 0)], 1)
        pack = jnp.concatenate([tokens, grad_y, rg.astype(BF16)], 0)

        def to_partner(v):
            return move("expert", partner, v)

        def to_across(v):
            return move("expert", across, v)

        def to_next(v):
            return move("data", around, v)

        def to_prev(v):
            return move("data", [(b, a) for a, b in around], v)

        gate_open = lax.optimization_barrier
        weights = (w_in1, w_in3, w_out)
        here, other, far, z1 = pack, to_partner(pack), to_across(pack), to_next(pack)
        *acc, own_a, send_a = run_stage(lead, [here, other], weights, None, 2, n_exp)
        far, z1, *acc = gate_open((far, z1, *acc))
        z1y, z2, z3y = to_across(z1), to_next(z1), to_prev(far)
        block = [far, to_partner(far), z1, to_partner(z1)]
        *acc, own_b, send_b = run_stage(lead, block, weights, acc, 2, n_exp)
        z1y, z2, send_a, send_b, *acc = gate_open((z1y, z2, send_a, send_b, *acc))
        z2y, z3 = to_across(z2), to_next(z2)
        got_a, got_b = to_partner(send_a), to_partner(send_b)
        block = [z1y, to_partner(z1y), z2, to_partner(z2)]
        acc = run_stage(lead, block, weights, acc, 0, n_exp)
        z2y, z3, z3y, got_a, got_b, *acc = gate_open((z2y, z3, z3y, got_a, got_b, *acc))
        back = to_across(own_b + got_b)
        block = [z2y, to_partner(z2y), z3, to_partner(z3), z3y, to_partner(z3y)]
        acc1, acc3, acc2 = run_stage(lead, block, weights, acc, 0, n_exp)
        tok = tokens.shape[0]
        y_out = (own_a[:tok] + got_a[:tok] + back[:tok]).astype(BF16)
        grad_x = (own_a[tok:] + got_a[tok:] + back[tok:]).astype(BF16)
        return y_out, grad_x, acc1, acc3, acc2

    return jax.shard_map(body, mesh=mesh,
                         in_specs=(row_spec, row_spec, row_spec, row_spec, w_spec, w_spec, w_spec),
                         out_specs=(row_spec, row_spec, grad_spec, grad_spec, grad_spec),
                         check_vma=False)
```

```python
import functools

import jax
import jax.numpy as jnp
from jax import lax
from jax.experimental import pallas as pl
from jax.experimental.pallas import tpu as pltpu
from jax.sharding import PartitionSpec as P

MESH = pl.DeviceIdType.MESH
BLOCKS = ("other", "far", "far_o", "z1", "z1_o", "z1y", "z1y_o", "z2", "z2_o", "z2y", "z2y_o", "z3", "z3_o", "z3y", "z3y_o")
N_HOT = 2
RG_ROWS = 16
F32, BF16 = jnp.float32, jnp.bfloat16


def caps(tok_dev, top_k, n_exp):
    cap_hot = 3 * tok_dev // 8
    cap_cold = max(8, ((tok_dev * top_k - N_HOT * cap_hot) // (n_exp - N_HOT) + 7) // 8 * 8)
    return cap_cold, cap_hot


def dot_nn(a, b):
    return lax.dot_general(a, b, (((1,), (0,)), ((), ())), preferred_element_type=F32)


def dot_nt(a, b):
    return lax.dot_general(a, b, (((1,), (1,)), ((), ())), preferred_element_type=F32)


def dot_tn(a, b):
    return lax.dot_general(a, b, (((0,), (0,)), ((), ())), preferred_element_type=F32)


def prefix(m):
    lane = lax.broadcasted_iota(jnp.int32, m.shape, 1)
    step = 1
    while step < m.shape[1]:
        m = m + jnp.where(lane >= step, pltpu.roll(m, step, 1), 0.0)
        step *= 2
    return m


class Engine:
    def __init__(self, cfg, lead, weights, bases, outs, scratch, group):
        self.__dict__.update(cfg)
        self.lead, self.weights, self.bases, self.outs, self.group = lead, weights, bases, outs, group
        (self.rows_x, self.rows_d, self.meta, self.buf, self.hid, self.dab, self.w13, self.w2, self.g13, self.g2,
         self.src_sem, self.w_sem, self.in_sem, self.out_sem) = scratch[:14]
        self.own_scratch = scratch[14:]
        hot = jnp.logical_or(lead * self.n_loc == 0, lead * self.n_loc == self.n_exp // 2)
        self.far = jnp.where(hot, float(self.cap), float(2 * self.tok))
        self.cold, self.part = self.n_loc * self.cap, group * self.cap

    def triple(self, both, single, slot):
        f = self.d_ff
        return both.at[slot, :, 0:f], both.at[slot, :, f:2 * f], single.at[slot]

    def load_w(self, e):
        slot = lax.rem(e, 2)
        return [pltpu.make_async_copy(w.at[e], b, self.w_sem.at[slot, k])
                for k, (w, b) in enumerate(zip(self.weights, self.triple(self.w13, self.w2, slot)))]

    def load_g(self, e):
        slot = lax.rem(e, 4)
        return [pltpu.make_async_copy(w.at[e], b, self.in_sem.at[slot, k])
                for k, (w, b) in enumerate(zip(self.bases, self.triple(self.g13, self.g2, slot)))]

    def save_g(self, e):
        slot = lax.rem(e, 4)
        return [pltpu.make_async_copy(b, w.at[e], self.out_sem.at[slot, k])
                for k, (w, b) in enumerate(zip(self.outs, self.triple(self.g13, self.g2, slot)))]

    def match_rows(self, src, i, base, size):
        iota = lax.broadcasted_iota(jnp.int32, (size, self.tok), 0).astype(F32) + base
        return iota == self.meta[src, pl.ds(i, 1), :]

    def ranks(self, s):
        tok = self.tok
        rg = self.buf[s, 2 * tok:2 * tok + RG_ROWS, :].astype(F32)
        routes = rg[0:8, :tok]
        gates = (rg[8:16, :tok] + rg[0:8, tok:]) + rg[8:16, tok:]
        member, weight = [], []
        for i in range(self.n_loc):
            match = routes == (self.lead * self.n_loc + i).astype(F32)
            member.append(jnp.sum(jnp.where(match, 1.0, 0.0), axis=0, keepdims=True))
            weight.append(jnp.sum(jnp.where(match, gates, 0.0), axis=0, keepdims=True))
        member = jnp.concatenate(member, axis=0)
        self.meta[s, 0:8, :] = jnp.where(member > 0.0, prefix(member) - 1.0, -1.0)
        self.meta[s, 8:16, :] = jnp.concatenate(weight, axis=0)

    def gather(self, s, which):
        tok, meta, buf = self.tok, self.meta, self.buf
        pick, gate = [], []
        for i, base, at, size in which:
            match = self.match_rows(s, i, base, size)
            pick.append(jnp.where(match, 1.0, 0.0).astype(BF16))
            gate.append(jnp.sum(jnp.where(match, meta[s, pl.ds(8 + i, 1), :], 0.0), axis=1, keepdims=True))
        pick, gate = jnp.concatenate(pick, axis=0), jnp.concatenate(gate, axis=0)
        at, size = which[0][2], pick.shape[0]
        self.rows_x[s, at:at + size, :] = dot_nn(pick, buf[s, 0:tok, :]).astype(BF16)
        self.rows_d[s, at:at + size, :] = (dot_nn(pick, buf[s, tok:2 * tok, :]) * gate).astype(BF16)

    def block(self, n_src, n_own, at, size, keep, w, g, g_in):
        d_model, d_ff, hid, dab = self.d_model, self.d_ff, self.hid, self.dab
        w13, w2 = self.w13.at[w], self.w2.at[w]
        rows = n_src * size
        chunk = n_src if rows <= 4 * self.cap else 2
        for lo in range(0, n_src, chunk):
            m, at_c = chunk * size, lo * size
            x_c = self.rows_x[lo:lo + chunk, pl.ds(at, size), :].reshape(m, d_model)
            d_c = self.rows_d[lo:lo + chunk, pl.ds(at, size), :].reshape(m, d_model)
            ab = dot_nn(x_c, w13[...]).astype(BF16).astype(F32)
            dh = dot_nt(d_c, w2[...])
            a, b = ab[:, :d_ff], ab[:, d_ff:]
            sig = 0.5 * jnp.tanh(0.5 * a) + 0.5
            act = a * sig
            hid[at_c:at_c + m, :] = (act * b).astype(BF16)
            dab[at_c:at_c + m, 0:d_ff] = (dh * b * sig * (1.0 + a * (1.0 - sig))).astype(BF16)
            dab[at_c:at_c + m, d_ff:] = (dh * act).astype(BF16)
        xe = self.rows_x[0:n_src, pl.ds(at, size), :].reshape(rows, d_model)
        de = self.rows_d[0:n_src, pl.ds(at, size), :].reshape(rows, d_model)
        for out, lhs, rhs in ((self.g13, xe, dab[0:rows, :]), (self.g2, hid[0:rows, :], de)):
            if g_in:
                out[g] = out[g] + dot_tn(lhs, rhs)
            else:
                out[g] = dot_tn(lhs, rhs)
        if n_own:
            kept_o, kept_x = self.own_scratch[:2]
            m = n_own * size
            o = dot_nn(hid[0:m, :], w2[...]).astype(BF16)
            dx = dot_nt(dab[0:m, :], w13[...]).astype(BF16)
            kept_o[:, pl.ds(keep, size), :] = o.reshape(n_own, size, d_model)
            kept_x[:, pl.ds(keep, size), :] = dx.reshape(n_own, size, d_model)

    def stage(self, srcs, order, n_own, first, last, before, held, events, ship):
        n_src, n_loc, cap, group = len(srcs), self.n_loc, self.cap, self.group
        fetch = [pltpu.make_async_copy(r, self.buf.at[s], self.src_sem.at[s]) for s, r in enumerate(srcs)]
        for s in order:
            before[s]()
            fetch[s].start()

        def wave(p, carry):
            for s in order:
                @pl.when(p == 0)
                def _(s=s):
                    fetch[s].wait()
                    self.ranks(s)
                    self.gather(s, [(0, self.far, self.part, self.extra)])

            def two(t, carry):
                for s in (2 * t, 2 * t + 1):
                    self.gather(s, [(group * p + i, 0.0, i * cap, cap) for i in range(group)])
                return carry

            lax.fori_loop(0, n_src // 2, two, 0)

            def one(i, carry):
                e = group * p + i
                wait(self.load_w(e))
                if last:
                    @pl.when(e + 1 < n_loc)
                    def _():
                        start(self.load_w(e + 1))
                else:
                    start(self.load_w(lax.rem(e + 1, n_loc)))

                @pl.when(e >= 2)
                def _():
                    wait(self.save_g(e - 2))

                for k, copies in enumerate(held):
                    @pl.when(e == k)
                    def _(copies=copies):
                        wait(copies)

                if first:
                    @pl.when(e + 2 >= n_loc)
                    def _():
                        start(self.load_g(e + 2 - n_loc))
                elif last:
                    @pl.when(e + 2 < n_loc)
                    def _():
                        start(self.load_g(e + 2))
                else:
                    start(self.load_g(lax.rem(e + 2, n_loc)))
                if not first:
                    wait(self.load_g(e))
                self.block(n_src, n_own, pl.multiple_of(i * cap, cap), cap, pl.multiple_of(e * cap, cap),
                           lax.rem(e, 2), lax.rem(e, 4), not first)

                @pl.when(e == 0)
                def more():
                    self.block(n_src, n_own, self.part, self.extra, self.cold, 0, 0, True)

                start(self.save_g(e))
                for k, event in events:
                    @pl.when(e == k)
                    def _(event=event):
                        event()
                return carry

            lax.fori_loop(0, group, one, 0)
            return carry

        lax.fori_loop(0, n_loc // group, wave, 0)
        if n_own or last:
            wait(self.save_g(n_loc - 2))
            wait(self.save_g(n_loc - 1))
        if n_own:
            self.combine(n_own, ship)

    def combine(self, n_own, ship):
        kept_o, kept_x, pick, gpick = self.own_scratch[:4]
        cold, extra, cap, tok = self.cold, self.extra, self.cap, self.tok
        pieces = [(i, 0.0, i * cap, cap) for i in range(self.n_loc)] + [(0, self.far, cold, extra)]

        def one(src, carry):
            for i, base, at, size in pieces:
                match = self.match_rows(src, i, base, size)
                gate = self.meta[src, 8 + i:9 + i, :]
                hi = gate.astype(BF16).astype(F32)
                mid = (gate - hi).astype(BF16).astype(F32)
                low = gate - hi - mid
                pick[at:at + size, :] = jnp.where(match, 1.0, 0.0).astype(BF16)
                for k, v in enumerate((hi, mid, low)):
                    at_k = k * cold + at if at < cold else 3 * cold + k * extra
                    gpick[at_k:at_k + size, :] = jnp.where(match, v, 0.0).astype(BF16)
            o, rest = kept_o[src, 0:cold, :], kept_o[src, cold:cold + extra, :]
            y = dot_tn(gpick[0:cold, :], o) + dot_tn(gpick[cold:2 * cold, :], o) + dot_tn(gpick[2 * cold:3 * cold, :], o)
            y = y + dot_tn(gpick[3 * cold:3 * cold + 3 * extra, :], jnp.concatenate([rest] * 3, axis=0))
            dx = dot_tn(pick[...], kept_x[src])
            self.g13[2 + src, 0:tok, :] = y
            self.g13[2 + src, tok:2 * tok, :] = dx
            for s in range(n_own):
                @pl.when(src == s)
                def _(s=s):
                    ship[s].start()
            return carry

        lax.fori_loop(0, n_own, one, 0)


def start(copies):
    for c in copies:
        c.start()


def wait(copies):
    for c in copies:
        c.wait()


def nothing():
    pass


def roam_kernel(cfg, lead_ref, pack, w1, w3, w2, g1, g3, g2, land, own_a, own_b, got_a, got_b, *scratch):
    send_sem, recv_sem, part_sem = scratch[-3:]
    eng = Engine(cfg, lead_ref[0, 0], (w1, w3, w2), (g1, g3, g2), (g1, g3, g2), scratch[:-3], 2)
    q, r = lax.axis_index("data"), lax.axis_index("expert")
    n_data, n_er = cfg["n_data"], cfg["n_er"]
    partner = {"expert": r + 1 - 2 * lax.rem(r, 2)}
    across = {"expert": lax.rem(r + n_er // 2, n_er)}
    znext = {"data": lax.rem(q + 1, n_data)}
    zprev = {"data": lax.rem(q + n_data - 1, n_data)}

    def at(name):
        return land.at[BLOCKS.index(name)]

    flights = []

    def remote(src, dst, device):
        k = len(flights)
        copy = pltpu.make_async_remote_copy(src_ref=src, dst_ref=dst, send_sem=send_sem.at[k], recv_sem=recv_sem.at[k],
                                            device_id=device, device_id_type=MESH)
        flights.append(copy)
        return copy

    tok = cfg["tok"]
    half, full = pl.ds(0, tok), pl.ds(tok, tok + RG_ROWS)
    c_other = remote(pack, at("other"), partner)
    c_far = remote(pack, at("far"), across)
    c_z1 = remote(pack, at("z1"), znext)
    c_far_o = remote(at("far"), at("far_o"), partner)
    c_z1_o = remote(at("z1"), at("z1_o"), partner)
    c_z1y = remote(at("z1"), at("z1y"), across)
    c_z2 = remote(at("z1"), at("z2"), znext)
    c_z1y_o = remote(at("z1y"), at("z1y_o"), partner)
    c_z2_o = remote(at("z2"), at("z2_o"), partner)
    c_z2y = remote(at("z2"), at("z2y"), across)
    c_z3 = remote(at("z2"), at("z3"), znext)
    c_z3y_z = remote(at("far").at[half], at("z3y").at[half], zprev)
    c_z3y_y = remote(at("z3").at[full], at("z3y").at[full], across)
    c_z2y_o = remote(at("z2y"), at("z2y_o"), partner)
    c_z3_o = remote(at("z3"), at("z3_o"), partner)
    c_z3y_o = remote(at("z3y"), at("z3y_o"), partner)
    c_got_a = remote(eng.g13.at[3], got_a, partner)
    c_got_b = remote(eng.g13.at[3], got_b, partner)
    keep_a = pltpu.make_async_copy(eng.g13.at[2], own_a, part_sem.at[0])
    keep_b = pltpu.make_async_copy(eng.g13.at[2], own_b, part_sem.at[1])

    barrier = pltpu.get_barrier_semaphore()
    for device in (partner, across, znext, zprev):
        pl.semaphore_signal(barrier, inc=1, device_id=device, device_id_type=MESH)
    pl.semaphore_wait(barrier, 4)

    class Sent:
        def __init__(self, copy):
            self.copy = copy

        def wait(self):
            self.copy.wait_send()

    def arrived(copies, then):
        def event():
            for c in copies:
                c.wait_recv()
            start(then)
        return event

    start([c_other, c_far, c_z1])
    start(eng.load_w(0))
    eng.stage([pack, at("other")], (0, 1), 2, True, False, [nothing, c_other.wait_recv], (), (), [keep_a, c_got_a])
    eng.stage([at("far"), at("far_o"), at("z1"), at("z1_o")], (0, 2, 1, 3), 2, False, False,
              [arrived([c_far], [c_far_o]), c_far_o.wait_recv, arrived([c_z1], [c_z1_o, c_z1y, c_z2]), c_z1_o.wait_recv],
              ([keep_a], [Sent(c_got_a)]),
              ((7, arrived([c_z1y, c_z2], [c_z1y_o, c_z2_o, c_z2y, c_z3, c_z3y_z])),),
              [keep_b, c_got_b])
    eng.stage([at("z1y"), at("z2"), at("z1y_o"), at("z2_o")], (0, 1, 2, 3), 0, False, True,
              [nothing, nothing, c_z1y_o.wait_recv, c_z2_o.wait_recv],
              ([keep_b], [Sent(c_got_b)]),
              ((5, arrived([c_z2y, c_z3], [c_z3y_y, c_z2y_o, c_z3_o])), (7, arrived([c_z3y_z, c_z3y_y], [c_z3y_o]))), ())
    for c in (c_got_a, c_got_b, c_z2y_o, c_z3_o, c_z3y_o):
        c.wait_recv()
    for c in flights:
        if c is not c_got_a and c is not c_got_b:
            c.wait_send()


def rest_kernel(cfg, lead_ref, land, w1, w3, w2, b1, b3, b2, g1, g3, g2, *scratch):
    eng = Engine(cfg, lead_ref[0, 0], (w1, w3, w2), (b1, b3, b2), (g1, g3, g2), scratch, 2)
    start(eng.load_w(0))
    start(eng.load_g(0))
    start(eng.load_g(1))
    names = ("z2y", "z2y_o", "z3", "z3_o", "z3y", "z3y_o")
    eng.stage([land.at[BLOCKS.index(n)] for n in names], range(6), 0, False, True, [nothing] * 6, (), (), ())


def call_kernel(name, kernel, cfg, args, shapes, n_src, n_own, extra_scratch, params):
    tok, d_model, d_ff, n_loc, cap, extra = (cfg[k] for k in ("tok", "d_model", "d_ff", "n_loc", "cap", "extra"))
    rows = n_loc * cap + extra
    scratch = [pltpu.VMEM((n_src, 2 * cap + extra, d_model), BF16)] * 2 + [
        pltpu.VMEM((n_src, 16, tok), F32),
        pltpu.VMEM((n_src, 2 * tok + RG_ROWS, d_model), BF16),
        pltpu.VMEM((n_src * cap, d_ff), BF16),
        pltpu.VMEM((n_src * cap, 2 * d_ff), BF16),
    ]
    for slots, kind in ((2, BF16), (4, F32)):
        scratch += [pltpu.VMEM((slots, d_model, 2 * d_ff), kind), pltpu.VMEM((slots, d_ff, d_model), kind)]
    scratch += [pltpu.SemaphoreType.DMA(n) for n in ((n_src,), (2, 3), (4, 3), (4, 3))]
    if n_own:
        scratch += [pltpu.VMEM((n_own, rows, d_model), BF16)] * 2
        scratch += [pltpu.VMEM((rows, tok), BF16), pltpu.VMEM((3 * rows, tok), BF16)]
    unit = 2 * d_model * d_ff * rows
    return pl.pallas_call(
        functools.partial(kernel, cfg),
        in_specs=[pl.BlockSpec(memory_space=pltpu.SMEM)] + [pl.BlockSpec(memory_space=pl.ANY)] * (len(args) - 1),
        out_specs=[pl.BlockSpec(memory_space=pl.ANY)] * len(shapes),
        out_shape=shapes,
        scratch_shapes=scratch + extra_scratch,
        compiler_params=pltpu.CompilerParams(vmem_limit_bytes=67_000_000, **params),
        cost_estimate=pl.CostEstimate(flops=unit * (8 * n_src + 7 * n_own) // 8, bytes_accessed=100 << 20, transcendentals=0),
        name=name,
    )(*args)


def solution(mesh):
    n_data, n_er = mesh.shape["data"], mesh.shape["expert"]
    row_spec = P(("pod", "data", "expert"), None)
    w_spec = P("expert", None, None)
    grad_spec = P(("pod", "expert"), None, None)
    across = [(r, r ^ 2) for r in range(n_er)]

    def body(tokens, routes, gates, grad_y, w_in1, w_in3, w_out):
        n_loc, d_model, d_ff = w_in1.shape
        n_exp, tok = n_loc * n_er, tokens.shape[0]
        cap, cap_hot = caps(tok, routes.shape[1], n_exp)
        cfg = dict(tok=tok, d_model=d_model, d_ff=d_ff, n_loc=n_loc, n_exp=n_exp, cap=cap, extra=cap_hot - cap,
                   n_data=n_data, n_er=n_er)
        lead = lax.axis_index("expert").astype(jnp.int32).reshape(1, 1)
        gate = gates.T
        hi = lax.reduce_precision(gate, 8, 7)
        mid = lax.reduce_precision(gate - hi, 8, 7)
        low = gate - hi - mid
        rg = jnp.concatenate([jnp.concatenate([routes.T.astype(F32), hi], 0), jnp.concatenate([mid, low], 0)], 1)
        pack = jnp.concatenate([tokens, grad_y, rg.astype(BF16)], 0)
        weights = (w_in1, w_in3, w_out)
        grads = [jax.ShapeDtypeStruct(w.shape, F32) for w in weights]
        sums = [jax.ShapeDtypeStruct((2 * tok, d_model), F32)] * 4
        n_fly = 18
        land = jax.ShapeDtypeStruct((len(BLOCKS), *pack.shape), BF16)
        *acc, land, own_a, own_b, got_a, got_b = call_kernel(
            "roam", roam_kernel, cfg, [lead, pack, *weights], [*grads, land, *sums], 4, 2,
            [pltpu.SemaphoreType.DMA((n_fly,)), pltpu.SemaphoreType.DMA((n_fly,)), pltpu.SemaphoreType.DMA((2,))],
            dict(collective_id=0, has_side_effects=True))
        back = lax.ppermute(own_b + got_b, "expert", across)
        acc1, acc3, acc2 = call_kernel("rest", rest_kernel, cfg, [lead, land, *weights, *acc], grads, 6, 0, [], {})
        y_out = (own_a[:tok] + got_a[:tok] + back[:tok]).astype(BF16)
        grad_x = (own_a[tok:] + got_a[tok:] + back[tok:]).astype(BF16)
        return y_out, grad_x, acc1, acc3, acc2

    return jax.shard_map(body, mesh=mesh,
                         in_specs=(row_spec, row_spec, row_spec, row_spec, w_spec, w_spec, w_spec),
                         out_specs=(row_spec, row_spec, grad_spec, grad_spec, grad_spec),
                         check_vma=False)
```

```python
import functools

import jax
import jax.numpy as jnp
from jax import lax
from jax.experimental import pallas as pl
from jax.experimental.pallas import tpu as pltpu
from jax.sharding import PartitionSpec as P

MESH = pl.DeviceIdType.MESH
BLOCKS = ("other", "far", "far_o", "z1", "z1_o", "z1y", "z1y_o", "z2", "z2_o", "z2y", "z2y_o", "z3", "z3_o", "z3y", "z3y_o")
N_HOT = 2
RG_ROWS = 16
F32, BF16 = jnp.float32, jnp.bfloat16


def caps(tok_dev, top_k, n_exp):
    cap_hot = 3 * tok_dev // 8
    cap_cold = max(8, ((tok_dev * top_k - N_HOT * cap_hot) // (n_exp - N_HOT) + 7) // 8 * 8)
    return cap_cold, cap_hot


def dot_nn(a, b):
    return lax.dot_general(a, b, (((1,), (0,)), ((), ())), preferred_element_type=F32)


def dot_nt(a, b):
    return lax.dot_general(a, b, (((1,), (1,)), ((), ())), preferred_element_type=F32)


def dot_tn(a, b):
    return lax.dot_general(a, b, (((0,), (0,)), ((), ())), preferred_element_type=F32)


def prefix(m):
    lane = lax.broadcasted_iota(jnp.int32, m.shape, 1)
    step = 1
    while step < m.shape[1]:
        m = m + jnp.where(lane >= step, pltpu.roll(m, step, 1), 0.0)
        step *= 2
    return m


class Engine:
    def __init__(self, cfg, lead, weights, bases, outs, scratch, group):
        self.__dict__.update(cfg)
        self.lead, self.weights, self.bases, self.outs, self.group = lead, weights, bases, outs, group
        (self.rows_x, self.rows_d, self.meta, self.buf, self.hid, self.dab, self.w13, self.w2, self.g13, self.g2,
         self.src_sem, self.w_sem, self.in_sem, self.out_sem) = scratch[:14]
        self.own_scratch = scratch[14:]
        hot = jnp.logical_or(lead * self.n_loc == 0, lead * self.n_loc == self.n_exp // 2)
        self.far = jnp.where(hot, float(self.cap), float(2 * self.tok))
        self.cold, self.part = self.n_loc * self.cap, group * self.cap

    def triple(self, both, single, slot):
        f = self.d_ff
        return both.at[slot, :, 0:f], both.at[slot, :, f:2 * f], single.at[slot]

    def load_w(self, e):
        slot = lax.rem(e, 2)
        return [pltpu.make_async_copy(w.at[e], b, self.w_sem.at[slot, k])
                for k, (w, b) in enumerate(zip(self.weights, self.triple(self.w13, self.w2, slot)))]

    def load_g(self, e):
        slot = lax.rem(e, 4)
        return [pltpu.make_async_copy(w.at[e], b, self.in_sem.at[slot, k])
                for k, (w, b) in enumerate(zip(self.bases, self.triple(self.g13, self.g2, slot)))]

    def save_g(self, e):
        slot = lax.rem(e, 4)
        return [pltpu.make_async_copy(b, w.at[e], self.out_sem.at[slot, k])
                for k, (w, b) in enumerate(zip(self.outs, self.triple(self.g13, self.g2, slot)))]

    def fetches(self, s, ref):
        if not isinstance(ref, tuple):
            return [pltpu.make_async_copy(ref, self.buf.at[s], self.src_sem.at[s, 0])]
        dst = self.buf.at[s]
        return [pltpu.make_async_copy(r, dst.at[pl.ds(at, r.shape[0])], self.src_sem.at[s, k])
                for k, (r, at) in enumerate(zip(ref, (0, self.tok, 2 * self.tok)))]

    def match_rows(self, src, i, base, size):
        iota = lax.broadcasted_iota(jnp.int32, (size, self.tok), 0).astype(F32) + base
        return iota == self.meta[src, pl.ds(i, 1), :]

    def ranks(self, s):
        tok = self.tok
        rg = self.buf[s, 2 * tok:2 * tok + RG_ROWS, :].astype(F32)
        routes = rg[0:8, :tok]
        gates = (rg[8:16, :tok] + rg[0:8, tok:]) + rg[8:16, tok:]
        member, weight = [], []
        for i in range(self.n_loc):
            match = routes == (self.lead * self.n_loc + i).astype(F32)
            member.append(jnp.sum(jnp.where(match, 1.0, 0.0), axis=0, keepdims=True))
            weight.append(jnp.sum(jnp.where(match, gates, 0.0), axis=0, keepdims=True))
        member = jnp.concatenate(member, axis=0)
        self.meta[s, 0:8, :] = jnp.where(member > 0.0, prefix(member) - 1.0, -1.0)
        self.meta[s, 8:16, :] = jnp.concatenate(weight, axis=0)

    def gather(self, s, which):
        tok, meta, buf = self.tok, self.meta, self.buf
        pick, gate = [], []
        for i, base, at, size in which:
            match = self.match_rows(s, i, base, size)
            pick.append(jnp.where(match, 1.0, 0.0).astype(BF16))
            gate.append(jnp.sum(jnp.where(match, meta[s, pl.ds(8 + i, 1), :], 0.0), axis=1, keepdims=True))
        pick, gate = jnp.concatenate(pick, axis=0), jnp.concatenate(gate, axis=0)
        at, size = which[0][2], pick.shape[0]
        self.rows_x[s, at:at + size, :] = dot_nn(pick, buf[s, 0:tok, :]).astype(BF16)
        self.rows_d[s, at:at + size, :] = (dot_nn(pick, buf[s, tok:2 * tok, :]) * gate).astype(BF16)

    def block(self, n_src, n_own, at, size, keep, w, g, g_in):
        d_model, d_ff, hid, dab = self.d_model, self.d_ff, self.hid, self.dab
        w13, w2 = self.w13.at[w], self.w2.at[w]
        rows = n_src * size

        def load(ref):
            return ref[0:n_src, pl.ds(at, size), :].reshape(rows, d_model)

        ab = dot_nn(load(self.rows_x), w13[...]).astype(BF16).astype(F32)
        dh = dot_nt(load(self.rows_d), w2[...])
        a, b = ab[:, :d_ff], ab[:, d_ff:]
        sig = 0.5 * jnp.tanh(0.5 * a) + 0.5
        act = a * sig
        hid[0:rows, :] = (act * b).astype(BF16)
        dab[0:rows, 0:d_ff] = (dh * b * sig * (1.0 + a * (1.0 - sig))).astype(BF16)
        dab[0:rows, d_ff:] = (dh * act).astype(BF16)
        for out, lhs, rhs in ((self.g13, load(self.rows_x), dab[0:rows, :]), (self.g2, hid[0:rows, :], load(self.rows_d))):
            if g_in:
                out[g] = out[g] + dot_tn(lhs, rhs)
            else:
                out[g] = dot_tn(lhs, rhs)
        if n_own:
            kept_o, kept_x = self.own_scratch[:2]
            m = n_own * size
            o = dot_nn(hid[0:m, :], w2[...]).astype(BF16)
            dx = dot_nt(dab[0:m, :], w13[...]).astype(BF16)
            kept_o[:, pl.ds(keep, size), :] = o.reshape(n_own, size, d_model)
            kept_x[:, pl.ds(keep, size), :] = dx.reshape(n_own, size, d_model)

    def stage(self, srcs, order, n_own, first, last, before, held, events, ship, each=None):
        n_src, n_loc, cap, group = len(srcs), self.n_loc, self.cap, self.group
        fetch = [self.fetches(s, r) for s, r in enumerate(srcs)]
        for s in order:
            before[s]()
            start(fetch[s])

        def wave(p, carry):
            for s in order:
                @pl.when(p == 0)
                def _(s=s):
                    wait(fetch[s])
                    self.ranks(s)
                    self.gather(s, [(0, self.far, self.part, self.extra)])

            def two(t, carry):
                for s in (2 * t, 2 * t + 1):
                    self.gather(s, [(group * p + i, 0.0, i * cap, cap) for i in range(group)])
                return carry

            lax.fori_loop(0, n_src // 2, two, 0)

            def one(i, carry):
                e = group * p + i
                wait(self.load_w(e))
                if last:
                    @pl.when(e + 1 < n_loc)
                    def _():
                        start(self.load_w(e + 1))
                else:
                    start(self.load_w(lax.rem(e + 1, n_loc)))

                @pl.when(e >= 2)
                def _():
                    wait(self.save_g(e - 2))

                for k, copies in enumerate(held):
                    @pl.when(e == k)
                    def _(copies=copies):
                        wait(copies)

                if first:
                    @pl.when(e + 2 >= n_loc)
                    def _():
                        start(self.load_g(e + 2 - n_loc))
                elif last:
                    @pl.when(e + 2 < n_loc)
                    def _():
                        start(self.load_g(e + 2))
                else:
                    start(self.load_g(lax.rem(e + 2, n_loc)))
                if not first:
                    wait(self.load_g(e))
                self.block(n_src, n_own, pl.multiple_of(i * cap, cap), cap, pl.multiple_of(e * cap, cap),
                           lax.rem(e, 2), lax.rem(e, 4), not first)

                @pl.when(e == 0)
                def more():
                    self.block(n_src, n_own, self.part, self.extra, self.cold, 0, 0, True)

                start(self.save_g(e))
                for k, event in events:
                    @pl.when(e == k)
                    def _(event=event):
                        event()
                if each is not None:
                    each(e)
                return carry

            lax.fori_loop(0, group, one, 0)
            return carry

        lax.fori_loop(0, n_loc // group, wave, 0)
        if n_own or last:
            wait(self.save_g(n_loc - 2))
            wait(self.save_g(n_loc - 1))
        if n_own:
            self.combine(n_own, ship)

    def combine(self, n_own, ship):
        kept_o, kept_x = self.own_scratch[:2]
        cold, extra, cap, tok, n_loc = self.cold, self.extra, self.cap, self.tok, self.n_loc
        part, n_blk = self.part, n_loc // self.group
        pieces = [(i, 0.0, i // self.group, i % self.group * cap, cap) for i in range(n_loc)] + [(0, self.far, None, part, extra)]
        places = [(ref, pl.ds(lane * tok, tok)) for ref in (self.rows_x, self.rows_d) for lane in (0, 1)]

        def one(src, carry):
            for i, base, blk, at, size in pieces:
                match = self.match_rows(src, i, base, size)
                gate = self.meta[src, 8 + i:9 + i, :]
                hi = gate.astype(BF16).astype(F32)
                mid = (gate - hi).astype(BF16).astype(F32)
                low = gate - hi - mid
                for k, v in enumerate((hi, mid, low, 1.0)):
                    ref, lanes = places[0 if blk is None else k]
                    ref[k if blk is None else blk, at:at + size, lanes] = jnp.where(match, v, 0.0).astype(BF16)

            def chosen(k):
                ref, lanes = places[k]
                return ref[0:n_blk, 0:part, lanes].reshape(cold, tok)

            spare, lanes = places[0]
            o, rest = kept_o[src, 0:cold, :], kept_o[src, cold:cold + extra, :]
            y = dot_tn(chosen(0), o) + dot_tn(chosen(1), o) + dot_tn(chosen(2), o)
            y = y + dot_tn(spare[0:3, part:part + extra, lanes].reshape(3 * extra, tok), jnp.concatenate([rest] * 3, axis=0))
            dx = dot_tn(chosen(3), kept_x[src, 0:cold, :]) + dot_tn(spare[3, part:part + extra, lanes], kept_x[src, cold:cold + extra, :])
            self.g13[2 + src, 0:tok, :] = y
            self.g13[2 + src, tok:2 * tok, :] = dx
            for s in range(n_own):
                @pl.when(src == s)
                def _(s=s):
                    ship[s].start()
            return carry

        lax.fori_loop(0, n_own, one, 0)


def start(copies):
    for c in copies:
        c.start()


def wait(copies):
    for c in copies:
        c.wait()


def nothing():
    pass


class Adder:
    def __init__(self, a, b, out, held, load_sem, save_sem, ready):
        self.a, self.b, self.out, self.held, self.load_sem, self.save_sem, self.ready = a, b, out, held, load_sem, save_sem, ready
        self.rows = held.shape[2]

    def loads(self, k):
        slot, at = lax.rem(k, 2), pl.ds(pl.multiple_of(k * self.rows, self.rows), self.rows)
        return [pltpu.make_async_copy(v.at[at], self.held.at[slot, n], self.load_sem.at[slot, n]) for n, v in enumerate((self.a, self.b))]

    def save(self, k):
        slot, at = lax.rem(k, 2), pl.ds(pl.multiple_of(k * self.rows, self.rows), self.rows)
        return pltpu.make_async_copy(self.held.at[slot, 0], self.out.at[at], self.save_sem.at[slot])

    def add(self, k):
        wait(self.loads(k))
        slot = lax.rem(k, 2)
        self.held[slot, 0] = self.held[slot, 0] + self.held[slot, 1]
        self.save(k).start()

    def __call__(self, e):
        @pl.when(e == 0)
        def _():
            self.ready()

        @pl.when(e >= 1)
        def _():
            self.add(e - 1)

        @pl.when(e >= 2)
        def _():
            self.save(e - 2).wait()

        start(self.loads(e))

    def finish(self, last):
        self.add(last)
        self.save(last - 1).wait()
        self.save(last).wait()


def roam_kernel(cfg, lead_ref, tokens, grad_y, rg, w1, w3, w2, g1, g3, g2, land, own_a, own_b, got_a, got_b, mine, chip, *scratch):
    send_sem, recv_sem, part_sem, held, add_in_sem, add_out_sem = scratch[-6:]
    eng = Engine(cfg, lead_ref[0, 0], (w1, w3, w2), (g1, g3, g2), (g1, g3, g2), scratch[:-6], 2)
    q, r = lax.axis_index("data"), lax.axis_index("expert")
    n_data, n_er, tok, n_loc = cfg["n_data"], cfg["n_er"], cfg["tok"], cfg["n_loc"]
    partner = {"expert": r + 1 - 2 * lax.rem(r, 2)}
    across = {"expert": lax.rem(r + n_er // 2, n_er)}
    znext = {"data": lax.rem(q + 1, n_data)}
    zprev = {"data": lax.rem(q + n_data - 1, n_data)}

    def at(name, rows=None):
        ref = land.at[BLOCKS.index(name)]
        return ref if rows is None else ref.at[rows]

    flights = []

    def remote(src, dst, device):
        k = len(flights)
        copy = pltpu.make_async_remote_copy(src_ref=src, dst_ref=dst, send_sem=send_sem.at[k], recv_sem=recv_sem.at[k],
                                            device_id=device, device_id_type=MESH)
        flights.append(copy)
        return copy

    def first(name, device):
        parts = ((tokens, 0, tok), (grad_y, tok, tok), (rg, 2 * tok, RG_ROWS))
        return [remote(v, at(name, pl.ds(lo, n)), device) for v, lo, n in parts]

    def onward(src, dst, device):
        return [remote(at(src), at(dst), device)]

    upper, lower = pl.ds(0, tok), pl.ds(tok, tok + RG_ROWS)
    c_other, c_far, c_z1 = first("other", partner), first("far", across), first("z1", znext)
    c_far_o, c_z1_o = onward("far", "far_o", partner), onward("z1", "z1_o", partner)
    c_z1y, c_z2 = onward("z1", "z1y", across), onward("z1", "z2", znext)
    c_z1y_o, c_z2_o = onward("z1y", "z1y_o", partner), onward("z2", "z2_o", partner)
    c_z2y, c_z3 = onward("z2", "z2y", across), onward("z2", "z3", znext)
    c_z2y_o, c_z3_o = onward("z2y", "z2y_o", partner), onward("z3", "z3_o", partner)
    c_z3y_z = [remote(at("far", upper), at("z3y", upper), zprev)]
    c_z3y_y = [remote(at("z3", lower), at("z3y", lower), across)]
    c_z3y_zo = [remote(at("z3y", upper), at("z3y_o", upper), partner)]
    c_z3y_yo = [remote(at("z3y", lower), at("z3y_o", lower), partner)]
    c_got_a, c_got_b = [remote(eng.g13.at[3], got_a, partner)], [remote(eng.g13.at[3], got_b, partner)]
    keep_a = pltpu.make_async_copy(eng.g13.at[2], own_a, part_sem.at[0])
    keep_b = pltpu.make_async_copy(eng.g13.at[2], own_b, part_sem.at[1])

    barrier = pltpu.get_barrier_semaphore()
    for device in (partner, across, znext, zprev):
        pl.semaphore_signal(barrier, inc=1, device_id=device, device_id_type=MESH)
    pl.semaphore_wait(barrier, 4)

    class Sent:
        def __init__(self, copy):
            self.copy = copy

        def wait(self):
            self.copy.wait_send()

    def arrived(copies, then=()):
        def event():
            for c in copies:
                c.wait_recv()
            start(then)
        return event

    start(c_other + c_far + c_z1)
    start(eng.load_w(0))
    eng.stage([(tokens, grad_y, rg), at("other")], (0, 1), 2, True, False, [nothing, arrived(c_other)], (), (), [keep_a, c_got_a[0]])
    sum_a = Adder(own_a, got_a, mine, held, add_in_sem, add_out_sem, arrived(c_got_a))
    eng.stage([at("far"), at("far_o"), at("z1"), at("z1_o")], (0, 2, 1, 3), 2, False, False,
              [arrived(c_far, c_far_o), arrived(c_far_o), arrived(c_z1, c_z1_o + c_z1y + c_z2), arrived(c_z1_o)],
              ([keep_a], [Sent(c_got_a[0])]),
              ((6, arrived(c_z1y + c_z2, c_z2y + c_z3 + c_z3y_z + c_z1y_o + c_z2_o)),),
              [keep_b, c_got_b[0]], sum_a)
    sum_a.finish(n_loc - 1)
    sum_b = Adder(own_b, got_b, chip, held, add_in_sem, add_out_sem, arrived(c_got_b))
    eng.stage([at("z1y"), at("z2"), at("z1y_o"), at("z2_o")], (0, 1, 2, 3), 0, False, True,
              [nothing, nothing, arrived(c_z1y_o), arrived(c_z2_o)],
              ([keep_b], [Sent(c_got_b[0])]),
              ((3, arrived(c_z2y + c_z3, c_z3y_y + c_z2y_o + c_z3_o)), (6, arrived(c_z3y_z, c_z3y_zo))), (), sum_b)
    arrived(c_z3y_y, c_z3y_yo)()
    sum_b.finish(n_loc - 1)
    arrived(c_z2y_o + c_z3_o + c_z3y_zo + c_z3y_yo)()
    for c in flights:
        if c is not c_got_a[0] and c is not c_got_b[0]:
            c.wait_send()


def rest_kernel(cfg, lead_ref, land, w1, w3, w2, b1, b3, b2, g1, g3, g2, *scratch):
    eng = Engine(cfg, lead_ref[0, 0], (w1, w3, w2), (b1, b3, b2), (g1, g3, g2), scratch, 2)
    start(eng.load_w(0))
    start(eng.load_g(0))
    start(eng.load_g(1))
    names = ("z2y", "z2y_o", "z3", "z3_o", "z3y", "z3y_o")
    eng.stage([land.at[BLOCKS.index(n)] for n in names], range(6), 0, False, True, [nothing] * 6, (), (), ())


def call_kernel(name, kernel, cfg, args, shapes, n_src, n_own, extra_scratch, params):
    tok, d_model, d_ff, n_loc, cap, extra = (cfg[k] for k in ("tok", "d_model", "d_ff", "n_loc", "cap", "extra"))
    rows = n_loc * cap + extra
    scratch = [pltpu.VMEM((n_src, 2 * cap + extra, d_model), BF16)] * 2 + [
        pltpu.VMEM((n_src, 16, tok), F32),
        pltpu.VMEM((n_src, 2 * tok + RG_ROWS, d_model), BF16),
        pltpu.VMEM((n_src * cap, d_ff), BF16),
        pltpu.VMEM((n_src * cap, 2 * d_ff), BF16),
    ]
    for slots, kind in ((2, BF16), (4, F32)):
        scratch += [pltpu.VMEM((slots, d_model, 2 * d_ff), kind), pltpu.VMEM((slots, d_ff, d_model), kind)]
    scratch += [pltpu.SemaphoreType.DMA(n) for n in ((n_src, 3), (2, 3), (4, 3), (4, 3))]
    if n_own:
        scratch += [pltpu.VMEM((n_own, rows, d_model), BF16)] * 2
    unit = 2 * d_model * d_ff * rows
    return pl.pallas_call(
        functools.partial(kernel, cfg),
        in_specs=[pl.BlockSpec(memory_space=pltpu.SMEM)] + [pl.BlockSpec(memory_space=pl.ANY)] * (len(args) - 1),
        out_specs=[pl.BlockSpec(memory_space=pl.ANY)] * len(shapes),
        out_shape=shapes,
        scratch_shapes=scratch + extra_scratch,
        compiler_params=pltpu.CompilerParams(vmem_limit_bytes=67_000_000, **params),
        cost_estimate=pl.CostEstimate(flops=unit * (8 * n_src + 7 * n_own) // 8, bytes_accessed=100 << 20, transcendentals=0),
        name=name,
    )(*args)


def solution(mesh):
    n_data, n_er = mesh.shape["data"], mesh.shape["expert"]
    row_spec = P(("pod", "data", "expert"), None)
    w_spec = P("expert", None, None)
    grad_spec = P(("pod", "expert"), None, None)
    across = [(r, r ^ 2) for r in range(n_er)]

    def body(tokens, routes, gates, grad_y, w_in1, w_in3, w_out):
        n_loc, d_model, d_ff = w_in1.shape
        n_exp, tok = n_loc * n_er, tokens.shape[0]
        cap, cap_hot = caps(tok, routes.shape[1], n_exp)
        cfg = dict(tok=tok, d_model=d_model, d_ff=d_ff, n_loc=n_loc, n_exp=n_exp, cap=cap, extra=cap_hot - cap,
                   n_data=n_data, n_er=n_er)
        lead = lax.axis_index("expert").astype(jnp.int32).reshape(1, 1)
        gate = gates.T
        hi = lax.reduce_precision(gate, 8, 7)
        mid = lax.reduce_precision(gate - hi, 8, 7)
        low = gate - hi - mid
        rg = jnp.concatenate([jnp.concatenate([routes.T.astype(F32), hi], 0), jnp.concatenate([mid, low], 0)], 1).astype(BF16)
        weights = (w_in1, w_in3, w_out)
        grads = [jax.ShapeDtypeStruct(w.shape, F32) for w in weights]
        sums = [jax.ShapeDtypeStruct((2 * tok, d_model), F32)] * 6
        land = jax.ShapeDtypeStruct((len(BLOCKS), 2 * tok + RG_ROWS, d_model), BF16)
        dma, n_fly = pltpu.SemaphoreType.DMA, 27
        *acc, land, _, _, _, _, mine, chip = call_kernel(
            "roam", roam_kernel, cfg, [lead, tokens, grad_y, rg, *weights], [*grads, land, *sums], 4, 2,
            [dma((n_fly,)), dma((n_fly,)), dma((2,)), pltpu.VMEM((2, 2, 2 * tok // n_loc, d_model), F32), dma((2, 2)), dma((2,))],
            dict(collective_id=0, has_side_effects=True))
        back = lax.ppermute(chip, "expert", across)
        acc1, acc3, acc2 = call_kernel("rest", rest_kernel, cfg, [lead, land, *weights, *acc], grads, 6, 0, [], {})
        y_out = (mine[:tok] + back[:tok]).astype(BF16)
        grad_x = (mine[tok:] + back[tok:]).astype(BF16)
        return y_out, grad_x, acc1, acc3, acc2

    return jax.shard_map(body, mesh=mesh,
                         in_specs=(row_spec, row_spec, row_spec, row_spec, w_spec, w_spec, w_spec),
                         out_specs=(row_spec, row_spec, grad_spec, grad_spec, grad_spec),
                         check_vma=False)
```

```python
import functools

import jax
import jax.numpy as jnp
from jax import lax
from jax.experimental import pallas as pl
from jax.experimental.pallas import tpu as pltpu
from jax.sharding import PartitionSpec as P

MESH = pl.DeviceIdType.MESH
BLOCKS = ("other", "far", "far_o", "z1", "z1_o", "z1y", "z1y_o", "z2", "z2_o", "z2y", "z2y_o", "z3", "z3_o", "z3y", "z3y_o")
N_HOT = 2
RG_ROWS = 16
F32, BF16 = jnp.float32, jnp.bfloat16


def caps(tok_dev, top_k, n_exp):
    cap_hot = 3 * tok_dev // 8
    cap_cold = max(8, ((tok_dev * top_k - N_HOT * cap_hot) // (n_exp - N_HOT) + 7) // 8 * 8)
    return cap_cold, cap_hot


def dot_nn(a, b):
    return lax.dot_general(a, b, (((1,), (0,)), ((), ())), preferred_element_type=F32)


def dot_nt(a, b):
    return lax.dot_general(a, b, (((1,), (1,)), ((), ())), preferred_element_type=F32)


def dot_tn(a, b):
    return lax.dot_general(a, b, (((0,), (0,)), ((), ())), preferred_element_type=F32)


def prefix(m):
    lane = lax.broadcasted_iota(jnp.int32, m.shape, 1)
    step = 1
    while step < m.shape[1]:
        m = m + jnp.where(lane >= step, pltpu.roll(m, step, 1), 0.0)
        step *= 2
    return m


class Engine:
    def __init__(self, cfg, lead, weights, bases, outs, scratch, group):
        self.__dict__.update(cfg)
        self.lead, self.weights, self.bases, self.outs, self.group = lead, weights, bases, outs, group
        (self.rows_x, self.rows_d, self.meta, self.buf, self.hid, self.dab, self.w13, self.w2, self.g13, self.g2,
         self.src_sem, self.w_sem, self.in_sem, self.out_sem) = scratch[:14]
        self.own_scratch = scratch[14:]
        hot = jnp.logical_or(lead * self.n_loc == 0, lead * self.n_loc == self.n_exp // 2)
        self.far = jnp.where(hot, float(self.cap), float(2 * self.tok))
        self.cold, self.part = self.n_loc * self.cap, group * self.cap

    def triple(self, both, single, slot):
        f = self.d_ff
        return both.at[slot, :, 0:f], both.at[slot, :, f:2 * f], single.at[slot]

    def load_w(self, e):
        slot = lax.rem(e, 2)
        return [pltpu.make_async_copy(w.at[e], b, self.w_sem.at[slot, k])
                for k, (w, b) in enumerate(zip(self.weights, self.triple(self.w13, self.w2, slot)))]

    def load_g(self, e):
        slot = lax.rem(e, 4)
        return [pltpu.make_async_copy(w.at[e], b, self.in_sem.at[slot, k])
                for k, (w, b) in enumerate(zip(self.bases, self.triple(self.g13, self.g2, slot)))]

    def save_g(self, e):
        slot = lax.rem(e, 4)
        return [pltpu.make_async_copy(b, w.at[e], self.out_sem.at[slot, k])
                for k, (w, b) in enumerate(zip(self.outs, self.triple(self.g13, self.g2, slot)))]

    def fetches(self, s, ref):
        if not isinstance(ref, tuple):
            return [pltpu.make_async_copy(ref, self.buf.at[s], self.src_sem.at[s, 0])]
        dst = self.buf.at[s]
        return [pltpu.make_async_copy(r, dst.at[pl.ds(at, r.shape[0])], self.src_sem.at[s, k])
                for k, (r, at) in enumerate(zip(ref, (0, self.tok, 2 * self.tok)))]

    def match_rows(self, src, i, base, size):
        iota = lax.broadcasted_iota(jnp.int32, (size, self.tok), 0).astype(F32) + base
        return iota == self.meta[src, pl.ds(i, 1), :]

    def ranks(self, s):
        tok = self.tok
        rg = self.buf[s, 2 * tok:2 * tok + RG_ROWS, :].astype(F32)
        routes = rg[0:8, :tok]
        gates = (rg[8:16, :tok] + rg[0:8, tok:]) + rg[8:16, tok:]
        member, weight = [], []
        for i in range(self.n_loc):
            match = routes == (self.lead * self.n_loc + i).astype(F32)
            member.append(jnp.sum(jnp.where(match, 1.0, 0.0), axis=0, keepdims=True))
            weight.append(jnp.sum(jnp.where(match, gates, 0.0), axis=0, keepdims=True))
        member = jnp.concatenate(member, axis=0)
        self.meta[s, 0:8, :] = jnp.where(member > 0.0, prefix(member) - 1.0, -1.0)
        self.meta[s, 8:16, :] = jnp.concatenate(weight, axis=0)

    def gather(self, s, which):
        tok, meta, buf = self.tok, self.meta, self.buf
        pick, gate = [], []
        for i, base, at, size in which:
            match = self.match_rows(s, i, base, size)
            pick.append(jnp.where(match, 1.0, 0.0).astype(BF16))
            gate.append(jnp.sum(jnp.where(match, meta[s, pl.ds(8 + i, 1), :], 0.0), axis=1, keepdims=True))
        pick, gate = jnp.concatenate(pick, axis=0), jnp.concatenate(gate, axis=0)
        at, size = which[0][2], pick.shape[0]
        self.rows_x[s, at:at + size, :] = dot_nn(pick, buf[s, 0:tok, :]).astype(BF16)
        self.rows_d[s, at:at + size, :] = (dot_nn(pick, buf[s, tok:2 * tok, :]) * gate).astype(BF16)

    def block(self, n_src, n_own, at, size, keep, w, g, g_in):
        d_model, d_ff, hid, dab = self.d_model, self.d_ff, self.hid, self.dab
        w13, w2 = self.w13.at[w], self.w2.at[w]
        rows = n_src * size

        def load(ref):
            return ref[0:n_src, pl.ds(at, size), :].reshape(rows, d_model)

        ab = dot_nn(load(self.rows_x), w13[...]).astype(BF16).astype(F32)
        dh = dot_nt(load(self.rows_d), w2[...])
        a, b = ab[:, :d_ff], ab[:, d_ff:]
        sig = 0.5 * jnp.tanh(0.5 * a) + 0.5
        act = a * sig
        hid[0:rows, :] = (act * b).astype(BF16)
        dab[0:rows, 0:d_ff] = (dh * b * sig * (1.0 + a * (1.0 - sig))).astype(BF16)
        dab[0:rows, d_ff:] = (dh * act).astype(BF16)
        if size < self.cap:
            def columns(k, carry):
                cols = pl.ds(pl.multiple_of(k * d_ff, d_ff), d_ff)
                self.g13[g, :, cols] = self.g13[g, :, cols] + dot_tn(load(self.rows_x), dab[0:rows, cols])
                self.g2[g, :, cols] = self.g2[g, :, cols] + dot_tn(hid[0:rows, :], self.rows_d[0:n_src, pl.ds(at, size), cols].reshape(rows, d_ff))
                return carry

            lax.fori_loop(0, 2, columns, 0)
        else:
            for out, lhs, rhs in ((self.g13, load(self.rows_x), dab[0:rows, :]), (self.g2, hid[0:rows, :], load(self.rows_d))):
                if g_in:
                    out[g] = out[g] + dot_tn(lhs, rhs)
                else:
                    out[g] = dot_tn(lhs, rhs)
        if n_own:
            kept_o, kept_x = self.own_scratch[:2]
            m = n_own * size
            o = dot_nn(hid[0:m, :], w2[...]).astype(BF16)
            dx = dot_nt(dab[0:m, :], w13[...]).astype(BF16)
            kept_o[:, pl.ds(keep, size), :] = o.reshape(n_own, size, d_model)
            kept_x[:, pl.ds(keep, size), :] = dx.reshape(n_own, size, d_model)

    def stage(self, srcs, n_own, first, last, before, held, events, ship, each=None, prelude=lambda: None):
        n_src, n_loc, cap, group = len(srcs), self.n_loc, self.cap, self.group
        width = 1 if n_src == 2 else 2
        turns = n_src // width
        fetch = [self.fetches(s, r) for s, r in enumerate(srcs)]

        def ask(t):
            for s in range(t, n_src, turns):
                before[s]()
                start(fetch[s])

        eager = all(b is nothing for b in before)
        for t in range(turns if eager else 1):
            ask(t)
        prelude()

        def wave(p, carry):
            def turn(t, carry):
                some = [t + j * turns for j in range(width)]

                @pl.when(p == 0)
                def _():
                    for k in range(turns):
                        @pl.when(t == k)
                        def _(k=k):
                            for s in range(k, n_src, turns):
                                wait(fetch[s])
                    for s in some:
                        self.ranks(s)
                        self.gather(s, [(0, self.far, self.part, self.extra)])
                    for k in range(0 if eager else turns - 1):
                        @pl.when(t == k)
                        def _(k=k):
                            ask(k + 1)

                for s in some:
                    self.gather(s, [(group * p + i, 0.0, i * cap, cap) for i in range(group)])
                return carry

            lax.fori_loop(0, turns, turn, 0)

            def one(i, carry):
                e = group * p + i
                wait(self.load_w(e))
                if last:
                    @pl.when(e + 1 < n_loc)
                    def _():
                        start(self.load_w(e + 1))
                else:
                    start(self.load_w(lax.rem(e + 1, n_loc)))

                @pl.when(e >= 2)
                def _():
                    wait(self.save_g(e - 2))

                for k, copies in enumerate(held):
                    @pl.when(e == k)
                    def _(copies=copies):
                        wait(copies)

                if first:
                    @pl.when(e + 2 >= n_loc)
                    def _():
                        start(self.load_g(e + 2 - n_loc))
                elif last:
                    @pl.when(e + 2 < n_loc)
                    def _():
                        start(self.load_g(e + 2))
                else:
                    start(self.load_g(lax.rem(e + 2, n_loc)))
                if not first:
                    wait(self.load_g(e))
                self.block(n_src, n_own, pl.multiple_of(i * cap, cap), cap, pl.multiple_of(e * cap, cap),
                           lax.rem(e, 2), lax.rem(e, 4), not first)

                @pl.when(e == 0)
                def more():
                    self.block(n_src, n_own, self.part, self.extra, self.cold, 0, 0, True)

                start(self.save_g(e))
                for k, event in events:
                    @pl.when(e == k)
                    def _(event=event):
                        event()
                if each is not None:
                    each(e)
                return carry

            lax.fori_loop(0, group, one, 0)
            return carry

        lax.fori_loop(0, n_loc // group, wave, 0)
        if n_own:
            self.combine(n_own, ship)
        elif last:
            wait(self.save_g(n_loc - 2))
            wait(self.save_g(n_loc - 1))

    def combine(self, n_own, ship):
        kept_o, kept_x = self.own_scratch[:2]
        cold, extra, cap, tok, n_loc = self.cold, self.extra, self.cap, self.tok, self.n_loc
        part, n_blk = self.part, n_loc // self.group
        pieces = [(i, 0.0, i // self.group, i % self.group * cap, cap) for i in range(n_loc)] + [(0, self.far, None, part, extra)]
        places = [(ref, pl.ds(lane * tok, tok)) for ref in (self.rows_x, self.rows_d) for lane in (0, 1)]

        def one(src, carry):
            for s in range(n_own):
                @pl.when(src == s)
                def _(s=s):
                    wait(self.save_g(n_loc - 2 + s))

            for i, base, blk, at, size in pieces:
                match = self.match_rows(src, i, base, size)
                gate = self.meta[src, 8 + i:9 + i, :]
                hi = gate.astype(BF16).astype(F32)
                mid = (gate - hi).astype(BF16).astype(F32)
                low = gate - hi - mid
                for k, v in enumerate((hi, mid, low, 1.0)):
                    ref, lanes = places[0 if blk is None else k]
                    ref[k if blk is None else blk, at:at + size, lanes] = jnp.where(match, v, 0.0).astype(BF16)

            def chosen(k):
                ref, lanes = places[k]
                return ref[0:n_blk, 0:part, lanes].reshape(cold, tok)

            spare, lanes = places[0]
            wide = self.d_model // 2

            def columns(h, carry):
                cols = pl.ds(pl.multiple_of(h * wide, wide), wide)
                o, rest = kept_o[src, 0:cold, cols], kept_o[src, cold:cold + extra, cols]
                y = dot_tn(chosen(0), o) + dot_tn(chosen(1), o) + dot_tn(chosen(2), o)
                gates = spare[0:3, part:part + extra, lanes].reshape(3 * extra, tok)
                self.g13[2 + src, 0:tok, cols] = y + dot_tn(gates, jnp.concatenate([rest] * 3, axis=0))
                dx = dot_tn(chosen(3), kept_x[src, 0:cold, cols])
                gates = spare[3, part:part + extra, lanes]
                self.g13[2 + src, tok:2 * tok, cols] = dx + dot_tn(gates, kept_x[src, cold:cold + extra, cols])
                return carry

            lax.fori_loop(0, 2, columns, 0)
            for s in range(n_own):
                @pl.when(src == s)
                def _(s=s):
                    ship[s].start()
            return carry

        lax.fori_loop(0, n_own, one, 0)


def start(copies):
    for c in copies:
        c.start()


def wait(copies):
    for c in copies:
        c.wait()


def nothing():
    pass


class Adder:
    def __init__(self, a, b, out, held, load_sem, save_sem, ready):
        self.a, self.b, self.out, self.held, self.load_sem, self.save_sem, self.ready = a, b, out, held, load_sem, save_sem, ready
        self.rows = held.shape[2]

    def loads(self, k):
        slot, at = lax.rem(k, 2), pl.ds(pl.multiple_of(k * self.rows, self.rows), self.rows)
        return [pltpu.make_async_copy(v.at[at], self.held.at[slot, n], self.load_sem.at[slot, n]) for n, v in enumerate((self.a, self.b))]

    def save(self, k):
        slot, at = lax.rem(k, 2), pl.ds(pl.multiple_of(k * self.rows, self.rows), self.rows)
        return pltpu.make_async_copy(self.held.at[slot, 0], self.out.at[at], self.save_sem.at[slot])

    def add(self, k):
        wait(self.loads(k))
        slot = lax.rem(k, 2)
        self.held[slot, 0] = self.held[slot, 0] + self.held[slot, 1]
        self.save(k).start()

    def __call__(self, e):
        @pl.when(e == 0)
        def _():
            self.ready()

        @pl.when(e >= 1)
        def _():
            self.add(e - 1)

        @pl.when(e >= 2)
        def _():
            self.save(e - 2).wait()

        start(self.loads(e))

    def finish(self, last):
        self.add(last)
        self.save(last - 1).wait()
        self.save(last).wait()


def roam_kernel(cfg, lead_ref, tokens, grad_y, rg, w1, w3, w2, g1, g3, g2, land, own_a, own_b, got_a, got_b, mine, chip, *scratch):
    send_sem, recv_sem, part_sem, held, add_in_sem, add_out_sem = scratch[-6:]
    eng = Engine(cfg, lead_ref[0, 0], (w1, w3, w2), (g1, g3, g2), (g1, g3, g2), scratch[:-6], 2)
    q, r = lax.axis_index("data"), lax.axis_index("expert")
    n_data, n_er, tok, n_loc = cfg["n_data"], cfg["n_er"], cfg["tok"], cfg["n_loc"]
    partner = {"expert": r + 1 - 2 * lax.rem(r, 2)}
    across = {"expert": lax.rem(r + n_er // 2, n_er)}
    znext = {"data": lax.rem(q + 1, n_data)}
    zprev = {"data": lax.rem(q + n_data - 1, n_data)}

    def at(name, rows=None):
        ref = land.at[BLOCKS.index(name)]
        return ref if rows is None else ref.at[rows]

    flights = []

    def remote(src, dst, device):
        k = len(flights)
        copy = pltpu.make_async_remote_copy(src_ref=src, dst_ref=dst, send_sem=send_sem.at[k], recv_sem=recv_sem.at[k],
                                            device_id=device, device_id_type=MESH)
        flights.append(copy)
        return copy

    def first(name, device):
        parts = ((tokens, 0, tok), (grad_y, tok, tok), (rg, 2 * tok, RG_ROWS))
        return [remote(v, at(name, pl.ds(lo, n)), device) for v, lo, n in parts]

    def onward(src, dst, device):
        return [remote(at(src), at(dst), device)]

    upper, lower = pl.ds(0, tok), pl.ds(tok, tok + RG_ROWS)
    c_other, c_far, c_z1 = first("other", partner), first("far", across), first("z1", znext)
    c_far_o, c_z1_o = onward("far", "far_o", partner), onward("z1", "z1_o", partner)
    c_z1y, c_z2 = onward("z1", "z1y", across), onward("z1", "z2", znext)
    c_z1y_o, c_z2_o = onward("z1y", "z1y_o", partner), onward("z2", "z2_o", partner)
    c_z2y, c_z3 = onward("z2", "z2y", across), onward("z2", "z3", znext)
    c_z2y_o, c_z3_o = onward("z2y", "z2y_o", partner), onward("z3", "z3_o", partner)
    c_z3y_z = [remote(at("far", upper), at("z3y", upper), zprev)]
    c_z3y_y = [remote(at("z3", lower), at("z3y", lower), across)]
    c_z3y_zo = [remote(at("z3y", upper), at("z3y_o", upper), partner)]
    c_z3y_yo = [remote(at("z3y", lower), at("z3y_o", lower), partner)]
    c_got_a, c_got_b = [remote(eng.g13.at[3], got_a, partner)], [remote(eng.g13.at[3], got_b, partner)]
    keep_a = pltpu.make_async_copy(eng.g13.at[2], own_a, part_sem.at[0])
    keep_b = pltpu.make_async_copy(eng.g13.at[2], own_b, part_sem.at[1])

    barrier = pltpu.get_barrier_semaphore()
    for device in (partner, across, znext, zprev):
        pl.semaphore_signal(barrier, inc=1, device_id=device, device_id_type=MESH)
    pl.semaphore_wait(barrier, 4)

    class Sent:
        def __init__(self, copy):
            self.copy = copy

        def wait(self):
            self.copy.wait_send()

    def arrived(copies, then=()):
        def event():
            for c in copies:
                c.wait_recv()
            start(then)
        return event

    start(c_other + c_far + c_z1)
    eng.stage([(tokens, grad_y, rg), at("other")], 2, True, False, [nothing, arrived(c_other)], (), (), [keep_a, c_got_a[0]],
              prelude=lambda: start(eng.load_w(0)))
    sum_a = Adder(own_a, got_a, mine, held, add_in_sem, add_out_sem, arrived(c_got_a))
    eng.stage([at("far"), at("far_o"), at("z1"), at("z1_o")], 2, False, False,
              [arrived(c_far, c_far_o), arrived(c_far_o), arrived(c_z1, c_z1_o + c_z1y + c_z2), arrived(c_z1_o)],
              ([keep_a], [Sent(c_got_a[0])]),
              ((6, arrived(c_z1y + c_z2, c_z2y + c_z3 + c_z3y_z + c_z1y_o + c_z2_o)),),
              [keep_b, c_got_b[0]], sum_a)
    sum_a.finish(n_loc - 1)
    sum_b = Adder(own_b, got_b, chip, held, add_in_sem, add_out_sem, arrived(c_got_b))
    eng.stage([at("z1y"), at("z1y_o"), at("z2"), at("z2_o")], 0, False, True,
              [nothing, arrived(c_z1y_o), nothing, arrived(c_z2_o)],
              ([keep_b], [Sent(c_got_b[0])]),
              ((3, arrived(c_z2y + c_z3, c_z3y_y + c_z2y_o + c_z3_o)), (6, arrived(c_z3y_z, c_z3y_zo))), (), sum_b)
    arrived(c_z3y_y, c_z3y_yo)()
    sum_b.finish(n_loc - 1)
    arrived(c_z2y_o + c_z3_o + c_z3y_zo + c_z3y_yo)()
    for c in flights:
        if c is not c_got_a[0] and c is not c_got_b[0]:
            c.wait_send()


def rest_kernel(cfg, lead_ref, land, w1, w3, w2, b1, b3, b2, g1, g3, g2, *scratch):
    eng = Engine(cfg, lead_ref[0, 0], (w1, w3, w2), (b1, b3, b2), (g1, g3, g2), scratch, 2)

    def prelude():
        start(eng.load_w(0))
        for e in (0, 1):
            start(eng.load_g(e))

    names = ("z2y", "z2y_o", "z3", "z3_o", "z3y", "z3y_o")
    eng.stage([land.at[BLOCKS.index(n)] for n in names], 0, False, True, [nothing] * 6, (), (), (), prelude=prelude)


def call_kernel(name, kernel, cfg, args, shapes, n_src, n_own, extra_scratch, params):
    tok, d_model, d_ff, n_loc, cap, extra = (cfg[k] for k in ("tok", "d_model", "d_ff", "n_loc", "cap", "extra"))
    rows = n_loc * cap + extra
    scratch = [pltpu.VMEM((n_src, 2 * cap + extra, d_model), BF16)] * 2 + [
        pltpu.VMEM((n_src, 16, tok), F32),
        pltpu.VMEM((n_src, 2 * tok + RG_ROWS, d_model), BF16),
        pltpu.VMEM((n_src * cap, d_ff), BF16),
        pltpu.VMEM((n_src * cap, 2 * d_ff), BF16),
    ]
    for slots, kind in ((2, BF16), (4, F32)):
        scratch += [pltpu.VMEM((slots, d_model, 2 * d_ff), kind), pltpu.VMEM((slots, d_ff, d_model), kind)]
    scratch += [pltpu.SemaphoreType.DMA(n) for n in ((n_src, 3), (2, 3), (4, 3), (4, 3))]
    if n_own:
        scratch += [pltpu.VMEM((n_own, rows, d_model), BF16)] * 2
    unit = 2 * d_model * d_ff * rows
    return pl.pallas_call(
        functools.partial(kernel, cfg),
        in_specs=[pl.BlockSpec(memory_space=pltpu.SMEM)] + [pl.BlockSpec(memory_space=pl.ANY)] * (len(args) - 1),
        out_specs=[pl.BlockSpec(memory_space=pl.ANY)] * len(shapes),
        out_shape=shapes,
        scratch_shapes=scratch + extra_scratch,
        compiler_params=pltpu.CompilerParams(vmem_limit_bytes=67_000_000, **params),
        cost_estimate=pl.CostEstimate(flops=unit * (8 * n_src + 7 * n_own) // 8, bytes_accessed=100 << 20, transcendentals=0),
        name=name,
    )(*args)


def solution(mesh):
    n_data, n_er = mesh.shape["data"], mesh.shape["expert"]
    row_spec = P(("pod", "data", "expert"), None)
    w_spec = P("expert", None, None)
    grad_spec = P(("pod", "expert"), None, None)
    across = [(r, r ^ 2) for r in range(n_er)]

    def body(tokens, routes, gates, grad_y, w_in1, w_in3, w_out):
        n_loc, d_model, d_ff = w_in1.shape
        n_exp, tok = n_loc * n_er, tokens.shape[0]
        cap, cap_hot = caps(tok, routes.shape[1], n_exp)
        cfg = dict(tok=tok, d_model=d_model, d_ff=d_ff, n_loc=n_loc, n_exp=n_exp, cap=cap, extra=cap_hot - cap,
                   n_data=n_data, n_er=n_er)
        lead = lax.axis_index("expert").astype(jnp.int32).reshape(1, 1)
        gate = gates.T
        hi = lax.reduce_precision(gate, 8, 7)
        mid = lax.reduce_precision(gate - hi, 8, 7)
        low = gate - hi - mid
        rg = jnp.concatenate([jnp.concatenate([routes.T.astype(F32), hi], 0), jnp.concatenate([mid, low], 0)], 1).astype(BF16)
        weights = (w_in1, w_in3, w_out)
        grads = [jax.ShapeDtypeStruct(w.shape, F32) for w in weights]
        sums = [jax.ShapeDtypeStruct((2 * tok, d_model), F32)] * 6
        land = jax.ShapeDtypeStruct((len(BLOCKS), 2 * tok + RG_ROWS, d_model), BF16)
        dma, n_fly = pltpu.SemaphoreType.DMA, 27
        *acc, land, _, _, _, _, mine, chip = call_kernel(
            "roam", roam_kernel, cfg, [lead, tokens, grad_y, rg, *weights], [*grads, land, *sums], 4, 2,
            [dma((n_fly,)), dma((n_fly,)), dma((2,)), pltpu.VMEM((2, 2, 2 * tok // n_loc, d_model), F32), dma((2, 2)), dma((2,))],
            dict(collective_id=0, has_side_effects=True))
        back = lax.ppermute(chip, "expert", across)
        acc1, acc3, acc2 = call_kernel("rest", rest_kernel, cfg, [lead, land, *weights, *acc], grads, 6, 0, [], {})
        y_out = (mine[:tok] + back[:tok]).astype(BF16)
        grad_x = (mine[tok:] + back[tok:]).astype(BF16)
        return y_out, grad_x, acc1, acc3, acc2

    return jax.shard_map(body, mesh=mesh,
                         in_specs=(row_spec, row_spec, row_spec, row_spec, w_spec, w_spec, w_spec),
                         out_specs=(row_spec, row_spec, grad_spec, grad_spec, grad_spec),
                         check_vma=False)
```

```python
import functools

import jax
import jax.numpy as jnp
from jax import lax
from jax.experimental import pallas as pl
from jax.experimental.pallas import tpu as pltpu
from jax.sharding import PartitionSpec as P

MESH = pl.DeviceIdType.MESH
BLOCKS = ("other", "far", "far_o", "z1", "z1_o", "z1y", "z1y_o", "z2", "z2_o", "z2y", "z2y_o", "z3", "z3_o", "z3y", "z3y_o")
N_HOT = 2
RG_ROWS = 16
F32, BF16 = jnp.float32, jnp.bfloat16


def caps(tok_dev, top_k, n_exp):
    cap_hot = 3 * tok_dev // 8
    cap_cold = max(8, ((tok_dev * top_k - N_HOT * cap_hot) // (n_exp - N_HOT) + 7) // 8 * 8)
    return cap_cold, cap_hot


def dot_nn(a, b):
    return lax.dot_general(a, b, (((1,), (0,)), ((), ())), preferred_element_type=F32)


def dot_nt(a, b):
    return lax.dot_general(a, b, (((1,), (1,)), ((), ())), preferred_element_type=F32)


def dot_tn(a, b):
    return lax.dot_general(a, b, (((0,), (0,)), ((), ())), preferred_element_type=F32)


def prefix(m):
    lane = lax.broadcasted_iota(jnp.int32, m.shape, 1)
    step = 1
    while step < m.shape[1]:
        m = m + jnp.where(lane >= step, pltpu.roll(m, step, 1), 0.0)
        step *= 2
    return m


class Engine:
    def __init__(self, cfg, lead, weights, bases, outs, scratch, group):
        self.__dict__.update(cfg)
        self.lead, self.weights, self.bases, self.outs, self.group = lead, weights, bases, outs, group
        (self.rows_x, self.rows_d, self.meta, self.buf, self.hid, self.dab, self.w13, self.w2, self.g13, self.g2,
         self.src_sem, self.w_sem, self.in_sem, self.out_sem) = scratch[:14]
        self.own_scratch = scratch[14:]
        hot = jnp.logical_or(lead * self.n_loc == 0, lead * self.n_loc == self.n_exp // 2)
        self.far = jnp.where(hot, float(self.cap), float(2 * self.tok))
        self.cold, self.part = self.n_loc * self.cap, group * self.cap

    def triple(self, both, single, slot):
        f = self.d_ff
        return both.at[slot, :, 0:f], both.at[slot, :, f:2 * f], single.at[slot]

    def load_w(self, e):
        slot = lax.rem(e, 2)
        return [pltpu.make_async_copy(w.at[e], b, self.w_sem.at[slot, k])
                for k, (w, b) in enumerate(zip(self.weights, self.triple(self.w13, self.w2, slot)))]

    def load_g(self, e):
        slot = lax.rem(e, 4)
        return [pltpu.make_async_copy(w.at[e], b, self.in_sem.at[slot, k])
                for k, (w, b) in enumerate(zip(self.bases, self.triple(self.g13, self.g2, slot)))]

    def save_g(self, e):
        slot = lax.rem(e, 4)
        return [pltpu.make_async_copy(b, w.at[e], self.out_sem.at[slot, k])
                for k, (w, b) in enumerate(zip(self.outs, self.triple(self.g13, self.g2, slot)))]

    def fetches(self, s, ref):
        if not isinstance(ref, tuple):
            return [pltpu.make_async_copy(ref, self.buf.at[s], self.src_sem.at[s, 0])]
        dst = self.buf.at[s]
        return [pltpu.make_async_copy(r, dst.at[pl.ds(at, r.shape[0])], self.src_sem.at[s, k])
                for k, (r, at) in enumerate(zip(ref, (0, self.tok, 2 * self.tok)))]

    def match_rows(self, src, i, base, size):
        iota = lax.broadcasted_iota(jnp.int32, (size, self.tok), 0).astype(F32) + base
        return iota == self.meta[src, pl.ds(i, 1), :]

    def ranks(self, s):
        tok = self.tok
        rg = self.buf[s, 2 * tok:2 * tok + RG_ROWS, :].astype(F32)
        routes = rg[0:8, :tok]
        gates = (rg[8:16, :tok] + rg[0:8, tok:]) + rg[8:16, tok:]
        member, weight = [], []
        for i in range(self.n_loc):
            match = routes == (self.lead * self.n_loc + i).astype(F32)
            member.append(jnp.sum(jnp.where(match, 1.0, 0.0), axis=0, keepdims=True))
            weight.append(jnp.sum(jnp.where(match, gates, 0.0), axis=0, keepdims=True))
        member = jnp.concatenate(member, axis=0)
        self.meta[s, 0:8, :] = jnp.where(member > 0.0, prefix(member) - 1.0, -1.0)
        self.meta[s, 8:16, :] = jnp.concatenate(weight, axis=0)

    def gather(self, s, which):
        tok, meta, buf = self.tok, self.meta, self.buf
        pick, gate = [], []
        for i, base, at, size in which:
            match = self.match_rows(s, i, base, size)
            pick.append(jnp.where(match, 1.0, 0.0).astype(BF16))
            gate.append(jnp.sum(jnp.where(match, meta[s, pl.ds(8 + i, 1), :], 0.0), axis=1, keepdims=True))
        pick, gate = jnp.concatenate(pick, axis=0), jnp.concatenate(gate, axis=0)
        at, size = which[0][2], pick.shape[0]
        self.rows_x[s, at:at + size, :] = dot_nn(pick, buf[s, 0:tok, :]).astype(BF16)
        self.rows_d[s, at:at + size, :] = (dot_nn(pick, buf[s, tok:2 * tok, :]) * gate).astype(BF16)

    def block(self, n_src, n_own, at, size, keep, w, g, g_in):
        d_model, d_ff, hid, dab = self.d_model, self.d_ff, self.hid, self.dab
        w13, w2 = self.w13.at[w], self.w2.at[w]
        rows = n_src * size

        def load(ref):
            return ref[0:n_src, pl.ds(at, size), :].reshape(rows, d_model)

        ab = dot_nn(load(self.rows_x), w13[...]).astype(BF16).astype(F32)
        dh = dot_nt(load(self.rows_d), w2[...])
        a, b = ab[:, :d_ff], ab[:, d_ff:]
        sig = 0.5 * jnp.tanh(0.5 * a) + 0.5
        act = a * sig
        hid[0:rows, :] = (act * b).astype(BF16)
        dab[0:rows, 0:d_ff] = (dh * b * sig * (1.0 + a * (1.0 - sig))).astype(BF16)
        dab[0:rows, d_ff:] = (dh * act).astype(BF16)
        if size < self.cap:
            def columns(k, carry):
                cols = pl.ds(pl.multiple_of(k * d_ff, d_ff), d_ff)
                self.g13[g, :, cols] = self.g13[g, :, cols] + dot_tn(load(self.rows_x), dab[0:rows, cols])
                self.g2[g, :, cols] = self.g2[g, :, cols] + dot_tn(hid[0:rows, :], self.rows_d[0:n_src, pl.ds(at, size), cols].reshape(rows, d_ff))
                return carry

            lax.fori_loop(0, 2, columns, 0)
        else:
            for out, lhs, rhs in ((self.g13, load(self.rows_x), dab[0:rows, :]), (self.g2, hid[0:rows, :], load(self.rows_d))):
                if g_in:
                    out[g] = out[g] + dot_tn(lhs, rhs)
                else:
                    out[g] = dot_tn(lhs, rhs)
        if n_own:
            kept_o, kept_x = self.own_scratch[:2]
            m = n_own * size
            o = dot_nn(hid[0:m, :], w2[...]).astype(BF16)
            dx = dot_nt(dab[0:m, :], w13[...]).astype(BF16)
            kept_o[:, pl.ds(keep, size), :] = o.reshape(n_own, size, d_model)
            kept_x[:, pl.ds(keep, size), :] = dx.reshape(n_own, size, d_model)

    def stage(self, srcs, n_own, first, last, before, held, events, ship, each=None, prelude=lambda: None):
        n_src, n_loc, cap, group = len(srcs), self.n_loc, self.cap, self.group
        width = 1 if n_src == 2 else 2
        turns = n_src // width
        fetch = [self.fetches(s, r) for s, r in enumerate(srcs)]

        def ask(t):
            for s in range(t, n_src, turns):
                before[s]()
                start(fetch[s])

        eager = all(b is nothing for b in before)
        for t in range(turns if eager else 1):
            ask(t)
        prelude()

        def wave(p, carry):
            def turn(t, carry):
                some = [t + j * turns for j in range(width)]

                @pl.when(p == 0)
                def _():
                    for k in range(turns):
                        @pl.when(t == k)
                        def _(k=k):
                            for s in range(k, n_src, turns):
                                wait(fetch[s])
                    for s in some:
                        self.ranks(s)
                        self.gather(s, [(0, self.far, self.part, self.extra)])
                    for k in range(0 if eager else turns - 1):
                        @pl.when(t == k)
                        def _(k=k):
                            ask(k + 1)

                for s in some:
                    self.gather(s, [(group * p + i, 0.0, i * cap, cap) for i in range(group)])
                return carry

            lax.fori_loop(0, turns, turn, 0)

            def one(i, carry):
                e = group * p + i
                wait(self.load_w(e))
                if last:
                    @pl.when(e + 1 < n_loc)
                    def _():
                        start(self.load_w(e + 1))
                else:
                    start(self.load_w(lax.rem(e + 1, n_loc)))

                @pl.when(e >= 2)
                def _():
                    wait(self.save_g(e - 2))

                for k, copies in enumerate(held):
                    @pl.when(e == k)
                    def _(copies=copies):
                        wait(copies)

                if first:
                    @pl.when(e + 2 >= n_loc)
                    def _():
                        start(self.load_g(e + 2 - n_loc))
                elif last:
                    @pl.when(e + 2 < n_loc)
                    def _():
                        start(self.load_g(e + 2))
                else:
                    start(self.load_g(lax.rem(e + 2, n_loc)))
                if not first:
                    wait(self.load_g(e))
                self.block(n_src, n_own, pl.multiple_of(i * cap, cap), cap, pl.multiple_of(e * cap, cap),
                           lax.rem(e, 2), lax.rem(e, 4), not first)

                @pl.when(e == 0)
                def more():
                    self.block(n_src, n_own, self.part, self.extra, self.cold, 0, 0, True)

                start(self.save_g(e))
                for k, event in events:
                    @pl.when(e == k)
                    def _(event=event):
                        event()
                if each is not None:
                    each(e)
                return carry

            lax.fori_loop(0, group, one, 0)
            return carry

        lax.fori_loop(0, n_loc // group, wave, 0)
        if n_own:
            self.combine(n_own, ship)
        elif last:
            wait(self.save_g(n_loc - 2))
            wait(self.save_g(n_loc - 1))

    def combine(self, n_own, ship):
        kept_o, kept_x = self.own_scratch[:2]
        cold, extra, cap, tok, n_loc = self.cold, self.extra, self.cap, self.tok, self.n_loc
        part, n_blk = self.part, n_loc // self.group
        pieces = [(i, 0.0, i // self.group, i % self.group * cap, cap) for i in range(n_loc)] + [(0, self.far, None, part, extra)]
        places = [(ref, pl.ds(lane * tok, tok)) for ref in (self.rows_x, self.rows_d) for lane in (0, 1)]

        def one(src, carry):
            for s in range(n_own):
                @pl.when(src == s)
                def _(s=s):
                    wait(self.save_g(n_loc - 2 + s))

            for i, base, blk, at, size in pieces:
                match = self.match_rows(src, i, base, size)
                gate = self.meta[src, 8 + i:9 + i, :]
                hi = gate.astype(BF16).astype(F32)
                mid = (gate - hi).astype(BF16).astype(F32)
                low = gate - hi - mid
                for k, v in enumerate((hi, mid, low, 1.0)):
                    ref, lanes = places[0 if blk is None else k]
                    ref[k if blk is None else blk, at:at + size, lanes] = jnp.where(match, v, 0.0).astype(BF16)

            def chosen(k):
                ref, lanes = places[k]
                return ref[0:n_blk, 0:part, lanes].reshape(cold, tok)

            spare, lanes = places[0]
            wide = self.d_model // 2

            def columns(h, carry):
                cols = pl.ds(pl.multiple_of(h * wide, wide), wide)
                o, rest = kept_o[src, 0:cold, cols], kept_o[src, cold:cold + extra, cols]
                y = dot_tn(chosen(0), o) + dot_tn(chosen(1), o) + dot_tn(chosen(2), o)
                gates = spare[0:3, part:part + extra, lanes].reshape(3 * extra, tok)
                self.g13[2 + src, 0:tok, cols] = y + dot_tn(gates, jnp.concatenate([rest] * 3, axis=0))
                dx = dot_tn(chosen(3), kept_x[src, 0:cold, cols])
                gates = spare[3, part:part + extra, lanes]
                self.g13[2 + src, tok:2 * tok, cols] = dx + dot_tn(gates, kept_x[src, cold:cold + extra, cols])
                return carry

            lax.fori_loop(0, 2, columns, 0)
            for s in range(n_own):
                @pl.when(src == s)
                def _(s=s):
                    ship[s].start()
            return carry

        lax.fori_loop(0, n_own, one, 0)


def start(copies):
    for c in copies:
        c.start()


def wait(copies):
    for c in copies:
        c.wait()


def nothing():
    pass


class Adder:
    def __init__(self, a, b, out, held, load_sem, save_sem, ready):
        self.a, self.b, self.out, self.held, self.load_sem, self.save_sem, self.ready = a, b, out, held, load_sem, save_sem, ready
        self.rows = held.shape[2]
        self.n_head = out[0].shape[0] // self.rows if out[0] is not None else 0

    def loads(self, k):
        slot, at = lax.rem(k, 2), pl.ds(pl.multiple_of(k * self.rows, self.rows), self.rows)
        return [pltpu.make_async_copy(v.at[at], self.held.at[slot, n], self.load_sem.at[slot, n]) for n, v in enumerate((self.a, self.b))]

    def save(self, k, head=False):
        slot = lax.rem(k, 2)
        ref, k = (self.out[0], k) if head else (self.out[1], k - self.n_head)
        at = pl.ds(pl.multiple_of(k * self.rows, self.rows), self.rows)
        return pltpu.make_async_copy(self.held.at[slot, 0], ref.at[at], self.save_sem.at[slot])

    def add(self, k):
        wait(self.loads(k))
        slot = lax.rem(k, 2)
        self.held[slot, 0] = self.held[slot, 0] + self.held[slot, 1]
        if self.n_head:
            @pl.when(k < self.n_head)
            def _():
                self.save(k, True).start()

        @pl.when(k >= self.n_head)
        def _():
            self.save(k).start()

    def saved(self, k):
        if self.n_head:
            @pl.when(k < self.n_head)
            def _():
                self.save(k, True).wait()

        @pl.when(k >= self.n_head)
        def _():
            self.save(k).wait()

    def __call__(self, e):
        @pl.when(e == 0)
        def _():
            self.ready()

        @pl.when(e >= 1)
        def _():
            self.add(e - 1)

        @pl.when(e >= 2)
        def _():
            self.saved(e - 2)

        start(self.loads(e))

    def finish(self, last):
        self.add(last)
        self.saved(last - 1)
        self.saved(last)


def roam_kernel(cfg, lead_ref, tokens, grad_y, rg, w1, w3, w2, g1, g3, g2, land, own_a, own_b, got_a, got_b, mine, chip_a, chip_b, back_a, *scratch):
    send_sem, recv_sem, part_sem, held, add_in_sem, add_out_sem = scratch[-6:]
    eng = Engine(cfg, lead_ref[0, 0], (w1, w3, w2), (g1, g3, g2), (g1, g3, g2), scratch[:-6], 2)
    q, r = lax.axis_index("data"), lax.axis_index("expert")
    n_data, n_er, tok, n_loc = cfg["n_data"], cfg["n_er"], cfg["tok"], cfg["n_loc"]
    partner = {"expert": r + 1 - 2 * lax.rem(r, 2)}
    across = {"expert": lax.rem(r + n_er // 2, n_er)}
    znext = {"data": lax.rem(q + 1, n_data)}
    zprev = {"data": lax.rem(q + n_data - 1, n_data)}

    def at(name, rows=None):
        ref = land.at[BLOCKS.index(name)]
        return ref if rows is None else ref.at[rows]

    flights = []

    def remote(src, dst, device):
        k = len(flights)
        copy = pltpu.make_async_remote_copy(src_ref=src, dst_ref=dst, send_sem=send_sem.at[k], recv_sem=recv_sem.at[k],
                                            device_id=device, device_id_type=MESH)
        flights.append(copy)
        return copy

    def first(name, device):
        parts = ((tokens, 0, tok), (grad_y, tok, tok), (rg, 2 * tok, RG_ROWS))
        return [remote(v, at(name, pl.ds(lo, n)), device) for v, lo, n in parts]

    def onward(src, dst, device):
        return [remote(at(src), at(dst), device)]

    cut = (2 * tok + RG_ROWS) // 64 * 48
    upper, lower = pl.ds(0, cut), pl.ds(cut, 2 * tok + RG_ROWS - cut)
    c_back = [remote(chip_a, back_a, across)]
    c_other, c_far, c_z1 = first("other", partner), first("far", across), first("z1", znext)
    c_far_o, c_z1_o = onward("far", "far_o", partner), onward("z1", "z1_o", partner)
    c_z1y, c_z2 = onward("z1", "z1y", across), onward("z1", "z2", znext)
    c_z1y_o, c_z2_o = onward("z1y", "z1y_o", partner), onward("z2", "z2_o", partner)
    c_z2y, c_z3 = onward("z2", "z2y", across), onward("z2", "z3", znext)
    c_z2y_o, c_z3_o = onward("z2y", "z2y_o", partner), onward("z3", "z3_o", partner)
    c_z3y_z = [remote(at("far", upper), at("z3y", upper), zprev)]
    c_z3y_y = [remote(at("z3", lower), at("z3y", lower), across)]
    c_z3y_zo = [remote(at("z3y", upper), at("z3y_o", upper), partner)]
    c_z3y_yo = [remote(at("z3y", lower), at("z3y_o", lower), partner)]
    c_got_a, c_got_b = [remote(eng.g13.at[3], got_a, partner)], [remote(eng.g13.at[3], got_b, partner)]
    keep_a = pltpu.make_async_copy(eng.g13.at[2], own_a, part_sem.at[0])
    keep_b = pltpu.make_async_copy(eng.g13.at[2], own_b, part_sem.at[1])

    barrier = pltpu.get_barrier_semaphore()
    for device in (partner, across, znext, zprev):
        pl.semaphore_signal(barrier, inc=1, device_id=device, device_id_type=MESH)
    pl.semaphore_wait(barrier, 4)

    class Sent:
        def __init__(self, copy):
            self.copy = copy

        def wait(self):
            self.copy.wait_send()

    def arrived(copies, then=()):
        def event():
            for c in copies:
                c.wait_recv()
            start(then)
        return event

    start(c_other + c_far + c_z1)
    eng.stage([(tokens, grad_y, rg), at("other")], 2, True, False, [nothing, arrived(c_other)], (), (), [keep_a, c_got_a[0]],
              prelude=lambda: start(eng.load_w(0)))
    sum_a = Adder(own_a, got_a, (None, mine), held, add_in_sem, add_out_sem, arrived(c_got_a))
    eng.stage([at("far"), at("far_o"), at("z1"), at("z1_o")], 2, False, False,
              [arrived(c_far, c_far_o), arrived(c_far_o), arrived(c_z1, c_z1_o + c_z1y + c_z2), arrived(c_z1_o)],
              ([keep_a], [Sent(c_got_a[0])]),
              ((6, arrived(c_z1y + c_z2, c_z2y + c_z3 + c_z1y_o + c_z2_o)),),
              [keep_b, c_got_b[0]], sum_a)
    sum_a.finish(n_loc - 1)
    sum_b = Adder(own_b, got_b, (chip_a, chip_b), held, add_in_sem, add_out_sem, arrived(c_got_b))
    eng.stage([at("z1y"), at("z1y_o"), at("z2"), at("z2_o")], 0, False, True,
              [nothing, arrived(c_z1y_o), nothing, arrived(c_z2_o)],
              ([keep_b], [Sent(c_got_b[0])]),
              ((3, arrived(c_z2y + c_z3, c_z3y_y + c_z3y_z + c_z2y_o + c_z3_o)), (4, lambda: start(c_back)), (6, arrived(c_z3y_y, c_z3y_yo))), (), sum_b)
    sum_b.finish(n_loc - 1)
    arrived(c_z3y_z, c_z3y_zo)()
    arrived(c_z2y_o + c_z3_o + c_z3y_zo + c_z3y_yo + c_back)()
    for c in flights:
        if c is not c_got_a[0] and c is not c_got_b[0]:
            c.wait_send()


def rest_kernel(cfg, lead_ref, land, w1, w3, w2, b1, b3, b2, g1, g3, g2, *scratch):
    eng = Engine(cfg, lead_ref[0, 0], (w1, w3, w2), (b1, b3, b2), (g1, g3, g2), scratch, 2)

    def prelude():
        start(eng.load_w(0))
        for e in (0, 1):
            start(eng.load_g(e))

    names = ("z2y", "z2y_o", "z3", "z3_o", "z3y", "z3y_o")
    eng.stage([land.at[BLOCKS.index(n)] for n in names], 0, False, True, [nothing] * 6, (), (), (), prelude=prelude)


def call_kernel(name, kernel, cfg, args, shapes, n_src, n_own, extra_scratch, params):
    tok, d_model, d_ff, n_loc, cap, extra = (cfg[k] for k in ("tok", "d_model", "d_ff", "n_loc", "cap", "extra"))
    rows = n_loc * cap + extra
    scratch = [pltpu.VMEM((n_src, 2 * cap + extra, d_model), BF16)] * 2 + [
        pltpu.VMEM((n_src, 16, tok), F32),
        pltpu.VMEM((n_src, 2 * tok + RG_ROWS, d_model), BF16),
        pltpu.VMEM((n_src * cap, d_ff), BF16),
        pltpu.VMEM((n_src * cap, 2 * d_ff), BF16),
    ]
    for slots, kind in ((2, BF16), (4, F32)):
        scratch += [pltpu.VMEM((slots, d_model, 2 * d_ff), kind), pltpu.VMEM((slots, d_ff, d_model), kind)]
    scratch += [pltpu.SemaphoreType.DMA(n) for n in ((n_src, 3), (2, 3), (4, 3), (4, 3))]
    if n_own:
        scratch += [pltpu.VMEM((n_own, rows, d_model), BF16)] * 2
    unit = 2 * d_model * d_ff * rows
    return pl.pallas_call(
        functools.partial(kernel, cfg),
        in_specs=[pl.BlockSpec(memory_space=pltpu.SMEM)] + [pl.BlockSpec(memory_space=pl.ANY)] * (len(args) - 1),
        out_specs=[pl.BlockSpec(memory_space=pl.ANY)] * len(shapes),
        out_shape=shapes,
        scratch_shapes=scratch + extra_scratch,
        compiler_params=pltpu.CompilerParams(vmem_limit_bytes=67_000_000, **params),
        cost_estimate=pl.CostEstimate(flops=unit * (8 * n_src + 7 * n_own) // 8, bytes_accessed=100 << 20, transcendentals=0),
        name=name,
    )(*args)


def last_sum(mine, back_a, back_b, tok, d_model):
    rows = back_a.shape[0] // 2
    n_half = tok // rows

    def kernel(m_ref, a_ref, b_ref, y_ref, x_ref):
        j = pl.program_id(0)

        @pl.when(j < 2)
        def _():
            y_ref[...] = (m_ref[...] + a_ref[...]).astype(BF16)

        @pl.when(jnp.logical_and(j >= 2, j < n_half))
        def _():
            y_ref[...] = (m_ref[...] + b_ref[...]).astype(BF16)

        @pl.when(j >= n_half)
        def _():
            x_ref[...] = (m_ref[...] + b_ref[...]).astype(BF16)

    def spec(index):
        return pl.BlockSpec((rows, d_model), lambda j: (index(j), 0))

    return pl.pallas_call(
        kernel,
        grid=(2 * n_half,),
        in_specs=[spec(lambda j: j), spec(lambda j: jnp.minimum(j, 1)), spec(lambda j: jnp.maximum(j - 2, 0))],
        out_specs=[spec(lambda j: jnp.minimum(j, n_half - 1)), spec(lambda j: jnp.maximum(j - n_half, 0))],
        out_shape=[jax.ShapeDtypeStruct((tok, d_model), BF16)] * 2,
        name="last",
    )(mine, back_a, back_b)


def solution(mesh):
    n_data, n_er = mesh.shape["data"], mesh.shape["expert"]
    row_spec = P(("pod", "data", "expert"), None)
    w_spec = P("expert", None, None)
    grad_spec = P(("pod", "expert"), None, None)
    across = [(r, r ^ 2) for r in range(n_er)]

    def body(tokens, routes, gates, grad_y, w_in1, w_in3, w_out):
        n_loc, d_model, d_ff = w_in1.shape
        n_exp, tok = n_loc * n_er, tokens.shape[0]
        cap, cap_hot = caps(tok, routes.shape[1], n_exp)
        cfg = dict(tok=tok, d_model=d_model, d_ff=d_ff, n_loc=n_loc, n_exp=n_exp, cap=cap, extra=cap_hot - cap,
                   n_data=n_data, n_er=n_er)
        lead = lax.axis_index("expert").astype(jnp.int32).reshape(1, 1)
        gate = gates.T
        hi = lax.reduce_precision(gate, 8, 7)
        mid = lax.reduce_precision(gate - hi, 8, 7)
        low = gate - hi - mid
        rg = jnp.concatenate([jnp.concatenate([routes.T.astype(F32), hi], 0), jnp.concatenate([mid, low], 0)], 1).astype(BF16)
        weights = (w_in1, w_in3, w_out)
        grads = [jax.ShapeDtypeStruct(w.shape, F32) for w in weights]
        sums = [jax.ShapeDtypeStruct((2 * tok, d_model), F32)] * 6
        land = jax.ShapeDtypeStruct((len(BLOCKS), 2 * tok + RG_ROWS, d_model), BF16)
        dma, n_fly, quarter = pltpu.SemaphoreType.DMA, 28, 2 * (2 * tok // n_loc)
        sums[5:] = [jax.ShapeDtypeStruct((n, d_model), F32) for n in (quarter, 2 * tok - quarter, quarter)]
        *acc, land, _, _, _, _, mine, _, chip_b, back_a = call_kernel(
            "roam", roam_kernel, cfg, [lead, tokens, grad_y, rg, *weights], [*grads, land, *sums], 4, 2,
            [dma((n_fly,)), dma((n_fly,)), dma((2,)), pltpu.VMEM((2, 2, 2 * tok // n_loc, d_model), F32), dma((2, 2)), dma((2,))],
            dict(collective_id=0, has_side_effects=True))
        back_b = lax.ppermute(chip_b, "expert", across)
        acc1, acc3, acc2 = call_kernel("rest", rest_kernel, cfg, [lead, land, *weights, *acc], grads, 6, 0, [], {})
        y_out, grad_x = last_sum(mine, back_a, back_b, tok, d_model)
        return y_out, grad_x, acc1, acc3, acc2

    return jax.shard_map(body, mesh=mesh,
                         in_specs=(row_spec, row_spec, row_spec, row_spec, w_spec, w_spec, w_spec),
                         out_specs=(row_spec, row_spec, grad_spec, grad_spec, grad_spec),
                         check_vma=False)
```

```python
import functools

import jax
import jax.numpy as jnp
from jax import lax
from jax.experimental import pallas as pl
from jax.experimental.pallas import tpu as pltpu
from jax.sharding import PartitionSpec as P

MESH = pl.DeviceIdType.MESH
BLOCKS = ("other", "far", "far_o", "z1", "z1_o", "z1y", "z1y_o", "z2", "z2_o", "z2y", "z2y_o", "z3", "z3_o", "z3y", "z3y_o")
N_HOT = 2
RG_ROWS = 16
F32, BF16 = jnp.float32, jnp.bfloat16


def caps(tok_dev, top_k, n_exp):
    cap_hot = 3 * tok_dev // 8
    cap_cold = max(8, ((tok_dev * top_k - N_HOT * cap_hot) // (n_exp - N_HOT) + 7) // 8 * 8)
    return cap_cold, cap_hot


def dot_nn(a, b):
    return lax.dot_general(a, b, (((1,), (0,)), ((), ())), preferred_element_type=F32)


def dot_nt(a, b):
    return lax.dot_general(a, b, (((1,), (1,)), ((), ())), preferred_element_type=F32)


def dot_tn(a, b):
    return lax.dot_general(a, b, (((0,), (0,)), ((), ())), preferred_element_type=F32)


def prefix(m):
    lane = lax.broadcasted_iota(jnp.int32, m.shape, 1)
    step = 1
    while step < m.shape[1]:
        m = m + jnp.where(lane >= step, pltpu.roll(m, step, 1), 0.0)
        step *= 2
    return m


class Engine:
    def __init__(self, cfg, lead, weights, bases, outs, scratch, group):
        self.__dict__.update(cfg)
        self.lead, self.weights, self.bases, self.outs, self.group = lead, weights, bases, outs, group
        (self.rows_x, self.rows_d, self.meta, self.buf, self.hid, self.dab, self.w13, self.w2, self.g13, self.g2,
         self.src_sem, self.w_sem, self.in_sem, self.out_sem) = scratch[:14]
        self.own_scratch = scratch[14:]
        hot = jnp.logical_or(lead * self.n_loc == 0, lead * self.n_loc == self.n_exp // 2)
        self.far = jnp.where(hot, float(self.cap), float(2 * self.tok))
        self.cold, self.part = self.n_loc * self.cap, group * self.cap

    def triple(self, both, single, slot):
        f = self.d_ff
        return both.at[slot, :, 0:f], both.at[slot, :, f:2 * f], single.at[slot]

    def load_w(self, e):
        slot = lax.rem(e, 2)
        return [pltpu.make_async_copy(w.at[e], b, self.w_sem.at[slot, k])
                for k, (w, b) in enumerate(zip(self.weights, self.triple(self.w13, self.w2, slot)))]

    def load_g(self, e):
        slot = lax.rem(e, 4)
        return [pltpu.make_async_copy(w.at[e], b, self.in_sem.at[slot, k])
                for k, (w, b) in enumerate(zip(self.bases, self.triple(self.g13, self.g2, slot)))]

    def save_g(self, e):
        slot = lax.rem(e, 4)
        return [pltpu.make_async_copy(b, w.at[e], self.out_sem.at[slot, k])
                for k, (w, b) in enumerate(zip(self.outs, self.triple(self.g13, self.g2, slot)))]

    def fetches(self, s, ref):
        if not isinstance(ref, tuple):
            return [pltpu.make_async_copy(ref, self.buf.at[s], self.src_sem.at[s, 0])]
        dst = self.buf.at[s]
        return [pltpu.make_async_copy(r, dst.at[pl.ds(at, r.shape[0])], self.src_sem.at[s, k])
                for k, (r, at) in enumerate(zip(ref, (0, self.tok, 2 * self.tok)))]

    def match_rows(self, src, i, base, size):
        iota = lax.broadcasted_iota(jnp.int32, (size, self.tok), 0).astype(F32) + base
        return iota == self.meta[src, pl.ds(i, 1), :]

    def ranks(self, s):
        tok = self.tok
        rg = self.buf[s, 2 * tok:2 * tok + RG_ROWS, :].astype(F32)
        routes = rg[0:8, :tok]
        gates = (rg[8:16, :tok] + rg[0:8, tok:]) + rg[8:16, tok:]
        member, weight = [], []
        for i in range(self.n_loc):
            match = routes == (self.lead * self.n_loc + i).astype(F32)
            member.append(jnp.sum(jnp.where(match, 1.0, 0.0), axis=0, keepdims=True))
            weight.append(jnp.sum(jnp.where(match, gates, 0.0), axis=0, keepdims=True))
        member = jnp.concatenate(member, axis=0)
        self.meta[s, 0:8, :] = jnp.where(member > 0.0, prefix(member) - 1.0, -1.0)
        self.meta[s, 8:16, :] = jnp.concatenate(weight, axis=0)

    def gather(self, s, which):
        tok, meta, buf = self.tok, self.meta, self.buf
        pick, gate = [], []
        for i, base, at, size in which:
            match = self.match_rows(s, i, base, size)
            pick.append(jnp.where(match, 1.0, 0.0).astype(BF16))
            gate.append(jnp.sum(jnp.where(match, meta[s, pl.ds(8 + i, 1), :], 0.0), axis=1, keepdims=True))
        pick, gate = jnp.concatenate(pick, axis=0), jnp.concatenate(gate, axis=0)
        at, size = which[0][2], pick.shape[0]
        self.rows_x[s, at:at + size, :] = dot_nn(pick, buf[s, 0:tok, :]).astype(BF16)
        self.rows_d[s, at:at + size, :] = (dot_nn(pick, buf[s, tok:2 * tok, :]) * gate).astype(BF16)

    def block(self, n_src, n_own, at, size, keep, w, g, g_in, middle=lambda: None):
        d_model, d_ff, hid, dab = self.d_model, self.d_ff, self.hid, self.dab
        w13, w2 = self.w13.at[w], self.w2.at[w]
        rows = n_src * size

        def load(ref):
            return ref[0:n_src, pl.ds(at, size), :].reshape(rows, d_model)

        ab = dot_nn(load(self.rows_x), w13[...]).astype(BF16).astype(F32)
        dh = dot_nt(load(self.rows_d), w2[...])
        a, b = ab[:, :d_ff], ab[:, d_ff:]
        sig = 0.5 * jnp.tanh(0.5 * a) + 0.5
        act = a * sig
        hid[0:rows, :] = (act * b).astype(BF16)
        dab[0:rows, 0:d_ff] = (dh * b * sig * (1.0 + a * (1.0 - sig))).astype(BF16)
        dab[0:rows, d_ff:] = (dh * act).astype(BF16)
        middle()
        if size < self.cap:
            def columns(k, carry):
                cols = pl.ds(pl.multiple_of(k * d_ff, d_ff), d_ff)
                self.g13[g, :, cols] = self.g13[g, :, cols] + dot_tn(load(self.rows_x), dab[0:rows, cols])
                self.g2[g, :, cols] = self.g2[g, :, cols] + dot_tn(hid[0:rows, :], self.rows_d[0:n_src, pl.ds(at, size), cols].reshape(rows, d_ff))
                return carry

            lax.fori_loop(0, 2, columns, 0)
        else:
            for out, lhs, rhs in ((self.g13, load(self.rows_x), dab[0:rows, :]), (self.g2, hid[0:rows, :], load(self.rows_d))):
                if g_in:
                    out[g] = out[g] + dot_tn(lhs, rhs)
                else:
                    out[g] = dot_tn(lhs, rhs)
        if n_own:
            kept_o, kept_x = self.own_scratch[:2]
            m = n_own * size
            o = dot_nn(hid[0:m, :], w2[...]).astype(BF16)
            dx = dot_nt(dab[0:m, :], w13[...]).astype(BF16)
            kept_o[:, pl.ds(keep, size), :] = o.reshape(n_own, size, d_model)
            kept_x[:, pl.ds(keep, size), :] = dx.reshape(n_own, size, d_model)

    def stage(self, srcs, n_own, first, last, before, held, events, ship, each=None, prelude=lambda: None):
        n_src, n_loc, cap, group = len(srcs), self.n_loc, self.cap, self.group
        width = 1 if n_src == 2 else 2
        turns = n_src // width
        fetch = [self.fetches(s, r) for s, r in enumerate(srcs)]

        def ask(t):
            for s in range(t, n_src, turns):
                before[s]()
                start(fetch[s])

        eager = all(b is nothing for b in before)
        for t in range(turns if eager else 1):
            ask(t)
        prelude()

        def wave(p, carry):
            def turn(t, carry):
                some = [t + j * turns for j in range(width)]

                @pl.when(p == 0)
                def _():
                    for k in range(turns):
                        @pl.when(t == k)
                        def _(k=k):
                            for s in range(k, n_src, turns):
                                wait(fetch[s])
                    for s in some:
                        self.ranks(s)
                        self.gather(s, [(0, self.far, self.part, self.extra)])
                    for k in range(0 if eager or width == 1 else turns - 1):
                        @pl.when(t == k)
                        def _(k=k):
                            ask(k + 1)

                for s in some:
                    self.gather(s, [(group * p + i, 0.0, i * cap, cap) for i in range(group)])
                if width == 1 and not eager:
                    for k in range(turns - 1):
                        @pl.when(jnp.logical_and(p == 0, t == k))
                        def _(k=k):
                            ask(k + 1)
                return carry

            lax.fori_loop(0, turns, turn, 0)

            def one(i, carry):
                e = group * p + i
                wait(self.load_w(e))
                if last:
                    @pl.when(e + 1 < n_loc)
                    def _():
                        start(self.load_w(e + 1))
                else:
                    start(self.load_w(lax.rem(e + 1, n_loc)))

                def middle():
                    @pl.when(e >= 2)
                    def _():
                        wait(self.save_g(e - 2))

                    for k, copies in enumerate(held):
                        @pl.when(e == k)
                        def _(copies=copies):
                            wait(copies)

                    if first:
                        @pl.when(e + 2 >= n_loc)
                        def _():
                            start(self.load_g(e + 2 - n_loc))
                    elif last:
                        @pl.when(e + 2 < n_loc)
                        def _():
                            start(self.load_g(e + 2))
                    else:
                        start(self.load_g(lax.rem(e + 2, n_loc)))
                    if not first:
                        wait(self.load_g(e))

                self.block(n_src, n_own, pl.multiple_of(i * cap, cap), cap, pl.multiple_of(e * cap, cap),
                           lax.rem(e, 2), lax.rem(e, 4), not first, middle)

                @pl.when(e == 0)
                def more():
                    self.block(n_src, n_own, self.part, self.extra, self.cold, 0, 0, True)

                start(self.save_g(e))
                for k, event in events:
                    @pl.when(e == k)
                    def _(event=event):
                        event()
                if each is not None:
                    each(e)
                return carry

            lax.fori_loop(0, group, one, 0)
            return carry

        lax.fori_loop(0, n_loc // group, wave, 0)
        if n_own:
            self.combine(n_own, ship)
        elif last:
            wait(self.save_g(n_loc - 2))
            wait(self.save_g(n_loc - 1))

    def combine(self, n_own, ship):
        kept_o, kept_x = self.own_scratch[:2]
        cold, extra, cap, tok, n_loc = self.cold, self.extra, self.cap, self.tok, self.n_loc
        part, n_blk = self.part, n_loc // self.group
        pieces = [(i, 0.0, i // self.group, i % self.group * cap, cap) for i in range(n_loc)] + [(0, self.far, None, part, extra)]
        places = [(ref, pl.ds(lane * tok, tok)) for ref in (self.rows_x, self.rows_d) for lane in (0, 1)]

        def one(src, carry):
            for s in range(n_own):
                @pl.when(src == s)
                def _(s=s):
                    wait(self.save_g(n_loc - 2 + s))

            for i, base, blk, at, size in pieces:
                match = self.match_rows(src, i, base, size)
                gate = self.meta[src, 8 + i:9 + i, :]
                hi = gate.astype(BF16).astype(F32)
                mid = (gate - hi).astype(BF16).astype(F32)
                low = gate - hi - mid
                for k, v in enumerate((hi, mid, low, 1.0)):
                    ref, lanes = places[0 if blk is None else k]
                    ref[k if blk is None else blk, at:at + size, lanes] = jnp.where(match, v, 0.0).astype(BF16)

            def chosen(k):
                ref, lanes = places[k]
                return ref[0:n_blk, 0:part, lanes].reshape(cold, tok)

            spare, lanes = places[0]
            wide = self.d_model // 2

            def columns(h, carry):
                cols = pl.ds(pl.multiple_of(h * wide, wide), wide)
                o, rest = kept_o[src, 0:cold, cols], kept_o[src, cold:cold + extra, cols]
                y = dot_tn(chosen(0), o) + dot_tn(chosen(1), o) + dot_tn(chosen(2), o)
                gates = spare[0:3, part:part + extra, lanes].reshape(3 * extra, tok)
                self.g13[2 + src, 0:tok, cols] = y + dot_tn(gates, jnp.concatenate([rest] * 3, axis=0))
                dx = dot_tn(chosen(3), kept_x[src, 0:cold, cols])
                gates = spare[3, part:part + extra, lanes]
                self.g13[2 + src, tok:2 * tok, cols] = dx + dot_tn(gates, kept_x[src, cold:cold + extra, cols])
                return carry

            lax.fori_loop(0, 2, columns, 0)
            for s in range(n_own):
                @pl.when(src == s)
                def _(s=s):
                    ship[s].start()
            return carry

        lax.fori_loop(0, n_own, one, 0)


def start(copies):
    for c in copies:
        c.start()


def wait(copies):
    for c in copies:
        c.wait()


def nothing():
    pass


class Adder:
    def __init__(self, a, b, out, held, load_sem, save_sem, ready):
        self.a, self.b, self.out, self.held, self.load_sem, self.save_sem, self.ready = a, b, out, held, load_sem, save_sem, ready
        self.rows = held.shape[2]
        self.n_head = out[0].shape[0] // self.rows if out[0] is not None else 0

    def loads(self, k):
        slot, at = lax.rem(k, 2), pl.ds(pl.multiple_of(k * self.rows, self.rows), self.rows)
        return [pltpu.make_async_copy(v.at[at], self.held.at[slot, n], self.load_sem.at[slot, n]) for n, v in enumerate((self.a, self.b))]

    def save(self, k, head=False):
        slot = lax.rem(k, 2)
        ref, k = (self.out[0], k) if head else (self.out[1], k - self.n_head)
        at = pl.ds(pl.multiple_of(k * self.rows, self.rows), self.rows)
        return pltpu.make_async_copy(self.held.at[slot, 0], ref.at[at], self.save_sem.at[slot])

    def add(self, k):
        wait(self.loads(k))
        slot = lax.rem(k, 2)
        self.held[slot, 0] = self.held[slot, 0] + self.held[slot, 1]
        if self.n_head:
            @pl.when(k < self.n_head)
            def _():
                self.save(k, True).start()

        @pl.when(k >= self.n_head)
        def _():
            self.save(k).start()

    def saved(self, k):
        if self.n_head:
            @pl.when(k < self.n_head)
            def _():
                self.save(k, True).wait()

        @pl.when(k >= self.n_head)
        def _():
            self.save(k).wait()

    def __call__(self, e):
        @pl.when(e == 0)
        def _():
            self.ready()

        @pl.when(e >= 1)
        def _():
            self.add(e - 1)

        @pl.when(e >= 2)
        def _():
            self.saved(e - 2)

        start(self.loads(e))

    def finish(self, last):
        self.add(last)
        self.saved(last - 1)
        self.saved(last)


def roam_kernel(cfg, lead_ref, tokens, grad_y, rg, w1, w3, w2, g1, g3, g2, land, own_a, own_b, got_a, got_b, mine, chip_a, chip_b, back_a, *scratch):
    send_sem, recv_sem, part_sem, held, add_in_sem, add_out_sem = scratch[-6:]
    eng = Engine(cfg, lead_ref[0, 0], (w1, w3, w2), (g1, g3, g2), (g1, g3, g2), scratch[:-6], 2)
    q, r = lax.axis_index("data"), lax.axis_index("expert")
    n_data, n_er, tok, n_loc = cfg["n_data"], cfg["n_er"], cfg["tok"], cfg["n_loc"]
    partner = {"expert": r + 1 - 2 * lax.rem(r, 2)}
    across = {"expert": lax.rem(r + n_er // 2, n_er)}
    znext = {"data": lax.rem(q + 1, n_data)}
    zprev = {"data": lax.rem(q + n_data - 1, n_data)}

    def at(name, rows=None):
        ref = land.at[BLOCKS.index(name)]
        return ref if rows is None else ref.at[rows]

    flights = []

    def remote(src, dst, device):
        k = len(flights)
        copy = pltpu.make_async_remote_copy(src_ref=src, dst_ref=dst, send_sem=send_sem.at[k], recv_sem=recv_sem.at[k],
                                            device_id=device, device_id_type=MESH)
        flights.append(copy)
        return copy

    def first(name, device):
        parts = ((tokens, 0, tok), (grad_y, tok, tok), (rg, 2 * tok, RG_ROWS))
        return [remote(v, at(name, pl.ds(lo, n)), device) for v, lo, n in parts]

    def onward(src, dst, device):
        return [remote(at(src), at(dst), device)]

    cut = (2 * tok + RG_ROWS) // 64 * 48
    upper, lower = pl.ds(0, cut), pl.ds(cut, 2 * tok + RG_ROWS - cut)
    c_back = [remote(chip_a, back_a, across)]
    c_other, c_far, c_z1 = first("other", partner), first("far", across), first("z1", znext)
    c_far_o, c_z1_o = onward("far", "far_o", partner), onward("z1", "z1_o", partner)
    c_z1y, c_z2 = onward("z1", "z1y", across), onward("z1", "z2", znext)
    c_z1y_o, c_z2_o = onward("z1y", "z1y_o", partner), onward("z2", "z2_o", partner)
    c_z2y, c_z3 = onward("z2", "z2y", across), onward("z2", "z3", znext)
    c_z2y_o, c_z3_o = onward("z2y", "z2y_o", partner), onward("z3", "z3_o", partner)
    c_z3y_z = [remote(at("far", upper), at("z3y", upper), zprev)]
    c_z3y_y = [remote(at("z3", lower), at("z3y", lower), across)]
    c_z3y_zo = [remote(at("z3y", upper), at("z3y_o", upper), partner)]
    c_z3y_yo = [remote(at("z3y", lower), at("z3y_o", lower), partner)]
    c_got_a, c_got_b = [remote(eng.g13.at[3], got_a, partner)], [remote(eng.g13.at[3], got_b, partner)]
    keep_a = pltpu.make_async_copy(eng.g13.at[2], own_a, part_sem.at[0])
    keep_b = pltpu.make_async_copy(eng.g13.at[2], own_b, part_sem.at[1])

    barrier = pltpu.get_barrier_semaphore()
    for device in (partner, across, znext, zprev):
        pl.semaphore_signal(barrier, inc=1, device_id=device, device_id_type=MESH)
    pl.semaphore_wait(barrier, 4)

    class Sent:
        def __init__(self, copy):
            self.copy = copy

        def wait(self):
            self.copy.wait_send()

    def arrived(copies, then=()):
        def event():
            for c in copies:
                c.wait_recv()
            start(then)
        return event

    start(c_other + c_far + c_z1)
    eng.stage([(tokens, grad_y, rg), at("other")], 2, True, False, [nothing, arrived(c_other)], (), (), [keep_a, c_got_a[0]],
              prelude=lambda: start(eng.load_w(0)))
    sum_a = Adder(own_a, got_a, (None, mine), held, add_in_sem, add_out_sem, arrived(c_got_a))
    eng.stage([at("far"), at("far_o"), at("z1"), at("z1_o")], 2, False, False,
              [arrived(c_far, c_far_o), arrived(c_far_o), arrived(c_z1, c_z1_o + c_z1y + c_z2), arrived(c_z1_o)],
              ([keep_a], [Sent(c_got_a[0])]),
              ((4, arrived(c_z1y + c_z2, c_z2y + c_z3 + c_z1y_o + c_z2_o)),),
              [keep_b, c_got_b[0]], sum_a)
    sum_a.finish(n_loc - 1)
    sum_b = Adder(own_b, got_b, (chip_a, chip_b), held, add_in_sem, add_out_sem, arrived(c_got_b))
    eng.stage([at("z1y"), at("z1y_o"), at("z2"), at("z2_o")], 0, False, True,
              [nothing, arrived(c_z1y_o), nothing, arrived(c_z2_o)],
              ([keep_b], [Sent(c_got_b[0])]),
              ((0, arrived(c_z2y + c_z3, c_z3y_y + c_z3y_z + c_z2y_o + c_z3_o)), (4, lambda: start(c_back)), (6, arrived(c_z3y_y, c_z3y_yo))), (), sum_b)
    sum_b.finish(n_loc - 1)
    arrived(c_z3y_z, c_z3y_zo)()
    arrived(c_z2y_o + c_z3_o + c_z3y_zo + c_z3y_yo + c_back)()
    for c in flights:
        if c is not c_got_a[0] and c is not c_got_b[0]:
            c.wait_send()


def rest_kernel(cfg, lead_ref, land, w1, w3, w2, b1, b3, b2, g1, g3, g2, *scratch):
    eng = Engine(cfg, lead_ref[0, 0], (w1, w3, w2), (b1, b3, b2), (g1, g3, g2), scratch, 2)

    def prelude():
        start(eng.load_w(0))
        for e in (0, 1):
            start(eng.load_g(e))

    names = ("z2y", "z2y_o", "z3", "z3_o", "z3y", "z3y_o")
    eng.stage([land.at[BLOCKS.index(n)] for n in names], 0, False, True, [nothing] * 6, (), (), (), prelude=prelude)


def call_kernel(name, kernel, cfg, args, shapes, n_src, n_own, extra_scratch, params):
    tok, d_model, d_ff, n_loc, cap, extra = (cfg[k] for k in ("tok", "d_model", "d_ff", "n_loc", "cap", "extra"))
    rows = n_loc * cap + extra
    scratch = [pltpu.VMEM((n_src, 2 * cap + extra, d_model), BF16)] * 2 + [
        pltpu.VMEM((n_src, 16, tok), F32),
        pltpu.VMEM((n_src, 2 * tok + RG_ROWS, d_model), BF16),
        pltpu.VMEM((n_src * cap, d_ff), BF16),
        pltpu.VMEM((n_src * cap, 2 * d_ff), BF16),
    ]
    for slots, kind in ((2, BF16), (4, F32)):
        scratch += [pltpu.VMEM((slots, d_model, 2 * d_ff), kind), pltpu.VMEM((slots, d_ff, d_model), kind)]
    scratch += [pltpu.SemaphoreType.DMA(n) for n in ((n_src, 3), (2, 3), (4, 3), (4, 3))]
    if n_own:
        scratch += [pltpu.VMEM((n_own, rows, d_model), BF16)] * 2
    unit = 2 * d_model * d_ff * rows
    return pl.pallas_call(
        functools.partial(kernel, cfg),
        in_specs=[pl.BlockSpec(memory_space=pltpu.SMEM)] + [pl.BlockSpec(memory_space=pl.ANY)] * (len(args) - 1),
        out_specs=[pl.BlockSpec(memory_space=pl.ANY)] * len(shapes),
        out_shape=shapes,
        scratch_shapes=scratch + extra_scratch,
        compiler_params=pltpu.CompilerParams(vmem_limit_bytes=67_000_000, **params),
        cost_estimate=pl.CostEstimate(flops=unit * (8 * n_src + 7 * n_own) // 8, bytes_accessed=100 << 20, transcendentals=0),
        name=name,
    )(*args)


def last_sum(mine, back_a, back_b, tok, d_model):
    rows = back_a.shape[0] // 2
    n_all, n_half = 2 * tok // rows, tok // rows

    def kernel(m_ref, a_ref, b_ref, y_ref, x_ref, m, v, out, in_sem, out_sem):
        def piece(ref, j):
            return ref.at[pl.ds(j * rows, rows)]

        loads, saves = [], []
        for j in range(n_all):
            other = piece(a_ref, j) if j < 2 else piece(b_ref, j - 2)
            loads.append([pltpu.make_async_copy(piece(m_ref, j), m.at[j], in_sem.at[j, 0]),
                          pltpu.make_async_copy(other, v.at[j], in_sem.at[j, 1])])
            place = piece(y_ref, j) if j < n_half else piece(x_ref, j - n_half)
            saves.append(pltpu.make_async_copy(out.at[j], place, out_sem.at[j]))
        for copies in loads:
            start(copies)
        for j in range(n_all):
            wait(loads[j])
            out[j] = (m[j] + v[j]).astype(BF16)
            saves[j].start()
        wait(saves)

    dma = pltpu.SemaphoreType.DMA
    return pl.pallas_call(
        kernel,
        in_specs=[pl.BlockSpec(memory_space=pl.ANY)] * 3,
        out_specs=[pl.BlockSpec(memory_space=pl.ANY)] * 2,
        out_shape=[jax.ShapeDtypeStruct((tok, d_model), BF16)] * 2,
        scratch_shapes=[pltpu.VMEM((n_all, rows, d_model), F32)] * 2 + [pltpu.VMEM((n_all, rows, d_model), BF16), dma((n_all, 2)), dma((n_all,))],
        compiler_params=pltpu.CompilerParams(vmem_limit_bytes=67_000_000),
        name="last",
    )(mine, back_a, back_b)


def solution(mesh):
    n_data, n_er = mesh.shape["data"], mesh.shape["expert"]
    row_spec = P(("pod", "data", "expert"), None)
    w_spec = P("expert", None, None)
    grad_spec = P(("pod", "expert"), None, None)
    across = [(r, r ^ 2) for r in range(n_er)]

    def body(tokens, routes, gates, grad_y, w_in1, w_in3, w_out):
        n_loc, d_model, d_ff = w_in1.shape
        n_exp, tok = n_loc * n_er, tokens.shape[0]
        cap, cap_hot = caps(tok, routes.shape[1], n_exp)
        cfg = dict(tok=tok, d_model=d_model, d_ff=d_ff, n_loc=n_loc, n_exp=n_exp, cap=cap, extra=cap_hot - cap,
                   n_data=n_data, n_er=n_er)
        lead = lax.axis_index("expert").astype(jnp.int32).reshape(1, 1)
        gate = gates.T
        hi = lax.reduce_precision(gate, 8, 7)
        mid = lax.reduce_precision(gate - hi, 8, 7)
        low = gate - hi - mid
        rg = jnp.concatenate([jnp.concatenate([routes.T.astype(F32), hi], 0), jnp.concatenate([mid, low], 0)], 1).astype(BF16)
        weights = (w_in1, w_in3, w_out)
        grads = [jax.ShapeDtypeStruct(w.shape, F32) for w in weights]
        sums = [jax.ShapeDtypeStruct((2 * tok, d_model), F32)] * 6
        land = jax.ShapeDtypeStruct((len(BLOCKS), 2 * tok + RG_ROWS, d_model), BF16)
        dma, n_fly, quarter = pltpu.SemaphoreType.DMA, 28, 2 * (2 * tok // n_loc)
        sums[5:] = [jax.ShapeDtypeStruct((n, d_model), F32) for n in (quarter, 2 * tok - quarter, quarter)]
        *acc, land, _, _, _, _, mine, _, chip_b, back_a = call_kernel(
            "roam", roam_kernel, cfg, [lead, tokens, grad_y, rg, *weights], [*grads, land, *sums], 4, 2,
            [dma((n_fly,)), dma((n_fly,)), dma((2,)), pltpu.VMEM((2, 2, 2 * tok // n_loc, d_model), F32), dma((2, 2)), dma((2,))],
            dict(collective_id=0, has_side_effects=True))
        back_b = lax.ppermute(chip_b, "expert", across)
        acc1, acc3, acc2 = call_kernel("rest", rest_kernel, cfg, [lead, land, *weights, *acc], grads, 6, 0, [], {})
        y_out, grad_x = last_sum(mine, back_a, back_b, tok, d_model)
        return y_out, grad_x, acc1, acc3, acc2

    return jax.shard_map(body, mesh=mesh,
                         in_specs=(row_spec, row_spec, row_spec, row_spec, w_spec, w_spec, w_spec),
                         out_specs=(row_spec, row_spec, grad_spec, grad_spec, grad_spec),
                         check_vma=False)
```

```python
import functools

import jax
import jax.numpy as jnp
from jax import lax
from jax.experimental import pallas as pl
from jax.experimental.pallas import tpu as pltpu
from jax.sharding import PartitionSpec as P

MESH = pl.DeviceIdType.MESH
BLOCKS = ("other", "far", "far_o", "z1", "z1_o", "z1y", "z1y_o", "z2", "z2_o", "z2y", "z2y_o", "z3", "z3_o", "z3y", "z3y_o")
N_HOT = 2
RG_ROWS = 16
F32, BF16 = jnp.float32, jnp.bfloat16


def caps(tok_dev, top_k, n_exp):
    cap_hot = 3 * tok_dev // 8
    cap_cold = max(8, ((tok_dev * top_k - N_HOT * cap_hot) // (n_exp - N_HOT) + 7) // 8 * 8)
    return cap_cold, cap_hot


def dot_nn(a, b):
    return lax.dot_general(a, b, (((1,), (0,)), ((), ())), preferred_element_type=F32)


def dot_nt(a, b):
    return lax.dot_general(a, b, (((1,), (1,)), ((), ())), preferred_element_type=F32)


def dot_tn(a, b):
    return lax.dot_general(a, b, (((0,), (0,)), ((), ())), preferred_element_type=F32)


def prefix(m):
    lane = lax.broadcasted_iota(jnp.int32, m.shape, 1)
    step = 1
    while step < m.shape[1]:
        m = m + jnp.where(lane >= step, pltpu.roll(m, step, 1), 0.0)
        step *= 2
    return m


class Engine:
    def __init__(self, cfg, lead, weights, bases, outs, scratch, group):
        self.__dict__.update(cfg)
        self.lead, self.weights, self.bases, self.outs, self.group = lead, weights, bases, outs, group
        (self.rows_x, self.rows_d, self.meta, self.buf, self.hid, self.dab, self.w13, self.w2, self.g13, self.g2,
         self.src_sem, self.w_sem, self.in_sem, self.out_sem) = scratch[:14]
        self.own_scratch = scratch[14:]
        hot = jnp.logical_or(lead * self.n_loc == 0, lead * self.n_loc == self.n_exp // 2)
        self.far = jnp.where(hot, float(self.cap), float(2 * self.tok))
        self.cold, self.part = self.n_loc * self.cap, group * self.cap

    def triple(self, both, single, slot):
        f = self.d_ff
        return both.at[slot, :, 0:f], both.at[slot, :, f:2 * f], single.at[slot]

    def load_w(self, e):
        slot = lax.rem(e, 2)
        return [pltpu.make_async_copy(w.at[e], b, self.w_sem.at[slot, k])
                for k, (w, b) in enumerate(zip(self.weights, self.triple(self.w13, self.w2, slot)))]

    def load_g(self, e):
        slot = lax.rem(e, 4)
        return [pltpu.make_async_copy(w.at[e], b, self.in_sem.at[slot, k])
                for k, (w, b) in enumerate(zip(self.bases, self.triple(self.g13, self.g2, slot)))]

    def save_g(self, e):
        slot = lax.rem(e, 4)
        return [pltpu.make_async_copy(b, w.at[e], self.out_sem.at[slot, k])
                for k, (w, b) in enumerate(zip(self.outs, self.triple(self.g13, self.g2, slot)))]

    def fetches(self, s, ref):
        if not isinstance(ref, tuple):
            return [pltpu.make_async_copy(ref, self.buf.at[s], self.src_sem.at[s, 0])]
        dst = self.buf.at[s]
        return [pltpu.make_async_copy(r, dst.at[pl.ds(at, r.shape[0])], self.src_sem.at[s, k])
                for k, (r, at) in enumerate(zip(ref, (0, self.tok, 2 * self.tok)))]

    def match_rows(self, src, i, base, size):
        iota = lax.broadcasted_iota(jnp.int32, (size, self.tok), 0).astype(F32) + base
        return iota == self.meta[src, pl.ds(i, 1), :]

    def ranks(self, s):
        tok = self.tok
        rg = self.buf[s, 2 * tok:2 * tok + RG_ROWS, :].astype(F32)
        routes = rg[0:8, :tok]
        gates = (rg[8:16, :tok] + rg[0:8, tok:]) + rg[8:16, tok:]
        member, weight = [], []
        for i in range(self.n_loc):
            match = routes == (self.lead * self.n_loc + i).astype(F32)
            member.append(jnp.sum(jnp.where(match, 1.0, 0.0), axis=0, keepdims=True))
            weight.append(jnp.sum(jnp.where(match, gates, 0.0), axis=0, keepdims=True))
        member = jnp.concatenate(member, axis=0)
        self.meta[s, 0:8, :] = jnp.where(member > 0.0, prefix(member) - 1.0, -1.0)
        self.meta[s, 8:16, :] = jnp.concatenate(weight, axis=0)

    def gather(self, s, which):
        tok, meta, buf = self.tok, self.meta, self.buf
        pick, gate = [], []
        for i, base, at, size in which:
            match = self.match_rows(s, i, base, size)
            pick.append(jnp.where(match, 1.0, 0.0).astype(BF16))
            gate.append(jnp.sum(jnp.where(match, meta[s, pl.ds(8 + i, 1), :], 0.0), axis=1, keepdims=True))
        pick, gate = jnp.concatenate(pick, axis=0), jnp.concatenate(gate, axis=0)
        at, size = which[0][2], pick.shape[0]
        self.rows_x[s, at:at + size, :] = dot_nn(pick, buf[s, 0:tok, :]).astype(BF16)
        self.rows_d[s, at:at + size, :] = (dot_nn(pick, buf[s, tok:2 * tok, :]) * gate).astype(BF16)

    def block(self, n_src, n_own, at, size, keep, w, g, g_in, middle=lambda: None):
        d_model, d_ff, hid, dab = self.d_model, self.d_ff, self.hid, self.dab
        w13, w2 = self.w13.at[w], self.w2.at[w]
        rows = n_src * size

        def load(ref):
            return ref[0:n_src, pl.ds(at, size), :].reshape(rows, d_model)

        ab = dot_nn(load(self.rows_x), w13[...]).astype(BF16).astype(F32)
        dh = dot_nt(load(self.rows_d), w2[...])
        a, b = ab[:, :d_ff], ab[:, d_ff:]
        sig = 0.5 * jnp.tanh(0.5 * a) + 0.5
        act = a * sig
        hid[0:rows, :] = (act * b).astype(BF16)
        dab[0:rows, 0:d_ff] = (dh * b * sig * (1.0 + a * (1.0 - sig))).astype(BF16)
        dab[0:rows, d_ff:] = (dh * act).astype(BF16)
        middle()
        if size < self.cap:
            def columns(k, carry):
                cols = pl.ds(pl.multiple_of(k * d_ff, d_ff), d_ff)
                self.g13[g, :, cols] = self.g13[g, :, cols] + dot_tn(load(self.rows_x), dab[0:rows, cols])
                self.g2[g, :, cols] = self.g2[g, :, cols] + dot_tn(hid[0:rows, :], self.rows_d[0:n_src, pl.ds(at, size), cols].reshape(rows, d_ff))
                return carry

            lax.fori_loop(0, 2, columns, 0)
        else:
            for out, lhs, rhs in ((self.g13, load(self.rows_x), dab[0:rows, :]), (self.g2, hid[0:rows, :], load(self.rows_d))):
                if g_in:
                    out[g] = out[g] + dot_tn(lhs, rhs)
                else:
                    out[g] = dot_tn(lhs, rhs)
        if n_own:
            kept_o, kept_x = self.own_scratch[:2]
            m = n_own * size
            o = dot_nn(hid[0:m, :], w2[...]).astype(BF16)
            dx = dot_nt(dab[0:m, :], w13[...]).astype(BF16)
            kept_o[:, pl.ds(keep, size), :] = o.reshape(n_own, size, d_model)
            kept_x[:, pl.ds(keep, size), :] = dx.reshape(n_own, size, d_model)

    def stage(self, srcs, n_own, first, last, before, held, events, ship, each=None, prelude=lambda: None):
        n_src, n_loc, cap, group = len(srcs), self.n_loc, self.cap, self.group
        width = 1 if n_src == 2 else 2
        turns = n_src // width
        fetch = [self.fetches(s, r) for s, r in enumerate(srcs)]

        def ask(t):
            for s in range(t, n_src, turns):
                before[s]()
                start(fetch[s])

        eager = all(b is nothing for b in before)
        for t in range(turns if eager else 1):
            ask(t)
        prelude()
        if held:
            wait(held[0])
            start(self.load_g(2))

        def wave(p, carry):
            def turn(t, carry):
                some = [t + j * turns for j in range(width)]

                @pl.when(p == 0)
                def _():
                    for k in range(turns):
                        @pl.when(t == k)
                        def _(k=k):
                            for s in range(k, n_src, turns):
                                wait(fetch[s])
                    for s in some:
                        self.ranks(s)
                        self.gather(s, [(0, self.far, self.part, self.extra)])
                    for k in range(0 if eager or width == 1 else turns - 1):
                        @pl.when(t == k)
                        def _(k=k):
                            ask(k + 1)

                for s in some:
                    self.gather(s, [(group * p + i, 0.0, i * cap, cap) for i in range(group)])
                if width == 1 and not eager:
                    for k in range(turns - 1):
                        @pl.when(jnp.logical_and(p == 0, t == k))
                        def _(k=k):
                            ask(k + 1)
                return carry

            lax.fori_loop(0, turns, turn, 0)

            def one(i, carry):
                e = group * p + i
                wait(self.load_w(e))
                if last:
                    @pl.when(e + 1 < n_loc)
                    def _():
                        start(self.load_w(e + 1))
                else:
                    start(self.load_w(lax.rem(e + 1, n_loc)))

                def middle():
                    @pl.when(e >= 2)
                    def _():
                        wait(self.save_g(e - 2))

                    if held:
                        @pl.when(e == 0)
                        def _():
                            wait(held[1])
                            start(self.load_g(3))

                    if first:
                        @pl.when(e + 2 >= n_loc)
                        def _():
                            start(self.load_g(e + 2 - n_loc))
                    else:
                        @pl.when(jnp.logical_and(e >= 2, e + 2 < n_loc))
                        def _():
                            start(self.load_g(e + 2))

                        if not last:
                            @pl.when(e + 2 >= n_loc)
                            def _():
                                start(self.load_g(e + 2 - n_loc))
                    if not first:
                        wait(self.load_g(e))

                self.block(n_src, n_own, pl.multiple_of(i * cap, cap), cap, pl.multiple_of(e * cap, cap),
                           lax.rem(e, 2), lax.rem(e, 4), not first, middle)

                @pl.when(e == 0)
                def more():
                    self.block(n_src, n_own, self.part, self.extra, self.cold, 0, 0, True)

                start(self.save_g(e))
                for k, event in events:
                    @pl.when(e == k)
                    def _(event=event):
                        event()
                if each is not None:
                    each(e)
                return carry

            lax.fori_loop(0, group, one, 0)
            return carry

        lax.fori_loop(0, n_loc // group, wave, 0)
        if n_own:
            self.combine(n_own, ship)
        elif last:
            wait(self.save_g(n_loc - 2))
            wait(self.save_g(n_loc - 1))

    def combine(self, n_own, ship):
        kept_o, kept_x = self.own_scratch[:2]
        cold, extra, cap, tok, n_loc = self.cold, self.extra, self.cap, self.tok, self.n_loc
        part, n_blk = self.part, n_loc // self.group
        pieces = [(i, 0.0, i // self.group, i % self.group * cap, cap) for i in range(n_loc)] + [(0, self.far, None, part, extra)]
        places = [(ref, pl.ds(lane * tok, tok)) for ref in (self.rows_x, self.rows_d) for lane in (0, 1)]

        def one(src, carry):
            for s in range(n_own):
                @pl.when(src == s)
                def _(s=s):
                    wait(self.save_g(n_loc - 2 + s))

            for i, base, blk, at, size in pieces:
                match = self.match_rows(src, i, base, size)
                gate = self.meta[src, 8 + i:9 + i, :]
                hi = gate.astype(BF16).astype(F32)
                mid = (gate - hi).astype(BF16).astype(F32)
                low = gate - hi - mid
                for k, v in enumerate((hi, mid, low, 1.0)):
                    ref, lanes = places[0 if blk is None else k]
                    ref[k if blk is None else blk, at:at + size, lanes] = jnp.where(match, v, 0.0).astype(BF16)

            def chosen(k):
                ref, lanes = places[k]
                return ref[0:n_blk, 0:part, lanes].reshape(cold, tok)

            spare, lanes = places[0]
            wide = self.d_model // 2

            def columns(h, carry):
                cols = pl.ds(pl.multiple_of(h * wide, wide), wide)
                o, rest = kept_o[src, 0:cold, cols], kept_o[src, cold:cold + extra, cols]
                y = dot_tn(chosen(0), o) + dot_tn(chosen(1), o) + dot_tn(chosen(2), o)
                gates = spare[0:3, part:part + extra, lanes].reshape(3 * extra, tok)
                self.g13[2 + src, 0:tok, cols] = y + dot_tn(gates, jnp.concatenate([rest] * 3, axis=0))
                dx = dot_tn(chosen(3), kept_x[src, 0:cold, cols])
                gates = spare[3, part:part + extra, lanes]
                self.g13[2 + src, tok:2 * tok, cols] = dx + dot_tn(gates, kept_x[src, cold:cold + extra, cols])
                return carry

            lax.fori_loop(0, 2, columns, 0)
            for s in range(n_own):
                @pl.when(src == s)
                def _(s=s):
                    ship[s].start()
            return carry

        lax.fori_loop(0, n_own, one, 0)


def start(copies):
    for c in copies:
        c.start()


def wait(copies):
    for c in copies:
        c.wait()


def nothing():
    pass


class Adder:
    def __init__(self, a, b, out, held, load_sem, save_sem, ready):
        self.a, self.b, self.out, self.held, self.load_sem, self.save_sem, self.ready = a, b, out, held, load_sem, save_sem, ready
        self.rows = held.shape[2]
        self.n_head = out[0].shape[0] // self.rows if out[0] is not None else 0

    def loads(self, k):
        slot, at = lax.rem(k, 2), pl.ds(pl.multiple_of(k * self.rows, self.rows), self.rows)
        return [pltpu.make_async_copy(v.at[at], self.held.at[slot, n], self.load_sem.at[slot, n]) for n, v in enumerate((self.a, self.b))]

    def save(self, k, head=False):
        slot = lax.rem(k, 2)
        ref, k = (self.out[0], k) if head else (self.out[1], k - self.n_head)
        at = pl.ds(pl.multiple_of(k * self.rows, self.rows), self.rows)
        return pltpu.make_async_copy(self.held.at[slot, 0], ref.at[at], self.save_sem.at[slot])

    def add(self, k):
        wait(self.loads(k))
        slot = lax.rem(k, 2)
        self.held[slot, 0] = self.held[slot, 0] + self.held[slot, 1]
        if self.n_head:
            @pl.when(k < self.n_head)
            def _():
                self.save(k, True).start()

        @pl.when(k >= self.n_head)
        def _():
            self.save(k).start()

    def saved(self, k):
        if self.n_head:
            @pl.when(k < self.n_head)
            def _():
                self.save(k, True).wait()

        @pl.when(k >= self.n_head)
        def _():
            self.save(k).wait()

    def __call__(self, e):
        @pl.when(e == 0)
        def _():
            self.ready()

        @pl.when(e >= 1)
        def _():
            self.add(e - 1)

        @pl.when(e >= 2)
        def _():
            self.saved(e - 2)

        start(self.loads(e))

    def finish(self, last):
        self.add(last)
        self.saved(last - 1)
        self.saved(last)


def roam_kernel(cfg, lead_ref, tokens, grad_y, rg, w1, w3, w2, g1, g3, g2, land, own_a, own_b, got_a, got_b, mine, chip_a, chip_b, back_a, *scratch):
    send_sem, recv_sem, part_sem, held, add_in_sem, add_out_sem = scratch[-6:]
    eng = Engine(cfg, lead_ref[0, 0], (w1, w3, w2), (g1, g3, g2), (g1, g3, g2), scratch[:-6], 2)
    q, r = lax.axis_index("data"), lax.axis_index("expert")
    n_data, n_er, tok, n_loc = cfg["n_data"], cfg["n_er"], cfg["tok"], cfg["n_loc"]
    partner = {"expert": r + 1 - 2 * lax.rem(r, 2)}
    across = {"expert": lax.rem(r + n_er // 2, n_er)}
    znext = {"data": lax.rem(q + 1, n_data)}
    zprev = {"data": lax.rem(q + n_data - 1, n_data)}

    def at(name, rows=None):
        ref = land.at[BLOCKS.index(name)]
        return ref if rows is None else ref.at[rows]

    flights = []

    def remote(src, dst, device):
        k = len(flights)
        copy = pltpu.make_async_remote_copy(src_ref=src, dst_ref=dst, send_sem=send_sem.at[k], recv_sem=recv_sem.at[k],
                                            device_id=device, device_id_type=MESH)
        flights.append(copy)
        return copy

    def first(name, device):
        parts = ((tokens, 0, tok), (grad_y, tok, tok), (rg, 2 * tok, RG_ROWS))
        return [remote(v, at(name, pl.ds(lo, n)), device) for v, lo, n in parts]

    def onward(src, dst, device):
        return [remote(at(src), at(dst), device)]

    cut = (2 * tok + RG_ROWS) // 64 * 48
    upper, lower = pl.ds(0, cut), pl.ds(cut, 2 * tok + RG_ROWS - cut)
    c_back = [remote(chip_a, back_a, across)]
    c_other, c_far, c_z1 = first("other", partner), first("far", across), first("z1", znext)
    c_far_o, c_z1_o = onward("far", "far_o", partner), onward("z1", "z1_o", partner)
    c_z1y, c_z2 = onward("z1", "z1y", across), onward("z1", "z2", znext)
    c_z1y_o, c_z2_o = onward("z1y", "z1y_o", partner), onward("z2", "z2_o", partner)
    c_z2y, c_z3 = onward("z2", "z2y", across), onward("z2", "z3", znext)
    c_z2y_o, c_z3_o = onward("z2y", "z2y_o", partner), onward("z3", "z3_o", partner)
    c_z3y_z = [remote(at("far", upper), at("z3y", upper), zprev)]
    c_z3y_y = [remote(at("z3", lower), at("z3y", lower), across)]
    c_z3y_zo = [remote(at("z3y", upper), at("z3y_o", upper), partner)]
    c_z3y_yo = [remote(at("z3y", lower), at("z3y_o", lower), partner)]
    c_got_a, c_got_b = [remote(eng.g13.at[3], got_a, partner)], [remote(eng.g13.at[3], got_b, partner)]
    keep_a = pltpu.make_async_copy(eng.g13.at[2], own_a, part_sem.at[0])
    keep_b = pltpu.make_async_copy(eng.g13.at[2], own_b, part_sem.at[1])

    barrier = pltpu.get_barrier_semaphore()
    for device in (partner, across, znext, zprev):
        pl.semaphore_signal(barrier, inc=1, device_id=device, device_id_type=MESH)
    pl.semaphore_wait(barrier, 4)

    class Sent:
        def __init__(self, copy):
            self.copy = copy

        def wait(self):
            self.copy.wait_send()

    def arrived(copies, then=()):
        def event():
            for c in copies:
                c.wait_recv()
            start(then)
        return event

    start(c_other + c_far + c_z1)
    eng.stage([(tokens, grad_y, rg), at("other")], 2, True, False, [nothing, arrived(c_other)], (), (), [keep_a, c_got_a[0]],
              prelude=lambda: start(eng.load_w(0)))
    sum_a = Adder(own_a, got_a, (None, mine), held, add_in_sem, add_out_sem, arrived(c_got_a))
    eng.stage([at("far"), at("far_o"), at("z1"), at("z1_o")], 2, False, False,
              [arrived(c_far, c_far_o), arrived(c_far_o), arrived(c_z1, c_z1_o + c_z1y + c_z2), arrived(c_z1_o)],
              ([keep_a], [Sent(c_got_a[0])]),
              ((5, arrived(c_z1y + c_z2, c_z2y + c_z3 + c_z1y_o + c_z2_o)),),
              [keep_b, c_got_b[0]], sum_a)
    sum_a.finish(n_loc - 1)
    sum_b = Adder(own_b, got_b, (chip_a, chip_b), held, add_in_sem, add_out_sem, arrived(c_got_b))
    eng.stage([at("z1y"), at("z1y_o"), at("z2"), at("z2_o")], 0, False, True,
              [nothing, arrived(c_z1y_o), nothing, arrived(c_z2_o)],
              ([keep_b], [Sent(c_got_b[0])]),
              ((1, arrived(c_z2y + c_z3, c_z3y_y + c_z3y_z + c_z2y_o + c_z3_o)), (4, lambda: start(c_back)), (6, arrived(c_z3y_y, c_z3y_yo))), (), sum_b)
    sum_b.finish(n_loc - 1)
    arrived(c_z3y_z, c_z3y_zo)()
    arrived(c_z2y_o + c_z3_o + c_z3y_zo + c_z3y_yo + c_back)()
    for c in flights:
        if c is not c_got_a[0] and c is not c_got_b[0]:
            c.wait_send()


def rest_kernel(cfg, lead_ref, land, w1, w3, w2, b1, b3, b2, g1, g3, g2, *scratch):
    eng = Engine(cfg, lead_ref[0, 0], (w1, w3, w2), (b1, b3, b2), (g1, g3, g2), scratch, 2)

    def prelude():
        start(eng.load_w(0))
        for e in range(4):
            start(eng.load_g(e))

    names = ("z2y", "z2y_o", "z3", "z3_o", "z3y", "z3y_o")
    eng.stage([land.at[BLOCKS.index(n)] for n in names], 0, False, True, [nothing] * 6, (), (), (), prelude=prelude)


def call_kernel(name, kernel, cfg, args, shapes, n_src, n_own, extra_scratch, params):
    tok, d_model, d_ff, n_loc, cap, extra = (cfg[k] for k in ("tok", "d_model", "d_ff", "n_loc", "cap", "extra"))
    rows = n_loc * cap + extra
    scratch = [pltpu.VMEM((n_src, 2 * cap + extra, d_model), BF16)] * 2 + [
        pltpu.VMEM((n_src, 16, tok), F32),
        pltpu.VMEM((n_src, 2 * tok + RG_ROWS, d_model), BF16),
        pltpu.VMEM((n_src * cap, d_ff), BF16),
        pltpu.VMEM((n_src * cap, 2 * d_ff), BF16),
    ]
    for slots, kind in ((2, BF16), (4, F32)):
        scratch += [pltpu.VMEM((slots, d_model, 2 * d_ff), kind), pltpu.VMEM((slots, d_ff, d_model), kind)]
    scratch += [pltpu.SemaphoreType.DMA(n) for n in ((n_src, 3), (2, 3), (4, 3), (4, 3))]
    if n_own:
        scratch += [pltpu.VMEM((n_own, rows, d_model), BF16)] * 2
    unit = 2 * d_model * d_ff * rows
    return pl.pallas_call(
        functools.partial(kernel, cfg),
        in_specs=[pl.BlockSpec(memory_space=pltpu.SMEM)] + [pl.BlockSpec(memory_space=pl.ANY)] * (len(args) - 1),
        out_specs=[pl.BlockSpec(memory_space=pl.ANY)] * len(shapes),
        out_shape=shapes,
        scratch_shapes=scratch + extra_scratch,
        compiler_params=pltpu.CompilerParams(vmem_limit_bytes=67_000_000, **params),
        cost_estimate=pl.CostEstimate(flops=unit * (8 * n_src + 7 * n_own) // 8, bytes_accessed=100 << 20, transcendentals=0),
        name=name,
    )(*args)


def last_sum(mine, back_a, back_b, tok, d_model):
    rows = back_a.shape[0] // 2
    n_all, n_half = 2 * tok // rows, tok // rows

    def kernel(m_ref, a_ref, b_ref, y_ref, x_ref, m, v, out, in_sem, out_sem):
        def piece(ref, j):
            return ref.at[pl.ds(j * rows, rows)]

        loads, saves = [], []
        for j in range(n_all):
            other = piece(a_ref, j) if j < 2 else piece(b_ref, j - 2)
            loads.append([pltpu.make_async_copy(piece(m_ref, j), m.at[j], in_sem.at[j, 0]),
                          pltpu.make_async_copy(other, v.at[j], in_sem.at[j, 1])])
            place = piece(y_ref, j) if j < n_half else piece(x_ref, j - n_half)
            saves.append(pltpu.make_async_copy(out.at[j], place, out_sem.at[j]))
        for copies in loads:
            start(copies)
        for j in range(n_all):
            wait(loads[j])
            out[j] = (m[j] + v[j]).astype(BF16)
            saves[j].start()
        wait(saves)

    dma = pltpu.SemaphoreType.DMA
    return pl.pallas_call(
        kernel,
        in_specs=[pl.BlockSpec(memory_space=pl.ANY)] * 3,
        out_specs=[pl.BlockSpec(memory_space=pl.ANY)] * 2,
        out_shape=[jax.ShapeDtypeStruct((tok, d_model), BF16)] * 2,
        scratch_shapes=[pltpu.VMEM((n_all, rows, d_model), F32)] * 2 + [pltpu.VMEM((n_all, rows, d_model), BF16), dma((n_all, 2)), dma((n_all,))],
        compiler_params=pltpu.CompilerParams(vmem_limit_bytes=67_000_000),
        name="last",
    )(mine, back_a, back_b)


def solution(mesh):
    n_data, n_er = mesh.shape["data"], mesh.shape["expert"]
    row_spec = P(("pod", "data", "expert"), None)
    w_spec = P("expert", None, None)
    grad_spec = P(("pod", "expert"), None, None)
    across = [(r, r ^ 2) for r in range(n_er)]

    def body(tokens, routes, gates, grad_y, w_in1, w_in3, w_out):
        n_loc, d_model, d_ff = w_in1.shape
        n_exp, tok = n_loc * n_er, tokens.shape[0]
        cap, cap_hot = caps(tok, routes.shape[1], n_exp)
        cfg = dict(tok=tok, d_model=d_model, d_ff=d_ff, n_loc=n_loc, n_exp=n_exp, cap=cap, extra=cap_hot - cap,
                   n_data=n_data, n_er=n_er)
        lead = lax.axis_index("expert").astype(jnp.int32).reshape(1, 1)
        gate = gates.T
        hi = lax.reduce_precision(gate, 8, 7)
        mid = lax.reduce_precision(gate - hi, 8, 7)
        low = gate - hi - mid
        rg = jnp.concatenate([jnp.concatenate([routes.T.astype(F32), hi], 0), jnp.concatenate([mid, low], 0)], 1).astype(BF16)
        weights = (w_in1, w_in3, w_out)
        grads = [jax.ShapeDtypeStruct(w.shape, F32) for w in weights]
        sums = [jax.ShapeDtypeStruct((2 * tok, d_model), F32)] * 6
        land = jax.ShapeDtypeStruct((len(BLOCKS), 2 * tok + RG_ROWS, d_model), BF16)
        dma, n_fly, quarter = pltpu.SemaphoreType.DMA, 28, 2 * (2 * tok // n_loc)
        sums[5:] = [jax.ShapeDtypeStruct((n, d_model), F32) for n in (quarter, 2 * tok - quarter, quarter)]
        *acc, land, _, _, _, _, mine, _, chip_b, back_a = call_kernel(
            "roam", roam_kernel, cfg, [lead, tokens, grad_y, rg, *weights], [*grads, land, *sums], 4, 2,
            [dma((n_fly,)), dma((n_fly,)), dma((2,)), pltpu.VMEM((2, 2, 2 * tok // n_loc, d_model), F32), dma((2, 2)), dma((2,))],
            dict(collective_id=0, has_side_effects=True))
        back_b = lax.ppermute(chip_b, "expert", across)
        acc1, acc3, acc2 = call_kernel("rest", rest_kernel, cfg, [lead, land, *weights, *acc], grads, 6, 0, [], {})
        y_out, grad_x = last_sum(mine, back_a, back_b, tok, d_model)
        return y_out, grad_x, acc1, acc3, acc2

    return jax.shard_map(body, mesh=mesh,
                         in_specs=(row_spec, row_spec, row_spec, row_spec, w_spec, w_spec, w_spec),
                         out_specs=(row_spec, row_spec, grad_spec, grad_spec, grad_spec),
                         check_vma=False)
```

```python
import functools

import jax
import jax.numpy as jnp
from jax import lax
from jax.experimental import pallas as pl
from jax.experimental.pallas import tpu as pltpu
from jax.sharding import PartitionSpec as P

MESH = pl.DeviceIdType.MESH
BLOCKS = ("other", "far", "far_o", "z1", "z1_o", "z1y", "z1y_o", "z2", "z2_o", "z2y", "z2y_o", "z3", "z3_o", "z3y", "z3y_o")
N_HOT = 2
RG_ROWS = 16
F32, BF16 = jnp.float32, jnp.bfloat16


def caps(tok_dev, top_k, n_exp):
    cap_hot = 3 * tok_dev // 8
    cap_cold = max(8, ((tok_dev * top_k - N_HOT * cap_hot) // (n_exp - N_HOT) + 7) // 8 * 8)
    return cap_cold, cap_hot


def dot_nn(a, b):
    return lax.dot_general(a, b, (((1,), (0,)), ((), ())), preferred_element_type=F32)


def dot_nt(a, b):
    return lax.dot_general(a, b, (((1,), (1,)), ((), ())), preferred_element_type=F32)


def dot_tn(a, b):
    return lax.dot_general(a, b, (((0,), (0,)), ((), ())), preferred_element_type=F32)


def prefix(m):
    lane = lax.broadcasted_iota(jnp.int32, m.shape, 1)
    step = 1
    while step < m.shape[1]:
        m = m + jnp.where(lane >= step, pltpu.roll(m, step, 1), 0.0)
        step *= 2
    return m


class Engine:
    def __init__(self, cfg, lead, weights, bases, outs, scratch, group):
        self.__dict__.update(cfg)
        self.lead, self.weights, self.bases, self.outs, self.group = lead, weights, bases, outs, group
        (self.rows_x, self.rows_d, self.meta, self.buf, self.hid, self.dab, self.w13, self.w2, self.g13, self.g2,
         self.src_sem, self.w_sem, self.in_sem, self.out_sem) = scratch[:14]
        self.own_scratch = scratch[14:]
        hot = jnp.logical_or(lead * self.n_loc == 0, lead * self.n_loc == self.n_exp // 2)
        self.far = jnp.where(hot, float(self.cap), float(2 * self.tok))
        self.cold, self.part = self.n_loc * self.cap, group * self.cap

    def triple(self, both, single, slot):
        f = self.d_ff
        return both.at[slot, :, 0:f], both.at[slot, :, f:2 * f], single.at[slot]

    def load_w(self, e):
        slot = lax.rem(e, 2)
        return [pltpu.make_async_copy(w.at[e], b, self.w_sem.at[slot, k])
                for k, (w, b) in enumerate(zip(self.weights, self.triple(self.w13, self.w2, slot)))]

    def load_g(self, e):
        slot = lax.rem(e, 4)
        return [pltpu.make_async_copy(w.at[e], b, self.in_sem.at[slot, k])
                for k, (w, b) in enumerate(zip(self.bases, self.triple(self.g13, self.g2, slot)))]

    def save_g(self, e):
        slot = lax.rem(e, 4)
        return [pltpu.make_async_copy(b, w.at[e], self.out_sem.at[slot, k])
                for k, (w, b) in enumerate(zip(self.outs, self.triple(self.g13, self.g2, slot)))]

    def fetches(self, s, ref):
        if not isinstance(ref, tuple):
            return [pltpu.make_async_copy(ref, self.buf.at[s], self.src_sem.at[s, 0])]
        dst = self.buf.at[s]
        return [pltpu.make_async_copy(r, dst.at[pl.ds(at, r.shape[0])], self.src_sem.at[s, k])
                for k, (r, at) in enumerate(zip(ref, (0, self.tok, 2 * self.tok)))]

    def match_rows(self, src, i, base, size):
        iota = lax.broadcasted_iota(jnp.int32, (size, self.tok), 0).astype(F32) + base
        return iota == self.meta[src, pl.ds(i, 1), :]

    def ranks(self, s):
        tok = self.tok
        rg = self.buf[s, 2 * tok:2 * tok + RG_ROWS, :].astype(F32)
        routes = rg[0:8, :tok]
        gates = (rg[8:16, :tok] + rg[0:8, tok:]) + rg[8:16, tok:]
        member, weight = [], []
        for i in range(self.n_loc):
            match = routes == (self.lead * self.n_loc + i).astype(F32)
            member.append(jnp.sum(jnp.where(match, 1.0, 0.0), axis=0, keepdims=True))
            weight.append(jnp.sum(jnp.where(match, gates, 0.0), axis=0, keepdims=True))
        member = jnp.concatenate(member, axis=0)
        self.meta[s, 0:8, :] = jnp.where(member > 0.0, prefix(member) - 1.0, -1.0)
        self.meta[s, 8:16, :] = jnp.concatenate(weight, axis=0)

    def gather(self, s, which):
        tok, meta, buf = self.tok, self.meta, self.buf
        pick, gate = [], []
        for i, base, at, size in which:
            match = self.match_rows(s, i, base, size)
            pick.append(jnp.where(match, 1.0, 0.0).astype(BF16))
            gate.append(jnp.sum(jnp.where(match, meta[s, pl.ds(8 + i, 1), :], 0.0), axis=1, keepdims=True))
        pick, gate = jnp.concatenate(pick, axis=0), jnp.concatenate(gate, axis=0)
        at, size = which[0][2], pick.shape[0]
        self.rows_x[s, at:at + size, :] = dot_nn(pick, buf[s, 0:tok, :]).astype(BF16)
        self.rows_d[s, at:at + size, :] = (dot_nn(pick, buf[s, tok:2 * tok, :]) * gate).astype(BF16)

    def block(self, n_src, n_own, at, size, keep, w, g, g_in, middle=lambda: None):
        d_model, d_ff, hid, dab = self.d_model, self.d_ff, self.hid, self.dab
        w13, w2 = self.w13.at[w], self.w2.at[w]
        rows = n_src * size

        def load(ref):
            return ref[0:n_src, pl.ds(at, size), :].reshape(rows, d_model)

        ab = dot_nn(load(self.rows_x), w13[...]).astype(BF16).astype(F32)
        dh = dot_nt(load(self.rows_d), w2[...])
        a, b = ab[:, :d_ff], ab[:, d_ff:]
        sig = 0.5 * jnp.tanh(0.5 * a) + 0.5
        act = a * sig
        hid[0:rows, :] = (act * b).astype(BF16)
        dab[0:rows, 0:d_ff] = (dh * b * sig * (1.0 + a * (1.0 - sig))).astype(BF16)
        dab[0:rows, d_ff:] = (dh * act).astype(BF16)
        middle()
        if size < self.cap:
            def columns(k, carry):
                cols = pl.ds(pl.multiple_of(k * d_ff, d_ff), d_ff)
                self.g13[g, :, cols] = self.g13[g, :, cols] + dot_tn(load(self.rows_x), dab[0:rows, cols])
                self.g2[g, :, cols] = self.g2[g, :, cols] + dot_tn(hid[0:rows, :], self.rows_d[0:n_src, pl.ds(at, size), cols].reshape(rows, d_ff))
                return carry

            lax.fori_loop(0, 2, columns, 0)
        else:
            for out, lhs, rhs in ((self.g13, load(self.rows_x), dab[0:rows, :]), (self.g2, hid[0:rows, :], load(self.rows_d))):
                if g_in:
                    out[g] = out[g] + dot_tn(lhs, rhs)
                else:
                    out[g] = dot_tn(lhs, rhs)
        if n_own:
            kept_o, kept_x = self.own_scratch[:2]
            m = n_own * size
            o = dot_nn(hid[0:m, :], w2[...]).astype(BF16)
            dx = dot_nt(dab[0:m, :], w13[...]).astype(BF16)
            kept_o[:, pl.ds(keep, size), :] = o.reshape(n_own, size, d_model)
            kept_x[:, pl.ds(keep, size), :] = dx.reshape(n_own, size, d_model)

    def stage(self, srcs, n_own, first, last, before, held, events, ship, each=None, prelude=lambda: None):
        n_src, n_loc, cap, group = len(srcs), self.n_loc, self.cap, self.group
        width = 1 if n_src == 2 else 2
        turns = n_src // width
        fetch = [self.fetches(s, r) for s, r in enumerate(srcs)]

        def ask(t):
            for s in range(t, n_src, turns):
                before[s]()
                start(fetch[s])

        eager = all(b is nothing for b in before)
        for t in range(turns if eager else 1):
            ask(t)
        prelude()
        if held:
            wait(held[0])
            start(self.load_g(2))

        def wave(p, carry):
            def turn(t, carry):
                some = [t + j * turns for j in range(width)]

                @pl.when(p == 0)
                def _():
                    for k in range(turns):
                        @pl.when(t == k)
                        def _(k=k):
                            for s in range(k, n_src, turns):
                                wait(fetch[s])
                    for s in some:
                        self.ranks(s)
                        self.gather(s, [(0, self.far, self.part, self.extra)])
                    for k in range(0 if eager or width == 1 else turns - 1):
                        @pl.when(t == k)
                        def _(k=k):
                            ask(k + 1)

                for s in some:
                    self.gather(s, [(group * p + i, 0.0, i * cap, cap) for i in range(group)])
                if width == 1 and not eager:
                    for k in range(turns - 1):
                        @pl.when(jnp.logical_and(p == 0, t == k))
                        def _(k=k):
                            ask(k + 1)
                return carry

            lax.fori_loop(0, turns, turn, 0)

            def one(i, carry):
                e = group * p + i
                wait(self.load_w(e))
                if last:
                    @pl.when(e + 1 < n_loc)
                    def _():
                        start(self.load_w(e + 1))
                else:
                    start(self.load_w(lax.rem(e + 1, n_loc)))

                def middle():
                    @pl.when(e >= 2)
                    def _():
                        wait(self.save_g(e - 2))

                    if held:
                        @pl.when(e == 0)
                        def _():
                            wait(held[1])
                            start(self.load_g(3))

                    if first:
                        @pl.when(e + 2 >= n_loc)
                        def _():
                            start(self.load_g(e + 2 - n_loc))
                    else:
                        @pl.when(jnp.logical_and(e >= (2 if held else 0), e + 2 < n_loc))
                        def _():
                            start(self.load_g(e + 2))

                        if not last:
                            @pl.when(e + 2 >= n_loc)
                            def _():
                                start(self.load_g(e + 2 - n_loc))
                    if not first:
                        wait(self.load_g(e))

                self.block(n_src, n_own, pl.multiple_of(i * cap, cap), cap, pl.multiple_of(e * cap, cap),
                           lax.rem(e, 2), lax.rem(e, 4), not first, middle)

                @pl.when(e == 0)
                def more():
                    self.block(n_src, n_own, self.part, self.extra, self.cold, 0, 0, True)

                start(self.save_g(e))
                for k, event in events:
                    @pl.when(e == k)
                    def _(event=event):
                        event()
                if each is not None:
                    each(e)
                return carry

            lax.fori_loop(0, group, one, 0)
            return carry

        lax.fori_loop(0, n_loc // group, wave, 0)
        if n_own:
            self.combine(n_own, ship)
        elif last:
            wait(self.save_g(n_loc - 2))
            wait(self.save_g(n_loc - 1))

    def combine(self, n_own, ship):
        kept_o, kept_x = self.own_scratch[:2]
        cold, extra, cap, tok, n_loc = self.cold, self.extra, self.cap, self.tok, self.n_loc
        part, n_blk = self.part, n_loc // self.group
        pieces = [(i, 0.0, i // self.group, i % self.group * cap, cap) for i in range(n_loc)] + [(0, self.far, None, part, extra)]
        places = [(ref, pl.ds(lane * tok, tok)) for ref in (self.rows_x, self.rows_d) for lane in (0, 1)]

        def one(src, carry):
            for s in range(n_own):
                @pl.when(src == s)
                def _(s=s):
                    wait(self.save_g(n_loc - 2 + s))

            for i, base, blk, at, size in pieces:
                match = self.match_rows(src, i, base, size)
                gate = self.meta[src, 8 + i:9 + i, :]
                hi = gate.astype(BF16).astype(F32)
                mid = (gate - hi).astype(BF16).astype(F32)
                low = gate - hi - mid
                for k, v in enumerate((hi, mid, low, 1.0)):
                    ref, lanes = places[0 if blk is None else k]
                    ref[k if blk is None else blk, at:at + size, lanes] = jnp.where(match, v, 0.0).astype(BF16)

            def chosen(k):
                ref, lanes = places[k]
                return ref[0:n_blk, 0:part, lanes].reshape(cold, tok)

            spare, lanes = places[0]
            wide = self.d_model // 2

            def columns(h, carry):
                cols = pl.ds(pl.multiple_of(h * wide, wide), wide)
                o, rest = kept_o[src, 0:cold, cols], kept_o[src, cold:cold + extra, cols]
                y = dot_tn(chosen(0), o) + dot_tn(chosen(1), o) + dot_tn(chosen(2), o)
                gates = spare[0:3, part:part + extra, lanes].reshape(3 * extra, tok)
                self.g13[2 + src, 0:tok, cols] = y + dot_tn(gates, jnp.concatenate([rest] * 3, axis=0))
                dx = dot_tn(chosen(3), kept_x[src, 0:cold, cols])
                gates = spare[3, part:part + extra, lanes]
                self.g13[2 + src, tok:2 * tok, cols] = dx + dot_tn(gates, kept_x[src, cold:cold + extra, cols])
                return carry

            lax.fori_loop(0, 2, columns, 0)
            for s in range(n_own):
                @pl.when(src == s)
                def _(s=s):
                    ship[s].start()
            return carry

        lax.fori_loop(0, n_own, one, 0)


def start(copies):
    for c in copies:
        c.start()


def wait(copies):
    for c in copies:
        c.wait()


def nothing():
    pass


class Adder:
    def __init__(self, a, b, out, held, load_sem, save_sem, ready):
        self.a, self.b, self.out, self.held, self.load_sem, self.save_sem, self.ready = a, b, out, held, load_sem, save_sem, ready
        self.rows = held.shape[2]
        self.n_head = out[0].shape[0] // self.rows if out[0] is not None else 0

    def loads(self, k):
        slot, at = lax.rem(k, 2), pl.ds(pl.multiple_of(k * self.rows, self.rows), self.rows)
        return [pltpu.make_async_copy(v.at[at], self.held.at[slot, n], self.load_sem.at[slot, n]) for n, v in enumerate((self.a, self.b))]

    def save(self, k, head=False):
        slot = lax.rem(k, 2)
        ref, k = (self.out[0], k) if head else (self.out[1], k - self.n_head)
        at = pl.ds(pl.multiple_of(k * self.rows, self.rows), self.rows)
        return pltpu.make_async_copy(self.held.at[slot, 0], ref.at[at], self.save_sem.at[slot])

    def add(self, k):
        wait(self.loads(k))
        slot = lax.rem(k, 2)
        self.held[slot, 0] = self.held[slot, 0] + self.held[slot, 1]
        if self.n_head:
            @pl.when(k < self.n_head)
            def _():
                self.save(k, True).start()

        @pl.when(k >= self.n_head)
        def _():
            self.save(k).start()

    def saved(self, k):
        if self.n_head:
            @pl.when(k < self.n_head)
            def _():
                self.save(k, True).wait()

        @pl.when(k >= self.n_head)
        def _():
            self.save(k).wait()

    def __call__(self, e):
        @pl.when(e == 0)
        def _():
            self.ready()

        @pl.when(e >= 1)
        def _():
            self.add(e - 1)

        @pl.when(e >= 2)
        def _():
            self.saved(e - 2)

        start(self.loads(e))

    def finish(self, last):
        self.add(last)
        self.saved(last - 1)
        self.saved(last)


def roam_kernel(cfg, lead_ref, tokens, grad_y, rg, w1, w3, w2, g1, g3, g2, land, own_a, own_b, got_a, got_b, mine, chip_a, chip_b, back_a, *scratch):
    send_sem, recv_sem, part_sem, held, add_in_sem, add_out_sem = scratch[-6:]
    eng = Engine(cfg, lead_ref[0, 0], (w1, w3, w2), (g1, g3, g2), (g1, g3, g2), scratch[:-6], 2)
    q, r = lax.axis_index("data"), lax.axis_index("expert")
    n_data, n_er, tok, n_loc = cfg["n_data"], cfg["n_er"], cfg["tok"], cfg["n_loc"]
    partner = {"expert": r + 1 - 2 * lax.rem(r, 2)}
    across = {"expert": lax.rem(r + n_er // 2, n_er)}
    znext = {"data": lax.rem(q + 1, n_data)}
    zprev = {"data": lax.rem(q + n_data - 1, n_data)}

    def at(name, rows=None):
        ref = land.at[BLOCKS.index(name)]
        return ref if rows is None else ref.at[rows]

    flights = []

    def remote(src, dst, device):
        k = len(flights)
        copy = pltpu.make_async_remote_copy(src_ref=src, dst_ref=dst, send_sem=send_sem.at[k], recv_sem=recv_sem.at[k],
                                            device_id=device, device_id_type=MESH)
        flights.append(copy)
        return copy

    def first(name, device):
        parts = ((tokens, 0, tok), (grad_y, tok, tok), (rg, 2 * tok, RG_ROWS))
        return [remote(v, at(name, pl.ds(lo, n)), device) for v, lo, n in parts]

    def onward(src, dst, device):
        return [remote(at(src), at(dst), device)]

    cut = (2 * tok + RG_ROWS) // 64 * 48
    upper, lower = pl.ds(0, cut), pl.ds(cut, 2 * tok + RG_ROWS - cut)
    c_back = [remote(chip_a, back_a, across)]
    c_other, c_far, c_z1 = first("other", partner), first("far", across), first("z1", znext)
    c_far_o, c_z1_o = onward("far", "far_o", partner), onward("z1", "z1_o", partner)
    c_z1y, c_z2 = onward("z1", "z1y", across), onward("z1", "z2", znext)
    c_z1y_o, c_z2_o = onward("z1y", "z1y_o", partner), onward("z2", "z2_o", partner)
    c_z2y, c_z3 = onward("z2", "z2y", across), onward("z2", "z3", znext)
    c_z2y_o, c_z3_o = onward("z2y", "z2y_o", partner), onward("z3", "z3_o", partner)
    c_z3y_z = [remote(at("far", upper), at("z3y", upper), zprev)]
    c_z3y_y = [remote(at("z3", lower), at("z3y", lower), across)]
    c_z3y_zo = [remote(at("z3y", upper), at("z3y_o", upper), partner)]
    c_z3y_yo = [remote(at("z3y", lower), at("z3y_o", lower), partner)]
    c_got_a, c_got_b = [remote(eng.g13.at[3], got_a, partner)], [remote(eng.g13.at[3], got_b, partner)]
    keep_a = pltpu.make_async_copy(eng.g13.at[2], own_a, part_sem.at[0])
    keep_b = pltpu.make_async_copy(eng.g13.at[2], own_b, part_sem.at[1])

    barrier = pltpu.get_barrier_semaphore()
    for device in (partner, across, znext, zprev):
        pl.semaphore_signal(barrier, inc=1, device_id=device, device_id_type=MESH)
    pl.semaphore_wait(barrier, 4)

    class Sent:
        def __init__(self, copy):
            self.copy = copy

        def wait(self):
            self.copy.wait_send()

    def arrived(copies, then=()):
        def event():
            for c in copies:
                c.wait_recv()
            start(then)
        return event

    start(c_other + c_far + c_z1)
    eng.stage([(tokens, grad_y, rg), at("other")], 2, True, False, [nothing, arrived(c_other)], (), (), [keep_a, c_got_a[0]],
              prelude=lambda: start(eng.load_w(0)))
    sum_a = Adder(own_a, got_a, (None, mine), held, add_in_sem, add_out_sem, arrived(c_got_a))
    eng.stage([at("far"), at("far_o"), at("z1"), at("z1_o")], 2, False, False,
              [arrived(c_far, c_far_o), arrived(c_far_o), arrived(c_z1, c_z1_o + c_z1y + c_z2), arrived(c_z1_o)],
              ([keep_a], [Sent(c_got_a[0])]),
              ((5, arrived(c_z1y + c_z2, c_z2y + c_z3 + c_z1y_o + c_z2_o)),),
              [keep_b, c_got_b[0]], sum_a)
    sum_a.finish(n_loc - 1)
    sum_b = Adder(own_b, got_b, (chip_a, chip_b), held, add_in_sem, add_out_sem, arrived(c_got_b))
    eng.stage([at("z1y"), at("z1y_o"), at("z2"), at("z2_o")], 0, False, True,
              [nothing, arrived(c_z1y_o), nothing, arrived(c_z2_o)],
              ([keep_b], [Sent(c_got_b[0])]),
              ((1, arrived(c_z2y + c_z3, c_z3y_y + c_z3y_z + c_z2y_o + c_z3_o)), (4, lambda: start(c_back)), (6, arrived(c_z3y_y, c_z3y_yo))), (), sum_b)
    sum_b.finish(n_loc - 1)
    arrived(c_z3y_z, c_z3y_zo)()
    arrived(c_z2y_o + c_z3_o + c_z3y_zo + c_z3y_yo + c_back)()
    for c in flights:
        if c is not c_got_a[0] and c is not c_got_b[0]:
            c.wait_send()


def rest_kernel(cfg, lead_ref, land, w1, w3, w2, b1, b3, b2, g1, g3, g2, *scratch):
    eng = Engine(cfg, lead_ref[0, 0], (w1, w3, w2), (b1, b3, b2), (g1, g3, g2), scratch, 2)

    def prelude():
        start(eng.load_w(0))
        for e in (0, 1):
            start(eng.load_g(e))

    names = ("z2y", "z2y_o", "z3", "z3_o", "z3y", "z3y_o")
    eng.stage([land.at[BLOCKS.index(n)] for n in names], 0, False, True, [nothing] * 6, (), (), (), prelude=prelude)


def call_kernel(name, kernel, cfg, args, shapes, n_src, n_own, extra_scratch, params):
    tok, d_model, d_ff, n_loc, cap, extra = (cfg[k] for k in ("tok", "d_model", "d_ff", "n_loc", "cap", "extra"))
    rows = n_loc * cap + extra
    scratch = [pltpu.VMEM((n_src, 2 * cap + extra, d_model), BF16)] * 2 + [
        pltpu.VMEM((n_src, 16, tok), F32),
        pltpu.VMEM((n_src, 2 * tok + RG_ROWS, d_model), BF16),
        pltpu.VMEM((n_src * cap, d_ff), BF16),
        pltpu.VMEM((n_src * cap, 2 * d_ff), BF16),
    ]
    for slots, kind in ((2, BF16), (4, F32)):
        scratch += [pltpu.VMEM((slots, d_model, 2 * d_ff), kind), pltpu.VMEM((slots, d_ff, d_model), kind)]
    scratch += [pltpu.SemaphoreType.DMA(n) for n in ((n_src, 3), (2, 3), (4, 3), (4, 3))]
    if n_own:
        scratch += [pltpu.VMEM((n_own, rows, d_model), BF16)] * 2
    unit = 2 * d_model * d_ff * rows
    return pl.pallas_call(
        functools.partial(kernel, cfg),
        in_specs=[pl.BlockSpec(memory_space=pltpu.SMEM)] + [pl.BlockSpec(memory_space=pl.ANY)] * (len(args) - 1),
        out_specs=[pl.BlockSpec(memory_space=pl.ANY)] * len(shapes),
        out_shape=shapes,
        scratch_shapes=scratch + extra_scratch,
        compiler_params=pltpu.CompilerParams(vmem_limit_bytes=67_000_000, **params),
        cost_estimate=pl.CostEstimate(flops=unit * (8 * n_src + 7 * n_own) // 8, bytes_accessed=100 << 20, transcendentals=0),
        name=name,
    )(*args)


def last_sum(mine, back_a, back_b, tok, d_model):
    rows = back_a.shape[0] // 2
    n_all, n_half = 2 * tok // rows, tok // rows

    def kernel(m_ref, a_ref, b_ref, y_ref, x_ref, m, v, out, in_sem, out_sem):
        def piece(ref, j):
            return ref.at[pl.ds(j * rows, rows)]

        loads, saves = [], []
        for j in range(n_all):
            other = piece(a_ref, j) if j < 2 else piece(b_ref, j - 2)
            loads.append([pltpu.make_async_copy(piece(m_ref, j), m.at[j], in_sem.at[j, 0]),
                          pltpu.make_async_copy(other, v.at[j], in_sem.at[j, 1])])
            place = piece(y_ref, j) if j < n_half else piece(x_ref, j - n_half)
            saves.append(pltpu.make_async_copy(out.at[j], place, out_sem.at[j]))
        for copies in loads:
            start(copies)
        for j in range(n_all):
            wait(loads[j])
            out[j] = (m[j] + v[j]).astype(BF16)
            saves[j].start()
        wait(saves)

    dma = pltpu.SemaphoreType.DMA
    return pl.pallas_call(
        kernel,
        in_specs=[pl.BlockSpec(memory_space=pl.ANY)] * 3,
        out_specs=[pl.BlockSpec(memory_space=pl.ANY)] * 2,
        out_shape=[jax.ShapeDtypeStruct((tok, d_model), BF16)] * 2,
        scratch_shapes=[pltpu.VMEM((n_all, rows, d_model), F32)] * 2 + [pltpu.VMEM((n_all, rows, d_model), BF16), dma((n_all, 2)), dma((n_all,))],
        compiler_params=pltpu.CompilerParams(vmem_limit_bytes=67_000_000),
        name="last",
    )(mine, back_a, back_b)


def solution(mesh):
    n_data, n_er = mesh.shape["data"], mesh.shape["expert"]
    row_spec = P(("pod", "data", "expert"), None)
    w_spec = P("expert", None, None)
    grad_spec = P(("pod", "expert"), None, None)
    across = [(r, r ^ 2) for r in range(n_er)]

    def body(tokens, routes, gates, grad_y, w_in1, w_in3, w_out):
        n_loc, d_model, d_ff = w_in1.shape
        n_exp, tok = n_loc * n_er, tokens.shape[0]
        cap, cap_hot = caps(tok, routes.shape[1], n_exp)
        cfg = dict(tok=tok, d_model=d_model, d_ff=d_ff, n_loc=n_loc, n_exp=n_exp, cap=cap, extra=cap_hot - cap,
                   n_data=n_data, n_er=n_er)
        lead = lax.axis_index("expert").astype(jnp.int32).reshape(1, 1)
        gate = gates.T
        hi = lax.reduce_precision(gate, 8, 7)
        mid = lax.reduce_precision(gate - hi, 8, 7)
        low = gate - hi - mid
        rg = jnp.concatenate([jnp.concatenate([routes.T.astype(F32), hi], 0), jnp.concatenate([mid, low], 0)], 1).astype(BF16)
        weights = (w_in1, w_in3, w_out)
        grads = [jax.ShapeDtypeStruct(w.shape, F32) for w in weights]
        sums = [jax.ShapeDtypeStruct((2 * tok, d_model), F32)] * 6
        land = jax.ShapeDtypeStruct((len(BLOCKS), 2 * tok + RG_ROWS, d_model), BF16)
        dma, n_fly, quarter = pltpu.SemaphoreType.DMA, 28, 2 * (2 * tok // n_loc)
        sums[5:] = [jax.ShapeDtypeStruct((n, d_model), F32) for n in (quarter, 2 * tok - quarter, quarter)]
        *acc, land, _, _, _, _, mine, _, chip_b, back_a = call_kernel(
            "roam", roam_kernel, cfg, [lead, tokens, grad_y, rg, *weights], [*grads, land, *sums], 4, 2,
            [dma((n_fly,)), dma((n_fly,)), dma((2,)), pltpu.VMEM((2, 2, 2 * tok // n_loc, d_model), F32), dma((2, 2)), dma((2,))],
            dict(collective_id=0, has_side_effects=True))
        back_b = lax.ppermute(chip_b, "expert", across)
        acc1, acc3, acc2 = call_kernel("rest", rest_kernel, cfg, [lead, land, *weights, *acc], grads, 6, 0, [], {})
        y_out, grad_x = last_sum(mine, back_a, back_b, tok, d_model)
        return y_out, grad_x, acc1, acc3, acc2

    return jax.shard_map(body, mesh=mesh,
                         in_specs=(row_spec, row_spec, row_spec, row_spec, w_spec, w_spec, w_spec),
                         out_specs=(row_spec, row_spec, grad_spec, grad_spec, grad_spec),
                         check_vma=False)
```

```python
import functools

import jax
import jax.numpy as jnp
from jax import lax
from jax.experimental import pallas as pl
from jax.experimental.pallas import tpu as pltpu
from jax.sharding import PartitionSpec as P

MESH = pl.DeviceIdType.MESH
BLOCKS = ("other", "far", "far_o", "z1", "z1_o", "z1y", "z1y_o", "z2", "z2_o", "z2y", "z2y_o", "z3", "z3_o", "z3y", "z3y_o")
N_HOT = 2
RG_ROWS = 16
F32, BF16 = jnp.float32, jnp.bfloat16


def caps(tok_dev, top_k, n_exp):
    cap_hot = 3 * tok_dev // 8
    cap_cold = max(8, ((tok_dev * top_k - N_HOT * cap_hot) // (n_exp - N_HOT) + 7) // 8 * 8)
    return cap_cold, cap_hot


def dot_nn(a, b):
    return lax.dot_general(a, b, (((1,), (0,)), ((), ())), preferred_element_type=F32)


def dot_nt(a, b):
    return lax.dot_general(a, b, (((1,), (1,)), ((), ())), preferred_element_type=F32)


def dot_tn(a, b):
    return lax.dot_general(a, b, (((0,), (0,)), ((), ())), preferred_element_type=F32)


def prefix(m):
    lane = lax.broadcasted_iota(jnp.int32, m.shape, 1)
    step = 1
    while step < m.shape[1]:
        m = m + jnp.where(lane >= step, pltpu.roll(m, step, 1), 0.0)
        step *= 2
    return m


class Engine:
    def __init__(self, cfg, lead, weights, bases, outs, scratch, group):
        self.__dict__.update(cfg)
        self.lead, self.weights, self.bases, self.outs, self.group = lead, weights, bases, outs, group
        (self.rows_x, self.rows_d, self.meta, self.buf, self.hid, self.dab, self.w13, self.w2, self.g13, self.g2,
         self.src_sem, self.w_sem, self.in_sem, self.out_sem) = scratch[:14]
        self.own_scratch = scratch[14:]
        hot = jnp.logical_or(lead * self.n_loc == 0, lead * self.n_loc == self.n_exp // 2)
        self.far = jnp.where(hot, float(self.cap), float(2 * self.tok))
        self.cold, self.part = self.n_loc * self.cap, group * self.cap

    def triple(self, both, single, slot):
        f = self.d_ff
        return both.at[slot, :, 0:f], both.at[slot, :, f:2 * f], single.at[slot]

    def load_w(self, e):
        slot = lax.rem(e, 2)
        return [pltpu.make_async_copy(w.at[e], b, self.w_sem.at[slot, k])
                for k, (w, b) in enumerate(zip(self.weights, self.triple(self.w13, self.w2, slot)))]

    def load_g(self, e):
        slot = lax.rem(e, 4)
        return [pltpu.make_async_copy(w.at[e], b, self.in_sem.at[slot, k])
                for k, (w, b) in enumerate(zip(self.bases, self.triple(self.g13, self.g2, slot)))]

    def save_g(self, e):
        slot = lax.rem(e, 4)
        return [pltpu.make_async_copy(b, w.at[e], self.out_sem.at[slot, k])
                for k, (w, b) in enumerate(zip(self.outs, self.triple(self.g13, self.g2, slot)))]

    def fetches(self, s, ref):
        if not isinstance(ref, tuple):
            return [pltpu.make_async_copy(ref, self.buf.at[s], self.src_sem.at[s, 0])]
        dst = self.buf.at[s]
        return [pltpu.make_async_copy(r, dst.at[pl.ds(at, r.shape[0])], self.src_sem.at[s, k])
                for k, (r, at) in enumerate(zip(ref, (0, self.tok, 2 * self.tok)))]

    def match_rows(self, src, i, base, size):
        iota = lax.broadcasted_iota(jnp.int32, (size, self.tok), 0).astype(F32) + base
        return iota == self.meta[src, pl.ds(i, 1), :]

    def ranks(self, s):
        tok = self.tok
        rg = self.buf[s, 2 * tok:2 * tok + RG_ROWS, :].astype(F32)
        routes = rg[0:8, :tok]
        gates = (rg[8:16, :tok] + rg[0:8, tok:]) + rg[8:16, tok:]
        member, weight = [], []
        for i in range(self.n_loc):
            match = routes == (self.lead * self.n_loc + i).astype(F32)
            member.append(jnp.sum(jnp.where(match, 1.0, 0.0), axis=0, keepdims=True))
            weight.append(jnp.sum(jnp.where(match, gates, 0.0), axis=0, keepdims=True))
        member = jnp.concatenate(member, axis=0)
        self.meta[s, 0:8, :] = jnp.where(member > 0.0, prefix(member) - 1.0, -1.0)
        self.meta[s, 8:16, :] = jnp.concatenate(weight, axis=0)

    def gather(self, s, which):
        tok, meta, buf = self.tok, self.meta, self.buf
        pick, gate = [], []
        for i, base, at, size in which:
            match = self.match_rows(s, i, base, size)
            pick.append(jnp.where(match, 1.0, 0.0).astype(BF16))
            gate.append(jnp.sum(jnp.where(match, meta[s, pl.ds(8 + i, 1), :], 0.0), axis=1, keepdims=True))
        pick, gate = jnp.concatenate(pick, axis=0), jnp.concatenate(gate, axis=0)
        at, size = which[0][2], pick.shape[0]
        self.rows_x[s, at:at + size, :] = dot_nn(pick, buf[s, 0:tok, :]).astype(BF16)
        self.rows_d[s, at:at + size, :] = (dot_nn(pick, buf[s, tok:2 * tok, :]) * gate).astype(BF16)

    def block(self, n_src, n_own, at, size, keep, w, g, g_in, middle=lambda: None):
        d_model, d_ff, hid, dab = self.d_model, self.d_ff, self.hid, self.dab
        w13, w2 = self.w13.at[w], self.w2.at[w]
        rows = n_src * size

        def load(ref):
            return ref[0:n_src, pl.ds(at, size), :].reshape(rows, d_model)

        ab = dot_nn(load(self.rows_x), w13[...]).astype(BF16).astype(F32)
        dh = dot_nt(load(self.rows_d), w2[...])
        a, b = ab[:, :d_ff], ab[:, d_ff:]
        sig = 0.5 * jnp.tanh(0.5 * a) + 0.5
        act = a * sig
        hid[0:rows, :] = (act * b).astype(BF16)
        dab[0:rows, 0:d_ff] = (dh * b * sig * (1.0 + a * (1.0 - sig))).astype(BF16)
        dab[0:rows, d_ff:] = (dh * act).astype(BF16)
        middle()
        if size < self.cap:
            def columns(k, carry):
                cols = pl.ds(pl.multiple_of(k * d_ff, d_ff), d_ff)
                self.g13[g, :, cols] = self.g13[g, :, cols] + dot_tn(load(self.rows_x), dab[0:rows, cols])
                self.g2[g, :, cols] = self.g2[g, :, cols] + dot_tn(hid[0:rows, :], self.rows_d[0:n_src, pl.ds(at, size), cols].reshape(rows, d_ff))
                return carry

            lax.fori_loop(0, 2, columns, 0)
        else:
            for out, lhs, rhs in ((self.g13, load(self.rows_x), dab[0:rows, :]), (self.g2, hid[0:rows, :], load(self.rows_d))):
                if g_in:
                    out[g] = out[g] + dot_tn(lhs, rhs)
                else:
                    out[g] = dot_tn(lhs, rhs)
        if n_own:
            kept_o, kept_x = self.own_scratch[:2]
            m = n_own * size
            o = dot_nn(hid[0:m, :], w2[...]).astype(BF16)
            dx = dot_nt(dab[0:m, :], w13[...]).astype(BF16)
            kept_o[:, pl.ds(keep, size), :] = o.reshape(n_own, size, d_model)
            kept_x[:, pl.ds(keep, size), :] = dx.reshape(n_own, size, d_model)

    def stage(self, srcs, n_own, first, last, before, held, events, ship, each=None, prelude=lambda: None):
        n_src, n_loc, cap, group = len(srcs), self.n_loc, self.cap, self.group
        width = 1 if n_src == 2 else 2
        turns = n_src // width
        fetch = [self.fetches(s, r) for s, r in enumerate(srcs)]

        def ask(t):
            for s in range(t, n_src, turns):
                before[s]()
                start(fetch[s])

        eager = all(b is nothing for b in before)
        for t in range(turns if eager else 1):
            ask(t)
        prelude()
        if held:
            wait(held[0])
            start(self.load_g(2))

        def wave(p, carry):
            def turn(t, carry):
                some = [t + j * turns for j in range(width)]

                @pl.when(p == 0)
                def _():
                    for k in range(turns):
                        @pl.when(t == k)
                        def _(k=k):
                            for s in range(k, n_src, turns):
                                wait(fetch[s])
                    for s in some:
                        self.ranks(s)
                        self.gather(s, [(0, self.far, self.part, self.extra)])
                    for k in range(0 if eager or width == 1 else turns - 1):
                        @pl.when(t == k)
                        def _(k=k):
                            ask(k + 1)

                for s in some:
                    self.gather(s, [(group * p + i, 0.0, i * cap, cap) for i in range(group)])
                if width == 1 and not eager:
                    for k in range(turns - 1):
                        @pl.when(jnp.logical_and(p == 0, t == k))
                        def _(k=k):
                            ask(k + 1)
                return carry

            lax.fori_loop(0, turns, turn, 0)

            def one(i, carry):
                e = group * p + i
                wait(self.load_w(e))
                if last:
                    @pl.when(e + 1 < n_loc)
                    def _():
                        start(self.load_w(e + 1))
                else:
                    start(self.load_w(lax.rem(e + 1, n_loc)))

                def middle():
                    @pl.when(e >= 2)
                    def _():
                        wait(self.save_g(e - 2))

                    if held:
                        @pl.when(e == 0)
                        def _():
                            wait(held[1])
                            start(self.load_g(3))

                    if first:
                        @pl.when(e + 2 >= n_loc)
                        def _():
                            start(self.load_g(e + 2 - n_loc))
                    else:
                        @pl.when(jnp.logical_and(e >= (2 if held else 0), e + 2 < n_loc))
                        def _():
                            start(self.load_g(e + 2))

                        if not last:
                            @pl.when(e + 2 >= n_loc)
                            def _():
                                start(self.load_g(e + 2 - n_loc))
                    if not first:
                        wait(self.load_g(e))

                self.block(n_src, n_own, pl.multiple_of(i * cap, cap), cap, pl.multiple_of(e * cap, cap),
                           lax.rem(e, 2), lax.rem(e, 4), not first, middle)

                @pl.when(e == 0)
                def more():
                    self.block(n_src, n_own, self.part, self.extra, self.cold, 0, 0, True)

                start(self.save_g(e))
                for k, event in events:
                    @pl.when(e == k)
                    def _(event=event):
                        event()
                if each is not None:
                    each(e)
                return carry

            lax.fori_loop(0, group, one, 0)
            return carry

        lax.fori_loop(0, n_loc // group, wave, 0)
        if n_own:
            self.combine(n_own, ship)
        elif last:
            wait(self.save_g(n_loc - 2))
            wait(self.save_g(n_loc - 1))

    def combine(self, n_own, ship):
        kept_o, kept_x = self.own_scratch[:2]
        cold, extra, cap, tok, n_loc = self.cold, self.extra, self.cap, self.tok, self.n_loc
        part, n_blk = self.part, n_loc // self.group
        pieces = [(i, 0.0, i // self.group, i % self.group * cap, cap) for i in range(n_loc)] + [(0, self.far, None, part, extra)]
        places = [(ref, pl.ds(lane * tok, tok)) for ref in (self.rows_x, self.rows_d) for lane in (0, 1)]

        def one(src, carry):
            for s in range(n_own):
                @pl.when(src == s)
                def _(s=s):
                    wait(self.save_g(n_loc - 2 + s))

            for i, base, blk, at, size in pieces:
                match = self.match_rows(src, i, base, size)
                gate = self.meta[src, 8 + i:9 + i, :]
                hi = gate.astype(BF16).astype(F32)
                mid = (gate - hi).astype(BF16).astype(F32)
                low = gate - hi - mid
                for k, v in enumerate((hi, mid, low, 1.0)):
                    ref, lanes = places[0 if blk is None else k]
                    ref[k if blk is None else blk, at:at + size, lanes] = jnp.where(match, v, 0.0).astype(BF16)

            def chosen(k):
                ref, lanes = places[k]
                return ref[0:n_blk, 0:part, lanes].reshape(cold, tok)

            spare, lanes = places[0]
            wide = self.d_model // 2

            def columns(h, carry):
                cols = pl.ds(pl.multiple_of(h * wide, wide), wide)
                o, rest = kept_o[src, 0:cold, cols], kept_o[src, cold:cold + extra, cols]
                y = dot_tn(chosen(0), o) + dot_tn(chosen(1), o) + dot_tn(chosen(2), o)
                gates = spare[0:3, part:part + extra, lanes].reshape(3 * extra, tok)
                self.g13[2 + src, 0:tok, cols] = y + dot_tn(gates, jnp.concatenate([rest] * 3, axis=0))
                dx = dot_tn(chosen(3), kept_x[src, 0:cold, cols])
                gates = spare[3, part:part + extra, lanes]
                self.g13[2 + src, tok:2 * tok, cols] = dx + dot_tn(gates, kept_x[src, cold:cold + extra, cols])
                return carry

            lax.fori_loop(0, 2, columns, 0)
            for s in range(n_own):
                @pl.when(src == s)
                def _(s=s):
                    ship[s].start()
            return carry

        lax.fori_loop(0, n_own, one, 0)


def start(copies):
    for c in copies:
        c.start()


def wait(copies):
    for c in copies:
        c.wait()


def nothing():
    pass


class Adder:
    def __init__(self, a, b, out, held, load_sem, save_sem, ready):
        self.a, self.b, self.out, self.held, self.load_sem, self.save_sem, self.ready = a, b, out, held, load_sem, save_sem, ready
        self.rows = held.shape[2]
        self.n_head = out[0].shape[0] // self.rows if out[0] is not None else 0

    def loads(self, k):
        slot, at = lax.rem(k, 2), pl.ds(pl.multiple_of(k * self.rows, self.rows), self.rows)
        return [pltpu.make_async_copy(v.at[at], self.held.at[slot, n], self.load_sem.at[slot, n]) for n, v in enumerate((self.a, self.b))]

    def save(self, k, head=False):
        slot = lax.rem(k, 2)
        ref, k = (self.out[0], k) if head else (self.out[1], k - self.n_head)
        at = pl.ds(pl.multiple_of(k * self.rows, self.rows), self.rows)
        return pltpu.make_async_copy(self.held.at[slot, 0], ref.at[at], self.save_sem.at[slot])

    def add(self, k):
        wait(self.loads(k))
        slot = lax.rem(k, 2)
        self.held[slot, 0] = self.held[slot, 0] + self.held[slot, 1]
        if self.n_head:
            @pl.when(k < self.n_head)
            def _():
                self.save(k, True).start()

        @pl.when(k >= self.n_head)
        def _():
            self.save(k).start()

    def saved(self, k):
        if self.n_head:
            @pl.when(k < self.n_head)
            def _():
                self.save(k, True).wait()

        @pl.when(k >= self.n_head)
        def _():
            self.save(k).wait()

    def __call__(self, e):
        @pl.when(e == 0)
        def _():
            self.ready()

        @pl.when(e >= 1)
        def _():
            self.add(e - 1)

        @pl.when(e >= 2)
        def _():
            self.saved(e - 2)

        start(self.loads(e))

    def finish(self, last):
        self.add(last)
        self.saved(last - 1)
        self.saved(last)


def roam_kernel(cfg, lead_ref, tokens, grad_y, rg, w1, w3, w2, g1, g3, g2, land, own_a, own_b, got_a, got_b, chip_a, chip_b, back_a, *scratch):
    send_sem, recv_sem, part_sem, held, add_in_sem, add_out_sem = scratch[-6:]
    eng = Engine(cfg, lead_ref[0, 0], (w1, w3, w2), (g1, g3, g2), (g1, g3, g2), scratch[:-6], 2)
    q, r = lax.axis_index("data"), lax.axis_index("expert")
    n_data, n_er, tok, n_loc = cfg["n_data"], cfg["n_er"], cfg["tok"], cfg["n_loc"]
    partner = {"expert": r + 1 - 2 * lax.rem(r, 2)}
    across = {"expert": lax.rem(r + n_er // 2, n_er)}
    znext = {"data": lax.rem(q + 1, n_data)}
    zprev = {"data": lax.rem(q + n_data - 1, n_data)}

    def at(name, rows=None):
        ref = land.at[BLOCKS.index(name)]
        return ref if rows is None else ref.at[rows]

    flights = []

    def remote(src, dst, device):
        k = len(flights)
        copy = pltpu.make_async_remote_copy(src_ref=src, dst_ref=dst, send_sem=send_sem.at[k], recv_sem=recv_sem.at[k],
                                            device_id=device, device_id_type=MESH)
        flights.append(copy)
        return copy

    def first(name, device):
        parts = ((tokens, 0, tok), (grad_y, tok, tok), (rg, 2 * tok, RG_ROWS))
        return [remote(v, at(name, pl.ds(lo, n)), device) for v, lo, n in parts]

    def onward(src, dst, device):
        return [remote(at(src), at(dst), device)]

    cut = (2 * tok + RG_ROWS) // 16 // 16 * 11 * 16
    upper = [pl.ds(0, tok), pl.ds(tok, cut - tok)]
    lower = pl.ds(cut, 2 * tok + RG_ROWS - cut)
    c_back = [remote(chip_a, back_a, across)]
    c_other, c_far, c_z1 = first("other", partner), first("far", across), first("z1", znext)
    c_far_o, c_z1_o = onward("far", "far_o", partner), onward("z1", "z1_o", partner)
    c_z1y, c_z2 = onward("z1", "z1y", across), onward("z1", "z2", znext)
    c_z1y_o, c_z2_o = onward("z1y", "z1y_o", partner), onward("z2", "z2_o", partner)
    c_z2y, c_z3 = onward("z2", "z2y", across), onward("z2", "z3", znext)
    c_z2y_o, c_z3_o = onward("z2y", "z2y_o", partner), onward("z3", "z3_o", partner)
    c_z3y_z = [remote(at("far", rows), at("z3y", rows), zprev) for rows in upper]
    c_z3y_y = [remote(at("z3", lower), at("z3y", lower), across)]
    c_z3y_zo = [remote(at("z3y", rows), at("z3y_o", rows), partner) for rows in upper]
    c_z3y_yo = [remote(at("z3y", lower), at("z3y_o", lower), partner)]
    c_got_a, c_got_b = [remote(eng.g13.at[3], got_a, partner)], [remote(eng.g13.at[3], got_b, partner)]
    keep_a = pltpu.make_async_copy(eng.g13.at[2], own_a, part_sem.at[0])
    keep_b = pltpu.make_async_copy(eng.g13.at[2], own_b, part_sem.at[1])

    barrier = pltpu.get_barrier_semaphore()
    for device in (partner, across, znext, zprev):
        pl.semaphore_signal(barrier, inc=1, device_id=device, device_id_type=MESH)
    pl.semaphore_wait(barrier, 4)

    class Sent:
        def __init__(self, copy):
            self.copy = copy

        def wait(self):
            self.copy.wait_send()

    def arrived(copies, then=()):
        def event():
            for c in copies:
                c.wait_recv()
            start(then)
        return event

    start(c_other + c_far + c_z1)
    eng.stage([(tokens, grad_y, rg), at("other")], 2, True, False, [nothing, arrived(c_other)], (), (), [keep_a, c_got_a[0]],
              prelude=lambda: start(eng.load_w(0)))
    eng.stage([at("far"), at("far_o"), at("z1"), at("z1_o")], 2, False, False,
              [arrived(c_far, c_far_o), arrived(c_far_o), arrived(c_z1, c_z1_o + c_z1y + c_z2), arrived(c_z1_o)],
              ([keep_a], [Sent(c_got_a[0])]),
              ((5, arrived(c_z1y + c_z2, c_z2y + c_z3 + c_z1y_o + c_z2_o)),),
              [keep_b, c_got_b[0]])
    sum_b = Adder(own_b, got_b, (chip_a, chip_b), held, add_in_sem, add_out_sem, arrived(c_got_b))
    eng.stage([at("z1y"), at("z1y_o"), at("z2"), at("z2_o")], 0, False, True,
              [nothing, arrived(c_z1y_o), nothing, arrived(c_z2_o)],
              ([keep_b], [Sent(c_got_b[0])]),
              ((1, arrived(c_z2y + c_z3, c_z3y_y + c_z3y_z + c_z2y_o + c_z3_o)), (4, lambda: start(c_back)), (6, arrived(c_z3y_y + c_z3y_z[:1], c_z3y_yo + c_z3y_zo[:1]))), (), sum_b)
    arrived(c_z3y_z[1:], c_z3y_zo[1:])()
    sum_b.finish(n_loc - 1)
    arrived(c_z2y_o + c_z3_o + c_z3y_zo + c_z3y_yo + c_back + c_got_a)()
    for c in flights:
        if c is not c_got_a[0] and c is not c_got_b[0]:
            c.wait_send()


def rest_kernel(cfg, lead_ref, land, w1, w3, w2, b1, b3, b2, g1, g3, g2, *scratch):
    eng = Engine(cfg, lead_ref[0, 0], (w1, w3, w2), (b1, b3, b2), (g1, g3, g2), scratch, 2)

    def prelude():
        start(eng.load_w(0))
        for e in (0, 1):
            start(eng.load_g(e))

    names = ("z2y", "z2y_o", "z3", "z3_o", "z3y", "z3y_o")
    eng.stage([land.at[BLOCKS.index(n)] for n in names], 0, False, True, [nothing] * 6, (), (), (), prelude=prelude)


def call_kernel(name, kernel, cfg, args, shapes, n_src, n_own, extra_scratch, params):
    tok, d_model, d_ff, n_loc, cap, extra = (cfg[k] for k in ("tok", "d_model", "d_ff", "n_loc", "cap", "extra"))
    rows = n_loc * cap + extra
    scratch = [pltpu.VMEM((n_src, 2 * cap + extra, d_model), BF16)] * 2 + [
        pltpu.VMEM((n_src, 16, tok), F32),
        pltpu.VMEM((n_src, 2 * tok + RG_ROWS, d_model), BF16),
        pltpu.VMEM((n_src * cap, d_ff), BF16),
        pltpu.VMEM((n_src * cap, 2 * d_ff), BF16),
    ]
    for slots, kind in ((2, BF16), (4, F32)):
        scratch += [pltpu.VMEM((slots, d_model, 2 * d_ff), kind), pltpu.VMEM((slots, d_ff, d_model), kind)]
    scratch += [pltpu.SemaphoreType.DMA(n) for n in ((n_src, 3), (2, 3), (4, 3), (4, 3))]
    if n_own:
        scratch += [pltpu.VMEM((n_own, rows, d_model), BF16)] * 2
    unit = 2 * d_model * d_ff * rows
    return pl.pallas_call(
        functools.partial(kernel, cfg),
        in_specs=[pl.BlockSpec(memory_space=pltpu.SMEM)] + [pl.BlockSpec(memory_space=pl.ANY)] * (len(args) - 1),
        out_specs=[pl.BlockSpec(memory_space=pl.ANY)] * len(shapes),
        out_shape=shapes,
        scratch_shapes=scratch + extra_scratch,
        compiler_params=pltpu.CompilerParams(vmem_limit_bytes=67_000_000, **params),
        cost_estimate=pl.CostEstimate(flops=unit * (8 * n_src + 7 * n_own) // 8, bytes_accessed=100 << 20, transcendentals=0),
        name=name,
    )(*args)


def last_sum(own_a, got_a, back_a, back_b, tok, d_model):
    rows = back_a.shape[0] // 2
    n_all, n_half = 2 * tok // rows, tok // rows

    def kernel(m_ref, n_ref, a_ref, b_ref, y_ref, x_ref, m, n, v, out, in_sem, out_sem):
        def piece(ref, j):
            return ref.at[pl.ds(j * rows, rows)]

        loads, saves = [], []
        for j in range(n_all):
            other = piece(a_ref, j) if j < 2 else piece(b_ref, j - 2)
            loads.append([pltpu.make_async_copy(piece(m_ref, j), m.at[j], in_sem.at[j, 0]),
                          pltpu.make_async_copy(piece(n_ref, j), n.at[j], in_sem.at[j, 1]),
                          pltpu.make_async_copy(other, v.at[j], in_sem.at[j, 2])])
            place = piece(y_ref, j) if j < n_half else piece(x_ref, j - n_half)
            saves.append(pltpu.make_async_copy(out.at[j], place, out_sem.at[j]))
        for copies in loads:
            start(copies)
        for j in range(n_all):
            wait(loads[j])
            out[j] = (m[j] + n[j] + v[j]).astype(BF16)
            saves[j].start()
        wait(saves)

    dma = pltpu.SemaphoreType.DMA
    return pl.pallas_call(
        kernel,
        in_specs=[pl.BlockSpec(memory_space=pl.ANY)] * 4,
        out_specs=[pl.BlockSpec(memory_space=pl.ANY)] * 2,
        out_shape=[jax.ShapeDtypeStruct((tok, d_model), BF16)] * 2,
        scratch_shapes=[pltpu.VMEM((n_all, rows, d_model), F32)] * 3 + [pltpu.VMEM((n_all, rows, d_model), BF16), dma((n_all, 3)), dma((n_all,))],
        compiler_params=pltpu.CompilerParams(vmem_limit_bytes=67_000_000),
        name="last",
    )(own_a, got_a, back_a, back_b)


def solution(mesh):
    n_data, n_er = mesh.shape["data"], mesh.shape["expert"]
    row_spec = P(("pod", "data", "expert"), None)
    w_spec = P("expert", None, None)
    grad_spec = P(("pod", "expert"), None, None)
    across = [(r, r ^ 2) for r in range(n_er)]

    def body(tokens, routes, gates, grad_y, w_in1, w_in3, w_out):
        n_loc, d_model, d_ff = w_in1.shape
        n_exp, tok = n_loc * n_er, tokens.shape[0]
        cap, cap_hot = caps(tok, routes.shape[1], n_exp)
        cfg = dict(tok=tok, d_model=d_model, d_ff=d_ff, n_loc=n_loc, n_exp=n_exp, cap=cap, extra=cap_hot - cap,
                   n_data=n_data, n_er=n_er)
        lead = lax.axis_index("expert").astype(jnp.int32).reshape(1, 1)
        gate = gates.T
        hi = lax.reduce_precision(gate, 8, 7)
        mid = lax.reduce_precision(gate - hi, 8, 7)
        low = gate - hi - mid
        rg = jnp.concatenate([jnp.concatenate([routes.T.astype(F32), hi], 0), jnp.concatenate([mid, low], 0)], 1).astype(BF16)
        weights = (w_in1, w_in3, w_out)
        grads = [jax.ShapeDtypeStruct(w.shape, F32) for w in weights]
        sums = [jax.ShapeDtypeStruct((2 * tok, d_model), F32)] * 4
        land = jax.ShapeDtypeStruct((len(BLOCKS), 2 * tok + RG_ROWS, d_model), BF16)
        dma, n_fly, quarter = pltpu.SemaphoreType.DMA, 28, 2 * (2 * tok // n_loc)
        sums += [jax.ShapeDtypeStruct((n, d_model), F32) for n in (quarter, 2 * tok - quarter, quarter)]
        *acc, land, own_a, _, got_a, _, _, chip_b, back_a = call_kernel(
            "roam", roam_kernel, cfg, [lead, tokens, grad_y, rg, *weights], [*grads, land, *sums], 4, 2,
            [dma((n_fly,)), dma((n_fly,)), dma((2,)), pltpu.VMEM((2, 2, 2 * tok // n_loc, d_model), F32), dma((2, 2)), dma((2,))],
            dict(collective_id=0, has_side_effects=True))
        back_b = lax.ppermute(chip_b, "expert", across)
        acc1, acc3, acc2 = call_kernel("rest", rest_kernel, cfg, [lead, land, *weights, *acc], grads, 6, 0, [], {})
        y_out, grad_x = last_sum(own_a, got_a, back_a, back_b, tok, d_model)
        return y_out, grad_x, acc1, acc3, acc2

    return jax.shard_map(body, mesh=mesh,
                         in_specs=(row_spec, row_spec, row_spec, row_spec, w_spec, w_spec, w_spec),
                         out_specs=(row_spec, row_spec, grad_spec, grad_spec, grad_spec),
                         check_vma=False)
```

```python
import functools

import jax
import jax.numpy as jnp
from jax import lax
from jax.experimental import pallas as pl
from jax.experimental.pallas import tpu as pltpu
from jax.sharding import PartitionSpec as P

MESH = pl.DeviceIdType.MESH
BLOCKS = ("other", "far", "far_o", "z1", "z1_o", "z1y", "z1y_o", "z2", "z2_o", "z2y", "z2y_o", "z3", "z3_o", "z3y", "z3y_o")
N_HOT = 2
RG_ROWS = 16
F32, BF16 = jnp.float32, jnp.bfloat16


def caps(tok_dev, top_k, n_exp):
    cap_hot = 3 * tok_dev // 8
    cap_cold = max(8, ((tok_dev * top_k - N_HOT * cap_hot) // (n_exp - N_HOT) + 7) // 8 * 8)
    return cap_cold, cap_hot


def dot_nn(a, b):
    return lax.dot_general(a, b, (((1,), (0,)), ((), ())), preferred_element_type=F32)


def dot_nt(a, b):
    return lax.dot_general(a, b, (((1,), (1,)), ((), ())), preferred_element_type=F32)


def dot_tn(a, b):
    return lax.dot_general(a, b, (((0,), (0,)), ((), ())), preferred_element_type=F32)


def prefix(m):
    lane = lax.broadcasted_iota(jnp.int32, m.shape, 1)
    step = 1
    while step < m.shape[1]:
        m = m + jnp.where(lane >= step, pltpu.roll(m, step, 1), 0.0)
        step *= 2
    return m


class Engine:
    def __init__(self, cfg, lead, weights, bases, outs, scratch, group):
        self.__dict__.update(cfg)
        self.lead, self.weights, self.bases, self.outs, self.group = lead, weights, bases, outs, group
        (self.rows_x, self.rows_d, self.meta, self.buf, self.hid, self.dab, self.w13, self.w2, self.g13, self.g2,
         self.src_sem, self.w_sem, self.in_sem, self.out_sem) = scratch[:14]
        self.own_scratch = scratch[14:]
        hot = jnp.logical_or(lead * self.n_loc == 0, lead * self.n_loc == self.n_exp // 2)
        self.far = jnp.where(hot, float(self.cap), float(2 * self.tok))
        self.cold, self.part = self.n_loc * self.cap, group * self.cap

    def triple(self, both, single, slot):
        f = self.d_ff
        return both.at[slot, :, 0:f], both.at[slot, :, f:2 * f], single.at[slot]

    def load_w(self, e):
        slot = lax.rem(e, 2)
        return [pltpu.make_async_copy(w.at[e], b, self.w_sem.at[slot, k])
                for k, (w, b) in enumerate(zip(self.weights, self.triple(self.w13, self.w2, slot)))]

    def load_g(self, e):
        slot = lax.rem(e, 4)
        return [pltpu.make_async_copy(w.at[e], b, self.in_sem.at[slot, k])
                for k, (w, b) in enumerate(zip(self.bases, self.triple(self.g13, self.g2, slot)))]

    def save_g(self, e):
        slot = lax.rem(e, 4)
        return [pltpu.make_async_copy(b, w.at[e], self.out_sem.at[slot, k])
                for k, (w, b) in enumerate(zip(self.outs, self.triple(self.g13, self.g2, slot)))]

    def fetches(self, s, ref):
        if not isinstance(ref, tuple):
            return [pltpu.make_async_copy(ref, self.buf.at[s], self.src_sem.at[s, 0])]
        dst = self.buf.at[s]
        return [pltpu.make_async_copy(r, dst.at[pl.ds(at, r.shape[0])], self.src_sem.at[s, k])
                for k, (r, at) in enumerate(zip(ref, (0, self.tok, 2 * self.tok)))]

    def match_rows(self, src, i, base, size):
        iota = lax.broadcasted_iota(jnp.int32, (size, self.tok), 0).astype(F32) + base
        return iota == self.meta[src, pl.ds(i, 1), :]

    def ranks(self, s):
        tok = self.tok
        rg = self.buf[s, 2 * tok:2 * tok + RG_ROWS, :].astype(F32)
        routes = rg[0:8, :tok]
        gates = (rg[8:16, :tok] + rg[0:8, tok:]) + rg[8:16, tok:]
        member, weight = [], []
        for i in range(self.n_loc):
            match = routes == (self.lead * self.n_loc + i).astype(F32)
            member.append(jnp.sum(jnp.where(match, 1.0, 0.0), axis=0, keepdims=True))
            weight.append(jnp.sum(jnp.where(match, gates, 0.0), axis=0, keepdims=True))
        member = jnp.concatenate(member, axis=0)
        self.meta[s, 0:8, :] = jnp.where(member > 0.0, prefix(member) - 1.0, -1.0)
        self.meta[s, 8:16, :] = jnp.concatenate(weight, axis=0)

    def gather(self, s, which):
        tok, meta, buf = self.tok, self.meta, self.buf
        pick, gate = [], []
        for i, base, at, size in which:
            match = self.match_rows(s, i, base, size)
            pick.append(jnp.where(match, 1.0, 0.0).astype(BF16))
            gate.append(jnp.sum(jnp.where(match, meta[s, pl.ds(8 + i, 1), :], 0.0), axis=1, keepdims=True))
        pick, gate = jnp.concatenate(pick, axis=0), jnp.concatenate(gate, axis=0)
        at, size = which[0][2], pick.shape[0]
        self.rows_x[s, at:at + size, :] = dot_nn(pick, buf[s, 0:tok, :]).astype(BF16)
        self.rows_d[s, at:at + size, :] = (dot_nn(pick, buf[s, tok:2 * tok, :]) * gate).astype(BF16)

    def block(self, n_src, n_own, at, size, keep, w, g, g_in, middle=lambda: None):
        d_model, d_ff, hid, dab = self.d_model, self.d_ff, self.hid, self.dab
        w13, w2 = self.w13.at[w], self.w2.at[w]
        rows = n_src * size

        def load(ref):
            return ref[0:n_src, pl.ds(at, size), :].reshape(rows, d_model)

        ab = dot_nn(load(self.rows_x), w13[...]).astype(BF16).astype(F32)
        dh = dot_nt(load(self.rows_d), w2[...])
        a, b = ab[:, :d_ff], ab[:, d_ff:]
        sig = 0.5 * jnp.tanh(0.5 * a) + 0.5
        act = a * sig
        hid[0:rows, :] = (act * b).astype(BF16)
        dab[0:rows, 0:d_ff] = (dh * b * sig * (1.0 + a * (1.0 - sig))).astype(BF16)
        dab[0:rows, d_ff:] = (dh * act).astype(BF16)
        middle()
        if size < self.cap and n_src <= 4:
            def columns(k, carry):
                cols = pl.ds(pl.multiple_of(k * d_ff, d_ff), d_ff)
                self.g13[g, :, cols] = self.g13[g, :, cols] + dot_tn(load(self.rows_x), dab[0:rows, cols])
                self.g2[g, :, cols] = self.g2[g, :, cols] + dot_tn(hid[0:rows, :], self.rows_d[0:n_src, pl.ds(at, size), cols].reshape(rows, d_ff))
                return carry

            lax.fori_loop(0, 2, columns, 0)
        else:
            for out, lhs, rhs in ((self.g13, load(self.rows_x), dab[0:rows, :]), (self.g2, hid[0:rows, :], load(self.rows_d))):
                if g_in:
                    out[g] = out[g] + dot_tn(lhs, rhs)
                else:
                    out[g] = dot_tn(lhs, rhs)
        if n_own:
            kept_o, kept_x = self.own_scratch[:2]
            m = n_own * size
            o = dot_nn(hid[0:m, :], w2[...]).astype(BF16)
            dx = dot_nt(dab[0:m, :], w13[...]).astype(BF16)
            kept_o[:, pl.ds(keep, size), :] = o.reshape(n_own, size, d_model)
            kept_x[:, pl.ds(keep, size), :] = dx.reshape(n_own, size, d_model)

    def stage(self, srcs, n_own, first, last, before, held, events, ship, each=None, prelude=lambda: None):
        n_src, n_loc, cap, group = len(srcs), self.n_loc, self.cap, self.group
        width = 1 if n_src == 2 else 2
        turns = n_src // width
        fetch = [self.fetches(s, r) for s, r in enumerate(srcs)]

        def ask(t):
            for s in range(t, n_src, turns):
                before[s]()
                start(fetch[s])

        eager = all(b is nothing for b in before)
        for t in range(turns if eager else 1):
            ask(t)
        prelude()

        def wave(p, carry):
            def turn(t, carry):
                some = [t + j * turns for j in range(width)]

                @pl.when(p == 0)
                def _():
                    for k in range(turns):
                        @pl.when(t == k)
                        def _(k=k):
                            for s in range(k, n_src, turns):
                                wait(fetch[s])
                    for s in some:
                        self.ranks(s)
                        self.gather(s, [(0, self.far, self.part, self.extra)])
                    for k in range(0 if eager or width == 1 else turns - 1):
                        @pl.when(t == k)
                        def _(k=k):
                            ask(k + 1)

                for s in some:
                    self.gather(s, [(group * p + i, 0.0, i * cap, cap) for i in range(group)])
                if width == 1 and not eager:
                    for k in range(turns - 1):
                        @pl.when(jnp.logical_and(p == 0, t == k))
                        def _(k=k):
                            ask(k + 1)
                return carry

            lax.fori_loop(0, turns, turn, 0)

            def one(i, carry):
                e = group * p + i
                wait(self.load_w(e))
                if last:
                    @pl.when(e + 1 < n_loc)
                    def _():
                        start(self.load_w(e + 1))
                else:
                    start(self.load_w(lax.rem(e + 1, n_loc)))

                def middle():
                    @pl.when(e >= 2)
                    def _():
                        wait(self.save_g(e - 2))

                    for k, copies in enumerate(held):
                        @pl.when(e == k)
                        def _(copies=copies):
                            wait(copies)

                    if first:
                        @pl.when(e + 2 >= n_loc)
                        def _():
                            start(self.load_g(e + 2 - n_loc))
                    elif last:
                        @pl.when(e + 2 < n_loc)
                        def _():
                            start(self.load_g(e + 2))
                    else:
                        start(self.load_g(lax.rem(e + 2, n_loc)))
                    if not first:
                        wait(self.load_g(e))

                self.block(n_src, n_own, pl.multiple_of(i * cap, cap), cap, pl.multiple_of(e * cap, cap),
                           lax.rem(e, 2), lax.rem(e, 4), not first, middle)

                @pl.when(e == 0)
                def more():
                    self.block(n_src, n_own, self.part, self.extra, self.cold, 0, 0, True)

                start(self.save_g(e))
                for k, event in events:
                    @pl.when(e == k)
                    def _(event=event):
                        event()
                if each is not None:
                    each(e)
                return carry

            lax.fori_loop(0, group, one, 0)
            return carry

        lax.fori_loop(0, n_loc // group, wave, 0)
        if n_own:
            self.combine(n_own, ship)
        elif last:
            wait(self.save_g(n_loc - 2))
            wait(self.save_g(n_loc - 1))

    def combine(self, n_own, ship):
        kept_o, kept_x = self.own_scratch[:2]
        cold, extra, cap, tok, n_loc = self.cold, self.extra, self.cap, self.tok, self.n_loc
        part, n_blk = self.part, n_loc // self.group
        pieces = [(i, 0.0, i // self.group, i % self.group * cap, cap) for i in range(n_loc)] + [(0, self.far, None, part, extra)]
        places = [(ref, pl.ds(lane * tok, tok)) for ref in (self.rows_x, self.rows_d) for lane in (0, 1)]

        def one(src, carry):
            for s in range(n_own):
                @pl.when(src == s)
                def _(s=s):
                    wait(self.save_g(n_loc - 2 + s))

            for i, base, blk, at, size in pieces:
                match = self.match_rows(src, i, base, size)
                gate = self.meta[src, 8 + i:9 + i, :]
                hi = gate.astype(BF16).astype(F32)
                mid = (gate - hi).astype(BF16).astype(F32)
                low = gate - hi - mid
                for k, v in enumerate((hi, mid, low, 1.0)):
                    ref, lanes = places[0 if blk is None else k]
                    ref[k if blk is None else blk, at:at + size, lanes] = jnp.where(match, v, 0.0).astype(BF16)

            def chosen(k):
                ref, lanes = places[k]
                return ref[0:n_blk, 0:part, lanes].reshape(cold, tok)

            spare, lanes = places[0]
            wide = self.d_model // 2

            def columns(h, carry):
                cols = pl.ds(pl.multiple_of(h * wide, wide), wide)
                o, rest = kept_o[src, 0:cold, cols], kept_o[src, cold:cold + extra, cols]
                y = dot_tn(chosen(0), o) + dot_tn(chosen(1), o) + dot_tn(chosen(2), o)
                gates = spare[0:3, part:part + extra, lanes].reshape(3 * extra, tok)
                self.g13[2 + src, 0:tok, cols] = y + dot_tn(gates, jnp.concatenate([rest] * 3, axis=0))
                dx = dot_tn(chosen(3), kept_x[src, 0:cold, cols])
                gates = spare[3, part:part + extra, lanes]
                self.g13[2 + src, tok:2 * tok, cols] = dx + dot_tn(gates, kept_x[src, cold:cold + extra, cols])
                return carry

            lax.fori_loop(0, 2, columns, 0)
            for s in range(n_own):
                @pl.when(src == s)
                def _(s=s):
                    ship[s].start()
            return carry

        lax.fori_loop(0, n_own, one, 0)


def start(copies):
    for c in copies:
        c.start()


def wait(copies):
    for c in copies:
        c.wait()


def nothing():
    pass


class Adder:
    def __init__(self, a, b, out, held, load_sem, save_sem, ready):
        self.a, self.b, self.out, self.held, self.load_sem, self.save_sem, self.ready = a, b, out, held, load_sem, save_sem, ready
        self.rows = held.shape[2]
        self.n_head = out[0].shape[0] // self.rows if out[0] is not None else 0

    def loads(self, k):
        slot, at = lax.rem(k, 2), pl.ds(pl.multiple_of(k * self.rows, self.rows), self.rows)
        return [pltpu.make_async_copy(v.at[at], self.held.at[slot, n], self.load_sem.at[slot, n]) for n, v in enumerate((self.a, self.b))]

    def save(self, k, head=False):
        slot = lax.rem(k, 2)
        ref, k = (self.out[0], k) if head else (self.out[1], k - self.n_head)
        at = pl.ds(pl.multiple_of(k * self.rows, self.rows), self.rows)
        return pltpu.make_async_copy(self.held.at[slot, 0], ref.at[at], self.save_sem.at[slot])

    def add(self, k):
        wait(self.loads(k))
        slot = lax.rem(k, 2)
        self.held[slot, 0] = self.held[slot, 0] + self.held[slot, 1]
        if self.n_head:
            @pl.when(k < self.n_head)
            def _():
                self.save(k, True).start()

        @pl.when(k >= self.n_head)
        def _():
            self.save(k).start()

    def saved(self, k):
        if self.n_head:
            @pl.when(k < self.n_head)
            def _():
                self.save(k, True).wait()

        @pl.when(k >= self.n_head)
        def _():
            self.save(k).wait()

    def __call__(self, e):
        @pl.when(e == 0)
        def _():
            self.ready()

        @pl.when(e >= 1)
        def _():
            self.add(e - 1)

        @pl.when(e >= 2)
        def _():
            self.saved(e - 2)

        start(self.loads(e))

    def finish(self, last):
        self.add(last)
        self.saved(last - 1)
        self.saved(last)


def roam_kernel(cfg, lead_ref, tokens, grad_y, rg, w1, w3, w2, g1, g3, g2, land, own_a, own_b, got_a, got_b, mine, chip_a, chip_b, back_a, *scratch):
    send_sem, recv_sem, part_sem, held, add_in_sem, add_out_sem = scratch[-6:]
    eng = Engine(cfg, lead_ref[0, 0], (w1, w3, w2), (g1, g3, g2), (g1, g3, g2), scratch[:-6], 2)
    q, r = lax.axis_index("data"), lax.axis_index("expert")
    n_data, n_er, tok, n_loc = cfg["n_data"], cfg["n_er"], cfg["tok"], cfg["n_loc"]
    partner = {"expert": r + 1 - 2 * lax.rem(r, 2)}
    across = {"expert": lax.rem(r + n_er // 2, n_er)}
    znext = {"data": lax.rem(q + 1, n_data)}
    zprev = {"data": lax.rem(q + n_data - 1, n_data)}

    def at(name, rows=None):
        ref = land.at[BLOCKS.index(name)]
        return ref if rows is None else ref.at[rows]

    flights = []

    def remote(src, dst, device):
        k = len(flights)
        copy = pltpu.make_async_remote_copy(src_ref=src, dst_ref=dst, send_sem=send_sem.at[k], recv_sem=recv_sem.at[k],
                                            device_id=device, device_id_type=MESH)
        flights.append(copy)
        return copy

    def first(name, device):
        parts = ((tokens, 0, tok), (grad_y, tok, tok), (rg, 2 * tok, RG_ROWS))
        return [remote(v, at(name, pl.ds(lo, n)), device) for v, lo, n in parts]

    def onward(src, dst, device):
        return [remote(at(src), at(dst), device)]

    cut = (2 * tok + RG_ROWS) // 16 // 16 * 11 * 16
    upper = [pl.ds(0, tok), pl.ds(tok, cut - tok)]
    lower = pl.ds(cut, 2 * tok + RG_ROWS - cut)
    c_back = [remote(chip_a, back_a, across)]
    c_other, c_far, c_z1 = first("other", partner), first("far", across), first("z1", znext)
    c_far_o, c_z1_o = onward("far", "far_o", partner), onward("z1", "z1_o", partner)
    c_z1y, c_z2 = onward("z1", "z1y", across), onward("z1", "z2", znext)
    c_z1y_o, c_z2_o = onward("z1y", "z1y_o", partner), onward("z2", "z2_o", partner)
    c_z2y, c_z3 = onward("z2", "z2y", across), onward("z2", "z3", znext)
    c_z2y_o, c_z3_o = onward("z2y", "z2y_o", partner), onward("z3", "z3_o", partner)
    c_z3y_z = [remote(at("far", rows), at("z3y", rows), zprev) for rows in upper]
    c_z3y_y = [remote(at("z3", lower), at("z3y", lower), across)]
    c_z3y_zo = [remote(at("z3y", rows), at("z3y_o", rows), partner) for rows in upper]
    c_z3y_yo = [remote(at("z3y", lower), at("z3y_o", lower), partner)]
    c_got_a, c_got_b = [remote(eng.g13.at[3], got_a, partner)], [remote(eng.g13.at[3], got_b, partner)]
    keep_a = pltpu.make_async_copy(eng.g13.at[2], own_a, part_sem.at[0])
    keep_b = pltpu.make_async_copy(eng.g13.at[2], own_b, part_sem.at[1])

    barrier = pltpu.get_barrier_semaphore()
    for device in (partner, across, znext, zprev):
        pl.semaphore_signal(barrier, inc=1, device_id=device, device_id_type=MESH)
    pl.semaphore_wait(barrier, 4)

    class Sent:
        def __init__(self, copy):
            self.copy = copy

        def wait(self):
            self.copy.wait_send()

    def arrived(copies, then=()):
        def event():
            for c in copies:
                c.wait_recv()
            start(then)
        return event

    start(c_other + c_far + c_z1)
    eng.stage([(tokens, grad_y, rg), at("other")], 2, True, False, [nothing, arrived(c_other)], (), (), [keep_a, c_got_a[0]],
              prelude=lambda: start(eng.load_w(0)))
    sum_a = Adder(own_a, got_a, (None, mine), held, add_in_sem, add_out_sem, arrived(c_got_a))
    eng.stage([at("far"), at("far_o"), at("z1"), at("z1_o")], 2, False, False,
              [arrived(c_far, c_far_o), arrived(c_far_o), arrived(c_z1, c_z1_o + c_z1y + c_z2), arrived(c_z1_o)],
              ([keep_a], [Sent(c_got_a[0])]),
              ((4, arrived(c_z1y + c_z2, c_z2y + c_z3 + c_z1y_o + c_z2_o)),),
              [keep_b, c_got_b[0]], sum_a)
    sum_a.finish(n_loc - 1)
    sum_b = Adder(own_b, got_b, (chip_a, chip_b), held, add_in_sem, add_out_sem, arrived(c_got_b))
    eng.stage([at("z1y"), at("z1y_o"), at("z2"), at("z2_o")], 0, False, True,
              [nothing, arrived(c_z1y_o), nothing, arrived(c_z2_o)],
              ([keep_b], [Sent(c_got_b[0])]),
              ((0, arrived(c_z2y + c_z3, c_z3y_y + c_z3y_z + c_z2y_o + c_z3_o)), (4, lambda: start(c_back)), (6, arrived(c_z3y_y + c_z3y_z[:1], c_z3y_yo + c_z3y_zo[:1]))), (), sum_b)
    sum_b.finish(n_loc - 1)
    arrived(c_z3y_z[1:], c_z3y_zo[1:])()
    arrived(c_z2y_o + c_z3_o + c_z3y_zo + c_z3y_yo + c_back)()
    for c in flights:
        if c is not c_got_a[0] and c is not c_got_b[0]:
            c.wait_send()


def rest_kernel(cfg, lead_ref, land, w1, w3, w2, b1, b3, b2, g1, g3, g2, *scratch):
    eng = Engine(cfg, lead_ref[0, 0], (w1, w3, w2), (b1, b3, b2), (g1, g3, g2), scratch, 2)

    def prelude():
        start(eng.load_w(0))
        for e in (0, 1):
            start(eng.load_g(e))

    names = ("z2y", "z2y_o", "z3", "z3_o", "z3y", "z3y_o")
    eng.stage([land.at[BLOCKS.index(n)] for n in names], 0, False, True, [nothing] * 6, (), (), (), prelude=prelude)


def call_kernel(name, kernel, cfg, args, shapes, n_src, n_own, extra_scratch, params):
    tok, d_model, d_ff, n_loc, cap, extra = (cfg[k] for k in ("tok", "d_model", "d_ff", "n_loc", "cap", "extra"))
    rows = n_loc * cap + extra
    scratch = [pltpu.VMEM((n_src, 2 * cap + extra, d_model), BF16)] * 2 + [
        pltpu.VMEM((n_src, 16, tok), F32),
        pltpu.VMEM((n_src, 2 * tok + RG_ROWS, d_model), BF16),
        pltpu.VMEM((n_src * cap, d_ff), BF16),
        pltpu.VMEM((n_src * cap, 2 * d_ff), BF16),
    ]
    for slots, kind in ((2, BF16), (4, F32)):
        scratch += [pltpu.VMEM((slots, d_model, 2 * d_ff), kind), pltpu.VMEM((slots, d_ff, d_model), kind)]
    scratch += [pltpu.SemaphoreType.DMA(n) for n in ((n_src, 3), (2, 3), (4, 3), (4, 3))]
    if n_own:
        scratch += [pltpu.VMEM((n_own, rows, d_model), BF16)] * 2
    unit = 2 * d_model * d_ff * rows
    return pl.pallas_call(
        functools.partial(kernel, cfg),
        in_specs=[pl.BlockSpec(memory_space=pltpu.SMEM)] + [pl.BlockSpec(memory_space=pl.ANY)] * (len(args) - 1),
        out_specs=[pl.BlockSpec(memory_space=pl.ANY)] * len(shapes),
        out_shape=shapes,
        scratch_shapes=scratch + extra_scratch,
        compiler_params=pltpu.CompilerParams(vmem_limit_bytes=67_000_000, **params),
        cost_estimate=pl.CostEstimate(flops=unit * (8 * n_src + 7 * n_own) // 8, bytes_accessed=100 << 20, transcendentals=0),
        name=name,
    )(*args)


def last_sum(mine, back_a, back_b, tok, d_model):
    rows = back_a.shape[0] // 2
    n_all, n_half = 2 * tok // rows, tok // rows

    def kernel(m_ref, a_ref, b_ref, y_ref, x_ref, m, v, out, in_sem, out_sem):
        def piece(ref, j):
            return ref.at[pl.ds(j * rows, rows)]

        loads, saves = [], []
        for j in range(n_all):
            other = piece(a_ref, j) if j < 2 else piece(b_ref, j - 2)
            loads.append([pltpu.make_async_copy(piece(m_ref, j), m.at[j], in_sem.at[j, 0]),
                          pltpu.make_async_copy(other, v.at[j], in_sem.at[j, 1])])
            place = piece(y_ref, j) if j < n_half else piece(x_ref, j - n_half)
            saves.append(pltpu.make_async_copy(out.at[j], place, out_sem.at[j]))
        for copies in loads:
            start(copies)
        for j in range(n_all):
            wait(loads[j])
            out[j] = (m[j] + v[j]).astype(BF16)
            saves[j].start()
        wait(saves)

    dma = pltpu.SemaphoreType.DMA
    return pl.pallas_call(
        kernel,
        in_specs=[pl.BlockSpec(memory_space=pl.ANY)] * 3,
        out_specs=[pl.BlockSpec(memory_space=pl.ANY)] * 2,
        out_shape=[jax.ShapeDtypeStruct((tok, d_model), BF16)] * 2,
        scratch_shapes=[pltpu.VMEM((n_all, rows, d_model), F32)] * 2 + [pltpu.VMEM((n_all, rows, d_model), BF16), dma((n_all, 2)), dma((n_all,))],
        compiler_params=pltpu.CompilerParams(vmem_limit_bytes=67_000_000),
        name="last",
    )(mine, back_a, back_b)


def solution(mesh):
    n_data, n_er = mesh.shape["data"], mesh.shape["expert"]
    row_spec = P(("pod", "data", "expert"), None)
    w_spec = P("expert", None, None)
    grad_spec = P(("pod", "expert"), None, None)
    across = [(r, r ^ 2) for r in range(n_er)]

    def body(tokens, routes, gates, grad_y, w_in1, w_in3, w_out):
        n_loc, d_model, d_ff = w_in1.shape
        n_exp, tok = n_loc * n_er, tokens.shape[0]
        cap, cap_hot = caps(tok, routes.shape[1], n_exp)
        cfg = dict(tok=tok, d_model=d_model, d_ff=d_ff, n_loc=n_loc, n_exp=n_exp, cap=cap, extra=cap_hot - cap,
                   n_data=n_data, n_er=n_er)
        lead = lax.axis_index("expert").astype(jnp.int32).reshape(1, 1)
        gate = gates.T
        hi = lax.reduce_precision(gate, 8, 7)
        mid = lax.reduce_precision(gate - hi, 8, 7)
        low = gate - hi - mid
        rg = jnp.concatenate([jnp.concatenate([routes.T.astype(F32), hi], 0), jnp.concatenate([mid, low], 0)], 1).astype(BF16)
        weights = (w_in1, w_in3, w_out)
        grads = [jax.ShapeDtypeStruct(w.shape, F32) for w in weights]
        sums = [jax.ShapeDtypeStruct((2 * tok, d_model), F32)] * 6
        land = jax.ShapeDtypeStruct((len(BLOCKS), 2 * tok + RG_ROWS, d_model), BF16)
        dma, n_fly, quarter = pltpu.SemaphoreType.DMA, 28, 2 * (2 * tok // n_loc)
        sums[5:] = [jax.ShapeDtypeStruct((n, d_model), F32) for n in (quarter, 2 * tok - quarter, quarter)]
        *acc, land, _, _, _, _, mine, _, chip_b, back_a = call_kernel(
            "roam", roam_kernel, cfg, [lead, tokens, grad_y, rg, *weights], [*grads, land, *sums], 4, 2,
            [dma((n_fly,)), dma((n_fly,)), dma((2,)), pltpu.VMEM((2, 2, 2 * tok // n_loc, d_model), F32), dma((2, 2)), dma((2,))],
            dict(collective_id=0, has_side_effects=True))
        back_b = lax.ppermute(chip_b, "expert", across)
        acc1, acc3, acc2 = call_kernel("rest", rest_kernel, cfg, [lead, land, *weights, *acc], grads, 6, 0, [], {})
        y_out, grad_x = last_sum(mine, back_a, back_b, tok, d_model)
        return y_out, grad_x, acc1, acc3, acc2

    return jax.shard_map(body, mesh=mesh,
                         in_specs=(row_spec, row_spec, row_spec, row_spec, w_spec, w_spec, w_spec),
                         out_specs=(row_spec, row_spec, grad_spec, grad_spec, grad_spec),
                         check_vma=False)
```
